32 devices in a mesh: groups: 2 (over y), src: 4 (over z), act: 4 (over x, core).
Axes of the slice: x: 2, y: 2, z: 4, core: 2. Of those that a mesh axis runs over, the one named last changes fastest.
Arguments:
- star_state: float32 [12, 4096], P(None, ('groups', 'src')), parts along dimension 1, may hold values from -6 to 6
- masses: float32 [4096], P(('groups', 'src')), parts along dimension 0, may hold values from 0.25 to 4
- phases: float32 [4096], P(('groups', 'src')), parts along dimension 0, may hold values from 0 to 1
- levels: int32 [4096], P(('groups', 'src')), parts along dimension 0, may hold values from 0 to 4, as said below
- active_list: int32 [2048], P(('groups', 'src', 'act')), parts along dimension 0, may hold values from 0 to 511, as said below
- active_count: int32 [32], P(('groups', 'src', 'act')), parts along dimension 0, may hold values from 0 to 64, as said below
Outputs:
- stepped_state: float32 [12, 4096], P(None, ('groups', 'src')), parts along dimension 1
The draws below stay inside these ranges and needn't reach their ends.
There are 2 independent parts, one for each index of `groups`. The reference program is written for one: setup_inputs(seed, part) draws one part's arguments, and reference() takes and returns one part's arrays. A program takes and returns all parts, laid end to end along the dimension named above; each array names one. Nothing has to cross between parts.
Inputs may be any that keep to these rules, and one draw needn't show every extreme that they name: `levels`: levels_j = 4 exactly for the stars that appear among the live entries of the lists. `active_list`: live entries (the first active_count ones of a device's 64) are distinct indices within the device's src shard; every active star of a shard is live in exactly one list of that shard's 4 devices; later slots hold arbitrary indices of the shard. `active_count`: at most 64 a device, reached in every draw; the counts of one src shard's devices sum to at most 128, reached by some shard in every draw.
All inputs are finite; a program needn't handle non-finite values.
Results may differ from the reference program's by a relative error of at most 0.0003.
Values sent between devices are 32-bit elements; how exact they have to be, the bound alone decides.
No kernel may reach another device: no remote copies, remote signals or barrier semaphores. Data moves between devices by JAX's collectives and lax.ppermute only.
A program may use at most 64 MiB of HBM per device.

```python
import math
import jax
import jax.numpy as jnp
from jax import lax

S_DEV = 512
A_SLOT = 64
LEVELS = 5
STEPS = 2
NSTARS = 2048
N_SRC = 4
N_ACT = 4


def layout(key):
    shards = NSTARS // S_DEV
    base = jax.random.fold_in(key, 7)
    keys = jax.random.split(base, 8)
    cap = A_SLOT
    first = jax.random.randint(keys[0], (shards,), cap // 4, cap + 1, dtype=jnp.int32)
    second = jax.random.randint(keys[1], (shards,), 0, cap + 1, dtype=jnp.int32)
    third = jax.random.randint(keys[2], (shards,), 0, jnp.minimum(cap, 2 * cap - first - second) + 1, dtype=jnp.int32)
    fourth = jax.random.randint(keys[3], (shards,), 0, jnp.minimum(cap, 2 * cap - first - second - third) + 1, dtype=jnp.int32)
    full_shard = jax.random.randint(keys[4], (), 0, shards, dtype=jnp.int32)
    is_full = jnp.arange(shards, dtype=jnp.int32) == full_shard
    first = jnp.where(is_full, cap, first)
    second = jnp.where(is_full, cap, second)
    third = jnp.where(is_full, 0, third)
    fourth = jnp.where(is_full, 0, fourth)
    grouped = jnp.stack([first, second, third, fourth], axis=1)
    scores = jax.random.randint(keys[5], (shards, 4), 0, 65536, dtype=jnp.int32) * 4 + jnp.arange(4, dtype=jnp.int32)[None, :]
    order = jnp.argsort(scores, axis=1)
    counts = jnp.take_along_axis(grouped, order, axis=1).astype(jnp.int32)
    totals = jnp.sum(counts, axis=1)
    star_scores = jax.random.randint(keys[6], (shards, S_DEV), 0, 65536, dtype=jnp.int32) * S_DEV + jnp.arange(S_DEV, dtype=jnp.int32)[None, :]
    chosen = jnp.argsort(star_scores, axis=1).astype(jnp.int32)
    rank_of = jnp.argsort(chosen, axis=1).astype(jnp.int32)
    list_starts = jnp.cumsum(counts, axis=1) - counts
    position = (list_starts[:, :, None] + jnp.arange(cap, dtype=jnp.int32)[None, None, :]) % S_DEV
    lists = jnp.take_along_axis(chosen, position.reshape(shards, 4 * cap), axis=1).astype(jnp.int32)
    coarse = jax.random.randint(keys[7], (shards, S_DEV), 0, LEVELS - 1, dtype=jnp.int32)
    level_table = jnp.where(rank_of < totals[:, None], LEVELS - 1, coarse).astype(jnp.int32)
    return (level_table.reshape(-1), lists.reshape(-1), counts.reshape(-1))


def draw_levels(key, part):
    return layout(key)[0]


def draw_active_list(key, part):
    return layout(key)[1]


def draw_active_count(key, part):
    return layout(key)[2]


def block_scale(key, extent, cuts, least, high):
    gain = 1.0
    for dim, shards_of in cuts:
        steps = jax.random.uniform(jax.random.fold_in(jax.random.fold_in(key, 6), dim), (shards_of,), jnp.float32, least / len(cuts), high / len(cuts))
        gain = gain * jnp.repeat(jnp.exp(steps), extent[dim] // shards_of).reshape((-1,) + (1,) * (len(extent) - 1 - dim))
    return gain


def centred(stream_key, dims, spread, reach, cuts=(), kind=jnp.bfloat16):
    entries = jax.random.normal(stream_key, dims, jnp.float32) * spread
    if len(cuts) > 0:
        entries = block_scale(stream_key, dims, cuts, -0.22, 0.18) * entries
    return jnp.clip(entries, min=-reach, max=reach).astype(kind)


def setup_inputs(seed: int = 0, part: int = 0) -> dict:
    streams_of = jax.random.split(jax.random.key(seed), 7)
    part_keys = jax.random.split(jax.random.fold_in(streams_of[6], part), 7)
    star_state = centred(part_keys[0], (12, NSTARS), 1.0, 6.0, ((1, 4),), jnp.float32)
    masses = jnp.clip(jnp.exp(math.log(4.0) - 2.7725887 * jax.random.uniform(part_keys[1], (NSTARS,), jnp.float32) ** block_scale(part_keys[1], (NSTARS,), ((0, 4),), -0.2, 0.2)), 0.25, 4.0)
    phases = jnp.clip(1.0 * jax.random.uniform(part_keys[2], (NSTARS,), jnp.float32) ** block_scale(part_keys[2], (NSTARS,), ((0, 4),), -0.2, 0.2), 0.0, 1.0)
    levels = draw_levels(jax.random.fold_in(jax.random.fold_in(streams_of[6], part), 71), part)
    active_list = draw_active_list(jax.random.fold_in(jax.random.fold_in(streams_of[6], part), 71), part)
    active_count = draw_active_count(jax.random.fold_in(jax.random.fold_in(streams_of[6], part), 71), part)
    return {"star_state": star_state, "masses": masses, "phases": phases, "levels": levels, "active_list": active_list, "active_count": active_count}


soften_sq = 0.0004
fine_step = 0.03125

def predict(star_state, elapsed):
    interval = elapsed[None, :]
    position = star_state[0:3] + interval * (star_state[3:6] + interval * (0.5 * star_state[6:9] + interval * star_state[9:12] / 6.0))
    velocity = star_state[3:6] + interval * (star_state[6:9] + 0.5 * interval * star_state[9:12])
    return jnp.concatenate([position, velocity], axis=0)

def pair_block(targets, sources):
    delta_pos = sources[0:3, None, :] - targets[0:3, :, None]
    delta_vel = sources[3:6, None, :] - targets[3:6, :, None]
    dist_sq = delta_pos[0] * delta_pos[0] + delta_pos[1] * delta_pos[1] + delta_pos[2] * delta_pos[2] + soften_sq
    inverse = lax.rsqrt(dist_sq)
    inv_sq = inverse * inverse
    weight = sources[6][None, :] * inverse * inv_sq
    radial = (delta_pos[0] * delta_vel[0] + delta_pos[1] * delta_vel[1] + delta_pos[2] * delta_vel[2]) * inv_sq * 3.0
    acceleration = lax.optimization_barrier(jnp.sum(weight[None] * delta_pos, axis=2))
    jerk_sum = lax.optimization_barrier(jnp.sum(weight[None] * (delta_vel - radial[None] * delta_pos), axis=2))
    return jnp.concatenate([acceleration, jerk_sum], axis=0)

def over_sources(targets, sources):
    count_src = sources.shape[1]
    width = 512
    if count_src > width and count_src % width == 0:
        blocks = sources.reshape(7, count_src // width, width).transpose(1, 0, 2)

        def accumulate(running, portion):
            return (running + pair_block(targets, portion), None)
        init = jnp.zeros((6, targets.shape[1]), jnp.float32)
        running, unused = lax.scan(accumulate, init, blocks)
        return running
    return pair_block(targets, sources)

def pair_forces(targets, sources):
    count_tgt = targets.shape[1]
    width = 512
    if count_tgt > width and count_tgt % width == 0:
        blocks = targets.reshape(6, count_tgt // width, width).transpose(1, 0, 2)
        result = lax.map(lambda portion: over_sources(portion, sources), blocks)
        return result.transpose(1, 0, 2).reshape(6, count_tgt)
    return over_sources(targets, sources)

def correct(old_state, predicted_rows, forces):
    step_len = fine_step
    acc_old = old_state[6:9]
    jerk_old = old_state[9:12]
    acc_new = forces[0:3]
    jerk_new = forces[3:6]
    snap_term = (-6.0 * (acc_old - acc_new) - step_len * (4.0 * jerk_old + 2.0 * jerk_new)) / (step_len * step_len)
    crackle = (12.0 * (acc_old - acc_new) + 6.0 * step_len * (jerk_old + jerk_new)) / (step_len * step_len * step_len)
    position = predicted_rows[0:3] + step_len ** 4 / 24.0 * snap_term + step_len ** 5 / 120.0 * crackle
    velocity = predicted_rows[3:6] + step_len ** 3 / 6.0 * snap_term + step_len ** 4 / 24.0 * crackle
    return jnp.concatenate([position, velocity, acc_new, jerk_new], axis=0)

def reference(star_state, masses, phases, levels, active_list, active_count):
    lists = active_list.reshape(N_SRC, N_ACT, A_SLOT).astype(jnp.int32)
    counts = active_count.reshape(N_SRC, N_ACT).astype(jnp.int32)
    list_ends = jnp.cumsum(counts, axis=1)
    list_starts = list_ends - counts
    totals = list_ends[:, -1]
    slot_index = jnp.arange(A_SLOT, dtype=jnp.int32)
    position = jnp.where(slot_index[None, None, :] < counts[:, :, None], list_starts[:, :, None] + slot_index[None, None, :], 2 * A_SLOT)
    shard_index = jnp.broadcast_to(jnp.arange(N_SRC, dtype=jnp.int32)[:, None, None], position.shape)
    compact = jnp.zeros((N_SRC, 2 * A_SLOT + 1), jnp.int32).at[shard_index, position].set(lists)[:, :2 * A_SLOT]
    live = jnp.arange(2 * A_SLOT, dtype=jnp.int32)[None, :] < totals[:, None]
    members = (jnp.arange(N_SRC, dtype=jnp.int32)[:, None] * S_DEV + compact).reshape(-1)
    write_index = jnp.where(live.reshape(-1), members, NSTARS).astype(jnp.int32)
    weights = masses / NSTARS
    tick_count = jnp.left_shift(jnp.int32(1), (LEVELS - 1 - levels).astype(jnp.int32)).astype(jnp.float32)
    state_now = star_state
    for substep in range(STEPS):
        elapsed = jnp.where(levels == LEVELS - 1, 1.0, phases * (tick_count - STEPS) + (substep + 1)) * fine_step
        predicted = predict(state_now, elapsed)
        sources = jnp.concatenate([predicted, weights[None, :]], axis=0)
        targets = predicted[:, members]
        forces = pair_forces(targets, sources)
        new_state = correct(state_now[:, members], targets, forces)
        state_now = state_now.at[:, write_index].set(new_state, mode='drop')
    return state_now
```

```python
import jax
import jax.numpy as jnp
from jax import lax
from jax.experimental import pallas as pl
from jax.experimental.pallas import tpu as pltpu
from jax.sharding import PartitionSpec as P

LEVELS = 5
STEPS = 2
MAX_DIRECT = 8


soften_sq = 0.0004
fine_step = 0.03125


def predict(star_state, elapsed):
    interval = elapsed[None, :]
    position = star_state[0:3] + interval * (
        star_state[3:6] + interval * (0.5 * star_state[6:9] + interval * star_state[9:12] / 6.0)
    )
    velocity = star_state[3:6] + interval * (star_state[6:9] + 0.5 * interval * star_state[9:12])
    return jnp.concatenate([position, velocity], axis=0)


def pair_block(targets, sources):
    delta_pos = sources[0:3, None, :] - targets[0:3, :, None]
    delta_vel = sources[3:6, None, :] - targets[3:6, :, None]
    dist_sq = (
        delta_pos[0] * delta_pos[0]
        + delta_pos[1] * delta_pos[1]
        + delta_pos[2] * delta_pos[2]
        + soften_sq
    )
    inverse = lax.rsqrt(dist_sq)
    inv_sq = inverse * inverse
    weight = sources[6][None, :] * inverse * inv_sq
    radial = (
        (delta_pos[0] * delta_vel[0] + delta_pos[1] * delta_vel[1] + delta_pos[2] * delta_vel[2])
        * inv_sq
        * 3.0
    )
    acceleration = jnp.sum(weight[None] * delta_pos, axis=2)
    jerk_sum = jnp.sum(weight[None] * (delta_vel - radial[None] * delta_pos), axis=2)
    return jnp.concatenate([acceleration, jerk_sum], axis=0)


def over_sources(targets, sources):
    count_src = sources.shape[1]
    width = 512
    blocks = sources.reshape(7, count_src // width, width).transpose(1, 0, 2)

    def accumulate(running, portion):
        return (running + pair_block(targets, portion), None)

    init = jnp.zeros((6, targets.shape[1]), jnp.float32)
    running, unused = lax.scan(accumulate, init, blocks)
    return running


def corrected(acc_old, jerk_old, position, velocity, acc_new, jerk_new):
    snap_term = (-6.0 * (acc_old - acc_new) - fine_step * (4.0 * jerk_old + 2.0 * jerk_new)) / (
        fine_step * fine_step
    )
    crackle = (12.0 * (acc_old - acc_new) + 6.0 * fine_step * (jerk_old + jerk_new)) / (
        fine_step * fine_step * fine_step
    )
    new_position = position + fine_step**4 / 24.0 * snap_term + fine_step**5 / 120.0 * crackle
    new_velocity = velocity + fine_step**3 / 6.0 * snap_term + fine_step**4 / 24.0 * crackle
    return new_position, new_velocity


def correct(old_state, predicted_rows, forces):
    new_position, new_velocity = corrected(
        old_state[6:9],
        old_state[9:12],
        predicted_rows[0:3],
        predicted_rows[3:6],
        forces[0:3],
        forces[3:6],
    )
    return jnp.concatenate([new_position, new_velocity, forces], axis=0)


def gather_per_device(star_state, masses, phases, levels, active_list, active_count):
    shard_size = star_state.shape[1]
    total_stars = shard_size * lax.axis_size("src")
    weights = masses / total_stars
    slot_count = active_list.shape[0]
    live = jnp.arange(slot_count, dtype=jnp.int32) < active_count[0]
    write_index = jnp.where(live, active_list, shard_size)
    tick_count = jnp.left_shift(jnp.int32(1), LEVELS - 1 - levels).astype(jnp.float32)
    state_now = star_state
    for substep in range(STEPS):
        elapsed = (
            jnp.where(levels == LEVELS - 1, 1.0, phases * (tick_count - STEPS) + (substep + 1))
            * fine_step
        )
        predicted = predict(state_now, elapsed)
        sources = jnp.concatenate([predicted, weights[None, :]], axis=0)
        targets = predicted[:, active_list]
        forces = over_sources(targets, lax.all_gather(sources, "src", axis=1, tiled=True))
        new_state = correct(state_now[:, active_list], targets, forces)
        all_new, all_index = (
            lax.all_gather(new_state, "act", axis=1, tiled=True),
            lax.all_gather(write_index, "act", axis=0, tiled=True),
        )
        state_now = state_now.at[:, all_index].set(all_new, mode="drop")
    return state_now


def three_terms(x):
    high = x.astype(jnp.bfloat16)
    rest = x - high.astype(jnp.float32)
    middle = rest.astype(jnp.bfloat16)
    low = (rest - middle.astype(jnp.float32)).astype(jnp.bfloat16)
    return jnp.concatenate([high, middle, low], axis=0)


def add_terms(y):
    rows = y.shape[0] // 3
    return (y[0:rows] + y[rows : 2 * rows]) + y[2 * rows : 3 * rows]


def advance(position, velocity, acceleration, jerk, step):
    ahead = position + step * (velocity + step * (0.5 * acceleration + step * jerk / 6.0))
    speed = velocity + step * (acceleration + 0.5 * step * jerk)
    return ahead, speed


def prepare(slots, total_stars, state_ref, mass_ref, phase_ref, level_ref, out_ref, place_ref):
    size = state_ref.shape[1]
    level = level_ref[...]
    active = level == LEVELS - 1
    mask = jnp.where(active, 1.0, 0.0)
    blocks = size // 128
    grouped = jnp.concatenate(
        [mask[:, 128 * b : 128 * (b + 1)] for b in range(blocks)]
        + [jnp.zeros((16 - blocks, 128), jnp.float32)],
        axis=0,
    ).astype(jnp.bfloat16)
    lane_in = lax.broadcasted_iota(jnp.int32, (128, 256), 0)
    lane_out = lax.broadcasted_iota(jnp.int32, (128, 256), 1)
    counting = jnp.where((lane_in <= lane_out) | (lane_out >= 128), 1.0, 0.0).astype(jnp.bfloat16)
    counts = jnp.dot(grouped, counting, preferred_element_type=jnp.float32)
    so_far = []
    before = jnp.zeros((1, 128), jnp.float32)
    for b in range(blocks):
        so_far.append(counts[b : b + 1, 0:128] + before)
        before = before + counts[b : b + 1, 128:256]
    rank = jnp.concatenate(so_far, axis=1)
    total = jnp.concatenate([before] * blocks, axis=1)
    star = lax.broadcasted_iota(jnp.int32, (1, size), 1).astype(jnp.float32)
    place = jnp.where(active, rank - 1.0, total + star - rank)
    place_ref[0:1, :] = place
    place_ref[1:2, :] = mask
    place_ref[2:8, :] = jnp.zeros((6, size), jnp.float32)

    tick_count = jnp.left_shift(jnp.int32(1), LEVELS - 1 - level).astype(jnp.float32)
    offset = phase_ref[...] * (tick_count - STEPS)
    position, velocity = state_ref[0:3, :], state_ref[3:6, :]
    acceleration, jerk = state_ref[6:9, :], state_ref[9:12, :]
    rows = []
    for substep in range(STEPS):
        elapsed = jnp.where(active, 1.0, offset + (substep + 1)) * fine_step
        rows.extend(advance(position, velocity, acceleration, jerk, elapsed))
        if substep == 0:
            rows.append(mass_ref[...] / total_stars)
            rows.append(mask)
    rows.append(jnp.zeros((2, size), jnp.float32))
    rows.extend([acceleration, jerk, jnp.zeros((10, size), jnp.float32)])
    terms = three_terms(jnp.concatenate(rows, axis=0))
    slot = lax.broadcasted_iota(jnp.int32, (size, size), 0).astype(jnp.float32)
    chosen = jnp.where(slot == place, 1.0, 0.0).astype(jnp.bfloat16)
    moved = add_terms(
        lax.dot_general(
            terms, chosen, (((1,), (1,)), ((), ())), preferred_element_type=jnp.float32
        )
    )
    out_ref[...] = moved[0:16]
    across = size // slots
    for k in range(6):
        out_ref[14 + k // across : 15 + k // across, slots * (k % across) : slots * (k % across + 1)] = (
            moved[16 + k : 17 + k, 0:slots]
        )


def pair_terms(source, target, sums):
    sx, sy, sz, su, sv, sw, weight = source
    tx, ty, tz, tu, tv, tw = target
    dx, dy, dz = sx - tx, sy - ty, sz - tz
    du, dv, dw = su - tu, sv - tv, sw - tw
    inverse = lax.rsqrt(dx * dx + dy * dy + dz * dz + soften_sq)
    inv_sq = inverse * inverse
    pull = weight * inverse * inv_sq
    radial = (dx * du + dy * dv + dz * dw) * (inv_sq * 3.0)
    ax, ay, az, jx, jy, jz = sums
    return (
        ax + pull * dx,
        ay + pull * dy,
        az + pull * dz,
        jx + pull * (du - radial * dx),
        jy + pull * (dv - radial * dy),
        jz + pull * (dw - radial * dz),
    )


def pair_sums(columns_ref, targets, unroll):
    count = columns_ref.shape[0] // 8
    lanes = targets[0].shape[1]
    spread = [
        [jnp.broadcast_to(t[r : r + 1], (8, lanes)) for r in range(6)] for t in targets
    ]

    def body(step, sums):
        for inner in range(unroll):
            group = columns_ref[pl.ds((step * unroll + inner) * 8, 8), :]
            source = [jnp.broadcast_to(group[:, r : r + 1], (8, lanes)) for r in range(7)]
            sums = tuple(pair_terms(source, t, s) for t, s in zip(spread, sums))
        return sums

    zero = jnp.zeros((8, lanes), jnp.float32)
    sums = lax.fori_loop(0, count // unroll, body, tuple((zero,) * 6 for _ in targets))
    return [jnp.concatenate([jnp.sum(q, axis=0, keepdims=True) for q in s], axis=0) for s in sums]


def advance_stars(slots, shards, *refs):
    sent = refs[:shards]
    state_ref, place_ref, out_ref, columns_ref = refs[shards:]
    size = state_ref.shape[1]
    across = size // slots
    for d in range(shards):
        columns_ref[d * size : (d + 1) * size, :] = jnp.transpose(sent[d][0:8, :])
    targets = [sent[d][0:6, 0:slots] for d in range(shards)]
    forces = pair_sums(columns_ref, targets, 8)
    own = None
    for d in range(shards):
        first = [
            sent[d][14 + k // across : 15 + k // across, slots * (k % across) : slots * (k % across + 1)]
            for k in range(6)
        ]
        first = jnp.concatenate(first, axis=0)
        acceleration, jerk = forces[d][0:3], forces[d][3:6]
        position, velocity = corrected(
            first[0:3], first[3:6], targets[d][0:3], targets[d][3:6], acceleration, jerk
        )
        ahead, speed = advance(position, velocity, acceleration, jerk, fine_step)
        active = sent[d][7:8, 0:slots] > 0.5
        still = sent[d][8:14, 0:slots]
        again = jnp.where(active, jnp.concatenate([ahead, speed], axis=0), still)
        if d == 0:
            own = again
        later = jnp.concatenate([again, sent[d][8:14, slots:size]], axis=1)
        later = jnp.concatenate([later, sent[d][6:8, :]], axis=0)
        columns_ref[d * size : (d + 1) * size, :] = jnp.transpose(later)
    second = pair_sums(columns_ref, [own], 16)[0]
    position, velocity = corrected(
        forces[0][0:3], forces[0][3:6], own[0:3], own[3:6], second[0:3], second[3:6]
    )
    new_rows = jnp.concatenate(
        [position, velocity, second, jnp.zeros((4, slots), jnp.float32)], axis=0
    )
    slot = lax.broadcasted_iota(jnp.int32, (slots, size), 0).astype(jnp.float32)
    chosen = jnp.where(slot == place_ref[0:1, :], 1.0, 0.0).astype(jnp.bfloat16)
    back = add_terms(jnp.dot(three_terms(new_rows), chosen, preferred_element_type=jnp.float32))
    out_ref[...] = jnp.where(place_ref[1:2, :] > 0.5, back[0:12], state_ref[...])


def direct_per_device(star_state, masses, phases, levels, active_list, active_count):
    del active_count
    size = star_state.shape[1]
    shards = lax.axis_size("src")
    slots = 2 * active_list.shape[0]
    whole = pl.BlockSpec(memory_space=pltpu.VMEM)
    message, place = pl.pallas_call(
        lambda *refs: prepare(slots, size * shards, *refs),
        out_shape=(
            jax.ShapeDtypeStruct((16, size), jnp.float32),
            jax.ShapeDtypeStruct((8, size), jnp.float32),
        ),
        in_specs=[whole] * 4,
        out_specs=(whole, whole),
        name="prepare",
    )(star_state, masses.reshape(1, size), phases.reshape(1, size), levels.reshape(1, size))
    sent = [message]
    for shift in range(1, shards):
        pairs = [(d, (d + shift) % shards) for d in range(shards)]
        sent.append(lax.ppermute(message, "src", pairs))
    return pl.pallas_call(
        lambda *refs: advance_stars(slots, shards, *refs),
        out_shape=jax.ShapeDtypeStruct((12, size), jnp.float32),
        in_specs=[whole] * (shards + 2),
        out_specs=whole,
        scratch_shapes=[pltpu.VMEM((shards * size, 8), jnp.float32)],
        name="advance_stars",
    )(*sent, star_state, place)


def solution(mesh):
    in_specs = (
        P(None, ("groups", "src")),
        P(("groups", "src")),
        P(("groups", "src")),
        P(("groups", "src")),
        P(("groups", "src", "act")),
        P(("groups", "src", "act")),
    )
    out_specs = P(None, ("groups", "src"))
    few = mesh.shape["src"] <= MAX_DIRECT
    return jax.shard_map(
        direct_per_device if few else gather_per_device,
        mesh=mesh,
        in_specs=in_specs,
        out_specs=out_specs,
        check_vma=False,
    )
```

```python
import jax
import jax.numpy as jnp
from jax import lax
from jax.experimental import pallas as pl
from jax.experimental.pallas import tpu as pltpu
from jax.sharding import PartitionSpec as P

LEVELS = 5
STEPS = 2
MAX_DIRECT = 8


soften_sq = 0.0004
fine_step = 0.03125


def predict(star_state, elapsed):
    interval = elapsed[None, :]
    position = star_state[0:3] + interval * (
        star_state[3:6] + interval * (0.5 * star_state[6:9] + interval * star_state[9:12] / 6.0)
    )
    velocity = star_state[3:6] + interval * (star_state[6:9] + 0.5 * interval * star_state[9:12])
    return jnp.concatenate([position, velocity], axis=0)


def pair_block(targets, sources):
    delta_pos = sources[0:3, None, :] - targets[0:3, :, None]
    delta_vel = sources[3:6, None, :] - targets[3:6, :, None]
    dist_sq = (
        delta_pos[0] * delta_pos[0]
        + delta_pos[1] * delta_pos[1]
        + delta_pos[2] * delta_pos[2]
        + soften_sq
    )
    inverse = lax.rsqrt(dist_sq)
    inv_sq = inverse * inverse
    weight = sources[6][None, :] * inverse * inv_sq
    radial = (
        (delta_pos[0] * delta_vel[0] + delta_pos[1] * delta_vel[1] + delta_pos[2] * delta_vel[2])
        * inv_sq
        * 3.0
    )
    acceleration = jnp.sum(weight[None] * delta_pos, axis=2)
    jerk_sum = jnp.sum(weight[None] * (delta_vel - radial[None] * delta_pos), axis=2)
    return jnp.concatenate([acceleration, jerk_sum], axis=0)


def over_sources(targets, sources):
    count_src = sources.shape[1]
    width = 512
    blocks = sources.reshape(7, count_src // width, width).transpose(1, 0, 2)

    def accumulate(running, portion):
        return (running + pair_block(targets, portion), None)

    init = jnp.zeros((6, targets.shape[1]), jnp.float32)
    running, unused = lax.scan(accumulate, init, blocks)
    return running


def corrected(acc_old, jerk_old, position, velocity, acc_new, jerk_new):
    snap_term = (-6.0 * (acc_old - acc_new) - fine_step * (4.0 * jerk_old + 2.0 * jerk_new)) / (
        fine_step * fine_step
    )
    crackle = (12.0 * (acc_old - acc_new) + 6.0 * fine_step * (jerk_old + jerk_new)) / (
        fine_step * fine_step * fine_step
    )
    new_position = position + fine_step**4 / 24.0 * snap_term + fine_step**5 / 120.0 * crackle
    new_velocity = velocity + fine_step**3 / 6.0 * snap_term + fine_step**4 / 24.0 * crackle
    return new_position, new_velocity


def correct(old_state, predicted_rows, forces):
    new_position, new_velocity = corrected(
        old_state[6:9],
        old_state[9:12],
        predicted_rows[0:3],
        predicted_rows[3:6],
        forces[0:3],
        forces[3:6],
    )
    return jnp.concatenate([new_position, new_velocity, forces], axis=0)


def gather_per_device(star_state, masses, phases, levels, active_list, active_count):
    shard_size = star_state.shape[1]
    total_stars = shard_size * lax.axis_size("src")
    weights = masses / total_stars
    slot_count = active_list.shape[0]
    live = jnp.arange(slot_count, dtype=jnp.int32) < active_count[0]
    write_index = jnp.where(live, active_list, shard_size)
    tick_count = jnp.left_shift(jnp.int32(1), LEVELS - 1 - levels).astype(jnp.float32)
    state_now = star_state
    for substep in range(STEPS):
        elapsed = (
            jnp.where(levels == LEVELS - 1, 1.0, phases * (tick_count - STEPS) + (substep + 1))
            * fine_step
        )
        predicted = predict(state_now, elapsed)
        sources = jnp.concatenate([predicted, weights[None, :]], axis=0)
        targets = predicted[:, active_list]
        forces = over_sources(targets, lax.all_gather(sources, "src", axis=1, tiled=True))
        new_state = correct(state_now[:, active_list], targets, forces)
        all_new, all_index = (
            lax.all_gather(new_state, "act", axis=1, tiled=True),
            lax.all_gather(write_index, "act", axis=0, tiled=True),
        )
        state_now = state_now.at[:, all_index].set(all_new, mode="drop")
    return state_now


def three_terms(x):
    high = x.astype(jnp.bfloat16)
    rest = x - high.astype(jnp.float32)
    middle = rest.astype(jnp.bfloat16)
    low = (rest - middle.astype(jnp.float32)).astype(jnp.bfloat16)
    return jnp.concatenate([high, middle, low], axis=0)


def add_terms(y):
    rows = y.shape[0] // 3
    return (y[0:rows] + y[rows : 2 * rows]) + y[2 * rows : 3 * rows]


def advance(position, velocity, acceleration, jerk, step):
    ahead = position + step * (velocity + step * (0.5 * acceleration + step * jerk / 6.0))
    speed = velocity + step * (acceleration + 0.5 * step * jerk)
    return ahead, speed


def prepare(slots, total_stars, state_ref, mass_ref, phase_ref, level_ref, out_ref, place_ref):
    size = state_ref.shape[1]
    level = level_ref[...]
    active = level == LEVELS - 1
    mask = jnp.where(active, 1.0, 0.0)
    blocks = size // 128
    grouped = jnp.concatenate(
        [mask[:, 128 * b : 128 * (b + 1)] for b in range(blocks)]
        + [jnp.zeros((16 - blocks, 128), jnp.float32)],
        axis=0,
    ).astype(jnp.bfloat16)
    lane_in = lax.broadcasted_iota(jnp.int32, (128, 256), 0)
    lane_out = lax.broadcasted_iota(jnp.int32, (128, 256), 1)
    counting = jnp.where((lane_in <= lane_out) | (lane_out >= 128), 1.0, 0.0).astype(jnp.bfloat16)
    counts = jnp.dot(grouped, counting, preferred_element_type=jnp.float32)
    so_far = []
    before = jnp.zeros((1, 128), jnp.float32)
    for b in range(blocks):
        so_far.append(counts[b : b + 1, 0:128] + before)
        before = before + counts[b : b + 1, 128:256]
    rank = jnp.concatenate(so_far, axis=1)
    total = jnp.concatenate([before] * blocks, axis=1)
    star = lax.broadcasted_iota(jnp.int32, (1, size), 1).astype(jnp.float32)
    place = jnp.where(active, rank - 1.0, total + star - rank)
    place_ref[0:1, :] = place
    place_ref[1:2, :] = mask
    place_ref[2:8, :] = jnp.zeros((6, size), jnp.float32)

    tick_count = jnp.left_shift(jnp.int32(1), LEVELS - 1 - level).astype(jnp.float32)
    offset = phase_ref[...] * (tick_count - STEPS)
    position, velocity = state_ref[0:3, :], state_ref[3:6, :]
    acceleration, jerk = state_ref[6:9, :], state_ref[9:12, :]
    rows = []
    for substep in range(STEPS):
        elapsed = jnp.where(active, 1.0, offset + (substep + 1)) * fine_step
        rows.extend(advance(position, velocity, acceleration, jerk, elapsed))
        if substep == 0:
            rows.append(mass_ref[...] / total_stars)
            rows.append(mask)
    rows.append(jnp.zeros((2, size), jnp.float32))
    rows.extend([acceleration, jerk, jnp.zeros((10, size), jnp.float32)])
    terms = three_terms(jnp.concatenate(rows, axis=0))
    slot = lax.broadcasted_iota(jnp.int32, (size, size), 0).astype(jnp.float32)
    chosen = jnp.where(slot == place, 1.0, 0.0).astype(jnp.bfloat16)
    moved = add_terms(
        lax.dot_general(
            terms, chosen, (((1,), (1,)), ((), ())), preferred_element_type=jnp.float32
        )
    )
    out_ref[...] = moved[0:16]
    across = size // slots
    for k in range(6):
        out_ref[14 + k // across : 15 + k // across, slots * (k % across) : slots * (k % across + 1)] = (
            moved[16 + k : 17 + k, 0:slots]
        )


def pair_terms(source, target, sums):
    sx, sy, sz, su, sv, sw, weight = source
    tx, ty, tz, tu, tv, tw = target
    dx, dy, dz = sx - tx, sy - ty, sz - tz
    du, dv, dw = su - tu, sv - tv, sw - tw
    inverse = lax.rsqrt(dx * dx + dy * dy + (dz * dz + soften_sq))
    inv_sq = inverse * inverse
    pull = weight * inverse * inv_sq
    radial = (dx * du + dy * dv + dz * dw) * (inv_sq * 3.0)
    ax, ay, az, jx, jy, jz = sums
    return (
        ax + pull * dx,
        ay + pull * dy,
        az + pull * dz,
        jx + pull * (du - radial * dx),
        jy + pull * (dv - radial * dy),
        jz + pull * (dw - radial * dz),
    )


def spread_sources(rows, spread_ref, first):
    for c in range(rows.shape[1] // 128):
        for r in range(7):
            spread_ref[r, 8 * (first + c) : 8 * (first + c + 1), :] = jnp.broadcast_to(
                rows[r : r + 1, 128 * c : 128 * (c + 1)], (8, 128)
            )


def spread_targets(rows, spread_ref, first):
    columns = jnp.transpose(rows)
    count = columns.shape[0]
    for r in range(6):
        spread_ref[r, first : first + count, :] = jnp.broadcast_to(
            columns[:, r : r + 1], (count, 128)
        )


def pair_sums(sources_ref, targets_ref, partial_ref, sums_ref, chunks, count, together):
    def reduce(place):
        for g in range(together):
            for q in range(6):
                part = partial_ref[(g * 6 + q) * 8 : (g * 6 + q + 1) * 8, :]
                sums_ref[pl.ds(place + 8 * g, 8), q : q + 1] = jnp.sum(part, axis=1, keepdims=True)

    def body(step, unused):
        base = pl.multiple_of(step * (8 * together), 8)
        reduce(base)
        for g in range(together):
            target = [targets_ref[r, pl.ds(base + 8 * g, 8), :] for r in range(6)]
            sums = (jnp.zeros((8, 128), jnp.float32),) * 6
            for c in range(chunks):
                source = [sources_ref[r, 8 * c : 8 * (c + 1), :] for r in range(7)]
                sums = pair_terms(source, target, sums)
            for q in range(6):
                partial_ref[(g * 6 + q) * 8 : (g * 6 + q + 1) * 8, :] = sums[q]
        return unused

    lax.fori_loop(0, count // (8 * together), body, 0)
    reduce(count)


def advance_stars(slots, shards, *refs):
    sent = refs[:shards]
    state_ref, place_ref, out_ref, sources_ref, targets_ref, partial_ref, sums_ref = refs[shards:]
    size = state_ref.shape[1]
    across = size // slots
    chunks = size // 128
    together = 4
    lead = 8 * together
    for d in range(shards):
        spread_sources(sent[d][0:8, :], sources_ref, d * chunks)
        spread_targets(sent[d][0:8, 0:slots], targets_ref, d * slots)
    partial_ref[...] = jnp.zeros_like(partial_ref)
    pair_sums(
        sources_ref, targets_ref, partial_ref, sums_ref, shards * chunks, shards * slots, together
    )
    own = None
    for d in range(shards):
        forces = jnp.transpose(sums_ref[lead + d * slots : lead + (d + 1) * slots, :])
        first = [
            sent[d][14 + k // across : 15 + k // across, slots * (k % across) : slots * (k % across + 1)]
            for k in range(6)
        ]
        first = jnp.concatenate(first, axis=0)
        position, velocity = corrected(
            first[0:3], first[3:6], sent[d][0:3, 0:slots], sent[d][3:6, 0:slots], forces[0:3], forces[3:6]
        )
        ahead, speed = advance(position, velocity, forces[0:3], forces[3:6], fine_step)
        active = sent[d][7:8, 0:slots] > 0.5
        still = sent[d][8:14, 0:slots]
        again = jnp.where(active, jnp.concatenate([ahead, speed], axis=0), still)
        if d == 0:
            own = jnp.concatenate([again, jnp.zeros((2, slots), jnp.float32)], axis=0)
            before = forces
        later = jnp.concatenate([again, sent[d][8:14, slots:size]], axis=1)
        spread_sources(
            jnp.concatenate([later, sent[d][6:8, :]], axis=0), sources_ref, d * chunks
        )
    spread_targets(own, targets_ref, 0)
    pair_sums(sources_ref, targets_ref, partial_ref, sums_ref, shards * chunks, slots, together)
    second = jnp.transpose(sums_ref[lead : lead + slots, :])
    position, velocity = corrected(
        before[0:3], before[3:6], own[0:3], own[3:6], second[0:3], second[3:6]
    )
    new_rows = jnp.concatenate(
        [position, velocity, second[0:6], jnp.zeros((4, slots), jnp.float32)], axis=0
    )
    slot = lax.broadcasted_iota(jnp.int32, (slots, size), 0).astype(jnp.float32)
    chosen = jnp.where(slot == place_ref[0:1, :], 1.0, 0.0).astype(jnp.bfloat16)
    back = add_terms(jnp.dot(three_terms(new_rows), chosen, preferred_element_type=jnp.float32))
    out_ref[...] = jnp.where(place_ref[1:2, :] > 0.5, back[0:12], state_ref[...])


def direct_per_device(star_state, masses, phases, levels, active_list, active_count):
    del active_count
    size = star_state.shape[1]
    shards = lax.axis_size("src")
    slots = 2 * active_list.shape[0]
    whole = pl.BlockSpec(memory_space=pltpu.VMEM)
    message, place = pl.pallas_call(
        lambda *refs: prepare(slots, size * shards, *refs),
        out_shape=(
            jax.ShapeDtypeStruct((16, size), jnp.float32),
            jax.ShapeDtypeStruct((8, size), jnp.float32),
        ),
        in_specs=[whole] * 4,
        out_specs=(whole, whole),
        compiler_params=pltpu.CompilerParams(vmem_limit_bytes=16 * 2**20),
        name="prepare",
    )(star_state, masses.reshape(1, size), phases.reshape(1, size), levels.reshape(1, size))
    sent = []
    for shift in range(shards - 1, 0, -1):
        pairs = [(d, (d + shift) % shards) for d in range(shards)]
        sent.insert(0, lax.ppermute(message, "src", pairs))
    sent.insert(0, message)
    return pl.pallas_call(
        lambda *refs: advance_stars(slots, shards, *refs),
        out_shape=jax.ShapeDtypeStruct((12, size), jnp.float32),
        in_specs=[whole] * (shards + 2),
        out_specs=whole,
        scratch_shapes=[
            pltpu.VMEM((7, shards * size // 16, 128), jnp.float32),
            pltpu.VMEM((6, shards * slots, 128), jnp.float32),
            pltpu.VMEM((24 * 8, 128), jnp.float32),
            pltpu.VMEM((shards * slots + 32, 8), jnp.float32),
        ],
        compiler_params=pltpu.CompilerParams(vmem_limit_bytes=16 * 2**20),
        name="advance_stars",
    )(*sent, star_state, place)


def solution(mesh):
    in_specs = (
        P(None, ("groups", "src")),
        P(("groups", "src")),
        P(("groups", "src")),
        P(("groups", "src")),
        P(("groups", "src", "act")),
        P(("groups", "src", "act")),
    )
    out_specs = P(None, ("groups", "src"))
    few = mesh.shape["src"] <= MAX_DIRECT
    return jax.shard_map(
        direct_per_device if few else gather_per_device,
        mesh=mesh,
        in_specs=in_specs,
        out_specs=out_specs,
        check_vma=False,
    )
```

```python
import jax
import jax.numpy as jnp
from jax import lax
from jax.experimental import pallas as pl
from jax.experimental.pallas import tpu as pltpu
from jax.sharding import PartitionSpec as P

LEVELS = 5
STEPS = 2
MAX_DIRECT = 8


soften_sq = 0.0004
fine_step = 0.03125


def predict(star_state, elapsed):
    interval = elapsed[None, :]
    position = star_state[0:3] + interval * (
        star_state[3:6] + interval * (0.5 * star_state[6:9] + interval * star_state[9:12] / 6.0)
    )
    velocity = star_state[3:6] + interval * (star_state[6:9] + 0.5 * interval * star_state[9:12])
    return jnp.concatenate([position, velocity], axis=0)


def pair_block(targets, sources):
    delta_pos = sources[0:3, None, :] - targets[0:3, :, None]
    delta_vel = sources[3:6, None, :] - targets[3:6, :, None]
    dist_sq = (
        delta_pos[0] * delta_pos[0]
        + delta_pos[1] * delta_pos[1]
        + delta_pos[2] * delta_pos[2]
        + soften_sq
    )
    inverse = lax.rsqrt(dist_sq)
    inv_sq = inverse * inverse
    weight = sources[6][None, :] * inverse * inv_sq
    radial = (
        (delta_pos[0] * delta_vel[0] + delta_pos[1] * delta_vel[1] + delta_pos[2] * delta_vel[2])
        * inv_sq
        * 3.0
    )
    acceleration = jnp.sum(weight[None] * delta_pos, axis=2)
    jerk_sum = jnp.sum(weight[None] * (delta_vel - radial[None] * delta_pos), axis=2)
    return jnp.concatenate([acceleration, jerk_sum], axis=0)


def over_sources(targets, sources):
    count_src = sources.shape[1]
    width = 512
    blocks = sources.reshape(7, count_src // width, width).transpose(1, 0, 2)

    def accumulate(running, portion):
        return (running + pair_block(targets, portion), None)

    init = jnp.zeros((6, targets.shape[1]), jnp.float32)
    running, unused = lax.scan(accumulate, init, blocks)
    return running


def corrected(acc_old, jerk_old, position, velocity, acc_new, jerk_new):
    snap_term = (-6.0 * (acc_old - acc_new) - fine_step * (4.0 * jerk_old + 2.0 * jerk_new)) / (
        fine_step * fine_step
    )
    crackle = (12.0 * (acc_old - acc_new) + 6.0 * fine_step * (jerk_old + jerk_new)) / (
        fine_step * fine_step * fine_step
    )
    new_position = position + fine_step**4 / 24.0 * snap_term + fine_step**5 / 120.0 * crackle
    new_velocity = velocity + fine_step**3 / 6.0 * snap_term + fine_step**4 / 24.0 * crackle
    return new_position, new_velocity


def correct(old_state, predicted_rows, forces):
    new_position, new_velocity = corrected(
        old_state[6:9],
        old_state[9:12],
        predicted_rows[0:3],
        predicted_rows[3:6],
        forces[0:3],
        forces[3:6],
    )
    return jnp.concatenate([new_position, new_velocity, forces], axis=0)


def gather_per_device(star_state, masses, phases, levels, active_list, active_count):
    shard_size = star_state.shape[1]
    total_stars = shard_size * lax.axis_size("src")
    weights = masses / total_stars
    slot_count = active_list.shape[0]
    live = jnp.arange(slot_count, dtype=jnp.int32) < active_count[0]
    write_index = jnp.where(live, active_list, shard_size)
    tick_count = jnp.left_shift(jnp.int32(1), LEVELS - 1 - levels).astype(jnp.float32)
    state_now = star_state
    for substep in range(STEPS):
        elapsed = (
            jnp.where(levels == LEVELS - 1, 1.0, phases * (tick_count - STEPS) + (substep + 1))
            * fine_step
        )
        predicted = predict(state_now, elapsed)
        sources = jnp.concatenate([predicted, weights[None, :]], axis=0)
        targets = predicted[:, active_list]
        forces = over_sources(targets, lax.all_gather(sources, "src", axis=1, tiled=True))
        new_state = correct(state_now[:, active_list], targets, forces)
        all_new, all_index = (
            lax.all_gather(new_state, "act", axis=1, tiled=True),
            lax.all_gather(write_index, "act", axis=0, tiled=True),
        )
        state_now = state_now.at[:, all_index].set(all_new, mode="drop")
    return state_now


def three_terms(x):
    high = x.astype(jnp.bfloat16)
    rest = x - high.astype(jnp.float32)
    middle = rest.astype(jnp.bfloat16)
    low = (rest - middle.astype(jnp.float32)).astype(jnp.bfloat16)
    return jnp.concatenate([high, middle, low], axis=0)


def add_terms(y):
    rows = y.shape[0] // 3
    return (y[0:rows] + y[rows : 2 * rows]) + y[2 * rows : 3 * rows]


def advance(position, velocity, acceleration, jerk, step):
    ahead = position + step * (velocity + step * (0.5 * acceleration + step * jerk / 6.0))
    speed = velocity + step * (acceleration + 0.5 * step * jerk)
    return ahead, speed


def prepare(slots, total_stars, *refs):
    out_ref, place_ref = refs[4:6]
    copies = [
        pltpu.make_async_copy(far, near, refs[10].at[k])
        for k, (far, near) in enumerate(zip(refs[0:4], refs[6:10]))
    ]
    for copy in copies:
        copy.start()
    for copy in copies:
        copy.wait()
    state_ref, mass_ref, phase_ref, level_ref = refs[6:10]
    size = state_ref.shape[1]
    level = level_ref[...]
    active = level == LEVELS - 1
    mask = jnp.where(active, 1.0, 0.0)
    blocks = size // 128
    grouped = jnp.concatenate(
        [mask[:, 128 * b : 128 * (b + 1)] for b in range(blocks)]
        + [jnp.zeros((16 - blocks, 128), jnp.float32)],
        axis=0,
    ).astype(jnp.bfloat16)
    lane_in = lax.broadcasted_iota(jnp.int32, (128, 256), 0)
    lane_out = lax.broadcasted_iota(jnp.int32, (128, 256), 1)
    counting = jnp.where((lane_in <= lane_out) | (lane_out >= 128), 1.0, 0.0).astype(jnp.bfloat16)
    counts = jnp.dot(grouped, counting, preferred_element_type=jnp.float32)
    so_far = []
    before = jnp.zeros((1, 128), jnp.float32)
    for b in range(blocks):
        so_far.append(counts[b : b + 1, 0:128] + before)
        before = before + counts[b : b + 1, 128:256]
    rank = jnp.concatenate(so_far, axis=1)
    total = jnp.concatenate([before] * blocks, axis=1)
    star = lax.broadcasted_iota(jnp.int32, (1, size), 1).astype(jnp.float32)
    place = jnp.where(active, rank - 1.0, total + star - rank)
    place_ref[0:1, :] = place
    place_ref[1:2, :] = mask
    place_ref[2:8, :] = jnp.zeros((6, size), jnp.float32)

    tick_count = jnp.left_shift(jnp.int32(1), LEVELS - 1 - level).astype(jnp.float32)
    offset = phase_ref[...] * (tick_count - STEPS)
    position, velocity = state_ref[0:3, :], state_ref[3:6, :]
    acceleration, jerk = state_ref[6:9, :], state_ref[9:12, :]
    rows = []
    for substep in range(STEPS):
        elapsed = jnp.where(active, 1.0, offset + (substep + 1)) * fine_step
        rows.extend(advance(position, velocity, acceleration, jerk, elapsed))
        if substep == 0:
            rows.append(mass_ref[...] / total_stars)
            rows.append(mask)
    rows.append(jnp.zeros((2, size), jnp.float32))
    rows.extend([acceleration, jerk, jnp.zeros((10, size), jnp.float32)])
    terms = three_terms(jnp.concatenate(rows, axis=0))
    slot = lax.broadcasted_iota(jnp.int32, (size, size), 0).astype(jnp.float32)
    chosen = jnp.where(slot == place, 1.0, 0.0).astype(jnp.bfloat16)
    moved = add_terms(
        lax.dot_general(
            terms, chosen, (((1,), (1,)), ((), ())), preferred_element_type=jnp.float32
        )
    )
    out_ref[...] = moved[0:16]
    across = size // slots
    for k in range(6):
        out_ref[14 + k // across : 15 + k // across, slots * (k % across) : slots * (k % across + 1)] = (
            moved[16 + k : 17 + k, 0:slots]
        )


def pair_terms(source, target, sums):
    sx, sy, sz, su, sv, sw, weight = source
    tx, ty, tz, tu, tv, tw = target
    dx, dy, dz = sx - tx, sy - ty, sz - tz
    du, dv, dw = su - tu, sv - tv, sw - tw
    inverse = lax.rsqrt(dx * dx + dy * dy + (dz * dz + soften_sq))
    inv_sq = inverse * inverse
    pull = weight * inverse * inv_sq
    radial = (dx * du + dy * dv + dz * dw) * (inv_sq * 3.0)
    ax, ay, az, jx, jy, jz = sums
    return (
        ax + pull * dx,
        ay + pull * dy,
        az + pull * dz,
        jx + pull * (du - radial * dx),
        jy + pull * (dv - radial * dy),
        jz + pull * (dw - radial * dz),
    )


def spread_sources(rows, spread_ref, first):
    for c in range(rows.shape[1] // 128):
        for r in range(7):
            spread_ref[r, 8 * (first + c) : 8 * (first + c + 1), :] = jnp.broadcast_to(
                rows[r : r + 1, 128 * c : 128 * (c + 1)], (8, 128)
            )


def spread_targets(rows, spread_ref, first):
    columns = jnp.transpose(rows)
    count = columns.shape[0]
    for r in range(6):
        spread_ref[r, first : first + count, :] = jnp.broadcast_to(
            columns[:, r : r + 1], (count, 128)
        )


def pair_sums(sources_ref, targets_ref, partial_ref, sums_ref, chunks, count, together):
    def reduce(place):
        for g in range(together):
            for q in range(6):
                part = partial_ref[(g * 6 + q) * 8 : (g * 6 + q + 1) * 8, :]
                sums_ref[pl.ds(place + 8 * g, 8), q : q + 1] = jnp.sum(part, axis=1, keepdims=True)

    def body(step, unused):
        base = pl.multiple_of(step * (8 * together), 8)
        reduce(base)
        for g in range(together):
            target = [targets_ref[r, pl.ds(base + 8 * g, 8), :] for r in range(6)]
            sums = (jnp.zeros((8, 128), jnp.float32),) * 6
            for c in range(chunks):
                source = [sources_ref[r, 8 * c : 8 * (c + 1), :] for r in range(7)]
                sums = pair_terms(source, target, sums)
            for q in range(6):
                partial_ref[(g * 6 + q) * 8 : (g * 6 + q + 1) * 8, :] = sums[q]
        return unused

    lax.fori_loop(0, count // (8 * together), body, 0)
    reduce(count)


def advance_stars(slots, shards, *refs):
    sent = (refs[0],) + refs[shards - 1 : 0 : -1]
    state_ref, place_ref, out_ref, sources_ref, targets_ref, partial_ref, sums_ref = refs[shards:]
    size = state_ref.shape[1]
    across = size // slots
    chunks = size // 128
    together = 4
    lead = 8 * together
    for d in range(shards):
        spread_sources(sent[d][0:8, :], sources_ref, d * chunks)
        spread_targets(sent[d][0:8, 0:slots], targets_ref, d * slots)
    partial_ref[...] = jnp.zeros_like(partial_ref)
    pair_sums(
        sources_ref, targets_ref, partial_ref, sums_ref, shards * chunks, shards * slots, together
    )
    own = None
    for d in range(shards):
        forces = jnp.transpose(sums_ref[lead + d * slots : lead + (d + 1) * slots, :])
        first = [
            sent[d][14 + k // across : 15 + k // across, slots * (k % across) : slots * (k % across + 1)]
            for k in range(6)
        ]
        first = jnp.concatenate(first, axis=0)
        position, velocity = corrected(
            first[0:3], first[3:6], sent[d][0:3, 0:slots], sent[d][3:6, 0:slots], forces[0:3], forces[3:6]
        )
        ahead, speed = advance(position, velocity, forces[0:3], forces[3:6], fine_step)
        active = sent[d][7:8, 0:slots] > 0.5
        still = sent[d][8:14, 0:slots]
        again = jnp.where(active, jnp.concatenate([ahead, speed], axis=0), still)
        if d == 0:
            own = jnp.concatenate([again, jnp.zeros((2, slots), jnp.float32)], axis=0)
            before = forces
        later = jnp.concatenate([again, sent[d][8:14, slots:size]], axis=1)
        spread_sources(
            jnp.concatenate([later, sent[d][6:8, :]], axis=0), sources_ref, d * chunks
        )
    spread_targets(own, targets_ref, 0)
    pair_sums(sources_ref, targets_ref, partial_ref, sums_ref, shards * chunks, slots, together)
    second = jnp.transpose(sums_ref[lead : lead + slots, :])
    position, velocity = corrected(
        before[0:3], before[3:6], own[0:3], own[3:6], second[0:3], second[3:6]
    )
    new_rows = jnp.concatenate(
        [position, velocity, second[0:6], jnp.zeros((4, slots), jnp.float32)], axis=0
    )
    slot = lax.broadcasted_iota(jnp.int32, (slots, size), 0).astype(jnp.float32)
    chosen = jnp.where(slot == place_ref[0:1, :], 1.0, 0.0).astype(jnp.bfloat16)
    back = add_terms(jnp.dot(three_terms(new_rows), chosen, preferred_element_type=jnp.float32))
    out_ref[...] = jnp.where(place_ref[1:2, :] > 0.5, back[0:12], state_ref[...])


def direct_per_device(star_state, masses, phases, levels, active_list, active_count):
    del active_count
    size = star_state.shape[1]
    shards = lax.axis_size("src")
    slots = 2 * active_list.shape[0]
    whole = pl.BlockSpec(memory_space=pltpu.VMEM)
    message, place = pl.pallas_call(
        lambda *refs: prepare(slots, size * shards, *refs),
        out_shape=(
            jax.ShapeDtypeStruct((16, size), jnp.float32),
            jax.ShapeDtypeStruct((8, size), jnp.float32),
        ),
        in_specs=[pl.BlockSpec(memory_space=pltpu.HBM)] * 4,
        out_specs=(whole, whole),
        scratch_shapes=[
            pltpu.VMEM((12, size), jnp.float32),
            pltpu.VMEM((1, size), jnp.float32),
            pltpu.VMEM((1, size), jnp.float32),
            pltpu.VMEM((1, size), jnp.int32),
            pltpu.SemaphoreType.DMA((4,)),
        ],
        compiler_params=pltpu.CompilerParams(vmem_limit_bytes=16 * 2**20),
        name="prepare",
    )(
        *(
            pltpu.with_memory_space_constraint(x, pltpu.HBM)
            for x in (star_state, masses.reshape(1, size), phases.reshape(1, size), levels.reshape(1, size))
        )
    )
    sent = [message]
    for shift in range(shards - 1, 0, -1):
        pairs = [(d, (d + shift) % shards) for d in range(shards)]
        sent.append(lax.ppermute(message, "src", pairs))
    return pl.pallas_call(
        lambda *refs: advance_stars(slots, shards, *refs),
        out_shape=jax.ShapeDtypeStruct((12, size), jnp.float32),
        in_specs=[whole] * (shards + 2),
        out_specs=whole,
        scratch_shapes=[
            pltpu.VMEM((7, shards * size // 16, 128), jnp.float32),
            pltpu.VMEM((6, shards * slots, 128), jnp.float32),
            pltpu.VMEM((24 * 8, 128), jnp.float32),
            pltpu.VMEM((shards * slots + 32, 8), jnp.float32),
        ],
        compiler_params=pltpu.CompilerParams(vmem_limit_bytes=16 * 2**20),
        name="advance_stars",
    )(*sent, star_state, place)


def solution(mesh):
    in_specs = (
        P(None, ("groups", "src")),
        P(("groups", "src")),
        P(("groups", "src")),
        P(("groups", "src")),
        P(("groups", "src", "act")),
        P(("groups", "src", "act")),
    )
    out_specs = P(None, ("groups", "src"))
    few = mesh.shape["src"] <= MAX_DIRECT
    return jax.shard_map(
        direct_per_device if few else gather_per_device,
        mesh=mesh,
        in_specs=in_specs,
        out_specs=out_specs,
        check_vma=False,
    )
```

```python
import functools

import jax
import jax.numpy as jnp
from jax import lax
from jax.experimental import pallas as pl
from jax.experimental.pallas import tpu as pltpu
from jax.sharding import PartitionSpec as P

LEVELS = 5
STEPS = 2
MAX_DIRECT = 8


soften_sq = 0.0004
fine_step = 0.03125


def predict(star_state, elapsed):
    interval = elapsed[None, :]
    position = star_state[0:3] + interval * (
        star_state[3:6] + interval * (0.5 * star_state[6:9] + interval * star_state[9:12] / 6.0)
    )
    velocity = star_state[3:6] + interval * (star_state[6:9] + 0.5 * interval * star_state[9:12])
    return jnp.concatenate([position, velocity], axis=0)


def pair_block(targets, sources):
    delta_pos = sources[0:3, None, :] - targets[0:3, :, None]
    delta_vel = sources[3:6, None, :] - targets[3:6, :, None]
    dist_sq = (
        delta_pos[0] * delta_pos[0]
        + delta_pos[1] * delta_pos[1]
        + delta_pos[2] * delta_pos[2]
        + soften_sq
    )
    inverse = lax.rsqrt(dist_sq)
    inv_sq = inverse * inverse
    weight = sources[6][None, :] * inverse * inv_sq
    radial = (
        (delta_pos[0] * delta_vel[0] + delta_pos[1] * delta_vel[1] + delta_pos[2] * delta_vel[2])
        * inv_sq
        * 3.0
    )
    acceleration = jnp.sum(weight[None] * delta_pos, axis=2)
    jerk_sum = jnp.sum(weight[None] * (delta_vel - radial[None] * delta_pos), axis=2)
    return jnp.concatenate([acceleration, jerk_sum], axis=0)


def over_sources(targets, sources):
    count_src = sources.shape[1]
    width = 512
    blocks = sources.reshape(7, count_src // width, width).transpose(1, 0, 2)

    def accumulate(running, portion):
        return (running + pair_block(targets, portion), None)

    init = jnp.zeros((6, targets.shape[1]), jnp.float32)
    running, unused = lax.scan(accumulate, init, blocks)
    return running


def corrected(acc_old, jerk_old, position, velocity, acc_new, jerk_new):
    snap_term = (-6.0 * (acc_old - acc_new) - fine_step * (4.0 * jerk_old + 2.0 * jerk_new)) / (
        fine_step * fine_step
    )
    crackle = (12.0 * (acc_old - acc_new) + 6.0 * fine_step * (jerk_old + jerk_new)) / (
        fine_step * fine_step * fine_step
    )
    new_position = position + fine_step**4 / 24.0 * snap_term + fine_step**5 / 120.0 * crackle
    new_velocity = velocity + fine_step**3 / 6.0 * snap_term + fine_step**4 / 24.0 * crackle
    return new_position, new_velocity


def correct(old_state, predicted_rows, forces):
    new_position, new_velocity = corrected(
        old_state[6:9],
        old_state[9:12],
        predicted_rows[0:3],
        predicted_rows[3:6],
        forces[0:3],
        forces[3:6],
    )
    return jnp.concatenate([new_position, new_velocity, forces], axis=0)


def gather_per_device(star_state, masses, phases, levels, active_list, active_count):
    shard_size = star_state.shape[1]
    total_stars = shard_size * lax.axis_size("src")
    weights = masses / total_stars
    slot_count = active_list.shape[0]
    live = jnp.arange(slot_count, dtype=jnp.int32) < active_count[0]
    write_index = jnp.where(live, active_list, shard_size)
    tick_count = jnp.left_shift(jnp.int32(1), LEVELS - 1 - levels).astype(jnp.float32)
    state_now = star_state
    for substep in range(STEPS):
        elapsed = (
            jnp.where(levels == LEVELS - 1, 1.0, phases * (tick_count - STEPS) + (substep + 1))
            * fine_step
        )
        predicted = predict(state_now, elapsed)
        sources = jnp.concatenate([predicted, weights[None, :]], axis=0)
        targets = predicted[:, active_list]
        forces = over_sources(targets, lax.all_gather(sources, "src", axis=1, tiled=True))
        new_state = correct(state_now[:, active_list], targets, forces)
        all_new, all_index = (
            lax.all_gather(new_state, "act", axis=1, tiled=True),
            lax.all_gather(write_index, "act", axis=0, tiled=True),
        )
        state_now = state_now.at[:, all_index].set(all_new, mode="drop")
    return state_now


def three_terms(x):
    high = x.astype(jnp.bfloat16)
    rest = x - high.astype(jnp.float32)
    middle = rest.astype(jnp.bfloat16)
    low = (rest - middle.astype(jnp.float32)).astype(jnp.bfloat16)
    return jnp.concatenate([high, middle, low], axis=0)


def add_terms(y):
    rows = y.shape[0] // 3
    return (y[0:rows] + y[rows : 2 * rows]) + y[2 * rows : 3 * rows]


def advance(position, velocity, acceleration, jerk, step):
    ahead = position + step * (velocity + step * (0.5 * acceleration + step * jerk / 6.0))
    speed = velocity + step * (acceleration + 0.5 * step * jerk)
    return ahead, speed


def prepare(slots, total_stars, *refs):
    out_ref, place_ref = refs[4:6]
    copies = [
        pltpu.make_async_copy(far, near, refs[10].at[k])
        for k, (far, near) in enumerate(zip(refs[0:4], refs[6:10]))
    ]
    for copy in copies:
        copy.start()
    for copy in copies:
        copy.wait()
    state_ref, mass_ref, phase_ref, level_ref = refs[6:10]
    size = state_ref.shape[1]
    level = level_ref[...]
    active = level == LEVELS - 1
    mask = jnp.where(active, 1.0, 0.0)
    blocks = size // 128
    grouped = jnp.concatenate(
        [mask[:, 128 * b : 128 * (b + 1)] for b in range(blocks)]
        + [jnp.zeros((16 - blocks, 128), jnp.float32)],
        axis=0,
    ).astype(jnp.bfloat16)
    lane_in = lax.broadcasted_iota(jnp.int32, (128, 256), 0)
    lane_out = lax.broadcasted_iota(jnp.int32, (128, 256), 1)
    counting = jnp.where((lane_in <= lane_out) | (lane_out >= 128), 1.0, 0.0).astype(jnp.bfloat16)
    counts = jnp.dot(grouped, counting, preferred_element_type=jnp.float32)
    so_far = []
    before = jnp.zeros((1, 128), jnp.float32)
    for b in range(blocks):
        so_far.append(counts[b : b + 1, 0:128] + before)
        before = before + counts[b : b + 1, 128:256]
    rank = jnp.concatenate(so_far, axis=1)
    total = jnp.concatenate([before] * blocks, axis=1)
    star = lax.broadcasted_iota(jnp.int32, (1, size), 1).astype(jnp.float32)
    place = jnp.where(active, rank - 1.0, total + star - rank)
    place_ref[0:1, :] = place
    place_ref[1:2, :] = mask
    place_ref[2:8, :] = jnp.zeros((6, size), jnp.float32)

    tick_count = jnp.left_shift(jnp.int32(1), LEVELS - 1 - level).astype(jnp.float32)
    offset = phase_ref[...] * (tick_count - STEPS)
    position, velocity = state_ref[0:3, :], state_ref[3:6, :]
    acceleration, jerk = state_ref[6:9, :], state_ref[9:12, :]
    rows = []
    for substep in range(STEPS):
        elapsed = jnp.where(active, 1.0, offset + (substep + 1)) * fine_step
        rows.extend(advance(position, velocity, acceleration, jerk, elapsed))
        if substep == 0:
            rows.append(mass_ref[...] / total_stars)
            rows.append(mask)
    rows.append(jnp.zeros((2, size), jnp.float32))
    rows.extend([acceleration, jerk, jnp.zeros((10, size), jnp.float32)])
    terms = three_terms(jnp.concatenate(rows, axis=0))
    slot = lax.broadcasted_iota(jnp.int32, (size, size), 0).astype(jnp.float32)
    chosen = jnp.where(slot == place, 1.0, 0.0).astype(jnp.bfloat16)
    moved = add_terms(
        lax.dot_general(
            terms, chosen, (((1,), (1,)), ((), ())), preferred_element_type=jnp.float32
        )
    )
    out_ref[...] = moved[0:16]
    across = size // slots
    for k in range(6):
        out_ref[14 + k // across : 15 + k // across, slots * (k % across) : slots * (k % across + 1)] = (
            moved[16 + k : 17 + k, 0:slots]
        )


def pair_terms(source, target, sums):
    sx, sy, sz, su, sv, sw, weight = source
    tx, ty, tz, tu, tv, tw = target
    dx, dy, dz = sx - tx, sy - ty, sz - tz
    du, dv, dw = su - tu, sv - tv, sw - tw
    inverse = lax.rsqrt(dx * dx + dy * dy + (dz * dz + soften_sq))
    inv_sq = inverse * inverse
    pull = weight * inverse * inv_sq
    radial = (dx * du + dy * dv + dz * dw) * (inv_sq * 3.0)
    ax, ay, az, jx, jy, jz = sums
    return (
        ax + pull * dx,
        ay + pull * dy,
        az + pull * dz,
        jx + pull * (du - radial * dx),
        jy + pull * (dv - radial * dy),
        jz + pull * (dw - radial * dz),
    )


def spread_sources(rows, spread_ref, first):
    for c in range(rows.shape[1] // 128):
        for r in range(7):
            spread_ref[r, 8 * (first + c) : 8 * (first + c + 1), :] = jnp.broadcast_to(
                rows[r : r + 1, 128 * c : 128 * (c + 1)], (8, 128)
            )


def spread_targets(rows, spread_ref):
    columns = jnp.transpose(rows)
    for r in range(6):
        spread_ref[r] = jnp.broadcast_to(columns[:, r : r + 1], (columns.shape[0], 128))


def run_pairs(groups, slots, together, finish, partial_ref, sums_ref):
    lead = 8 * together

    def reduce(place):
        for g in range(together):
            for j in range(len(groups)):
                for q in range(6):
                    row = ((g * len(groups) + j) * 6 + q) * 8
                    sums_ref[pl.ds(j * (slots + lead) + place + 8 * g, 8), q : q + 1] = jnp.sum(
                        partial_ref[row : row + 8, :], axis=1, keepdims=True
                    )

    def body(step, unused):
        base = pl.multiple_of(step * lead, 8)
        if finish:
            reduce(base)
        for g in range(together):
            here = pl.ds(base + 8 * g, 8)
            for j, (target_ref, before_ref, sources, after_ref) in enumerate(groups):
                target = [target_ref[r, here, :] for r in range(6)]
                if before_ref is None:
                    sums = (jnp.zeros((8, 128), jnp.float32),) * 6
                else:
                    sums = tuple(before_ref[q, here, :] for q in range(6))
                for source_ref in sources:
                    for c in range(source_ref.shape[1] // 8):
                        source = [source_ref[r, 8 * c : 8 * (c + 1), :] for r in range(7)]
                        sums = pair_terms(source, target, sums)
                for q in range(6):
                    if finish:
                        row = ((g * len(groups) + j) * 6 + q) * 8
                        partial_ref[row : row + 8, :] = sums[q]
                    else:
                        after_ref[q, here, :] = sums[q]
        return unused

    if finish:
        used = together * len(groups) * 48
        partial_ref[0:used, :] = jnp.zeros((used, 128), jnp.float32)
    lax.fori_loop(0, slots // lead, body, 0)
    if not finish:
        return None
    reduce(slots)
    return [
        jnp.transpose(sums_ref[j * (slots + lead) + lead : (j + 1) * (slots + lead), :])
        for j in range(len(groups))
    ]


def pair_groups(sent, sources, targets, before, after, slots):
    for d in range(len(before), len(targets)):
        fresh = sent[d - len(before)]
        spread_sources(fresh[0:8, :], sources[d], 0)
        spread_targets(fresh[0:8, 0:slots], targets[d])
    groups = []
    for d in range(len(targets)):
        if d < len(before):
            groups.append((targets[d], before[d], sources[len(before) :], after[d]))
        else:
            groups.append((targets[d], None, sources, after[d]))
    return groups


def meet(slots, known, fresh, together, *refs):
    sent, refs = refs[:fresh], refs[fresh:]
    every = known + fresh
    old_sources, old_targets, before = refs[:known], refs[known : 2 * known], refs[2 * known : 3 * known]
    refs = refs[3 * known :]
    new_sources, new_targets, after = refs[:fresh], refs[fresh : 2 * fresh], refs[2 * fresh :]
    groups = pair_groups(
        sent, old_sources + new_sources, old_targets + new_targets, before, after, slots
    )
    run_pairs(groups, slots, together, False, None, None)


def finish(slots, known, fresh, together, *refs):
    every = known + fresh
    sent, refs = refs[:every], refs[every:]
    old_sources, old_targets, before = refs[:known], refs[known : 2 * known], refs[2 * known : 3 * known]
    state_ref, place_ref, out_ref = refs[3 * known : 3 * known + 3]
    refs = refs[3 * known + 3 :]
    new_sources, new_targets = refs[:fresh], refs[fresh : 2 * fresh]
    later_ref, partial_ref, sums_ref = refs[2 * fresh :]
    groups = pair_groups(
        sent[known:],
        old_sources + new_sources,
        old_targets + new_targets,
        before,
        (None,) * every,
        slots,
    )
    size = state_ref.shape[1]
    across = size // slots
    chunks = size // 128
    forces = run_pairs(groups, slots, together, True, partial_ref, sums_ref)
    for d in range(every):
        first = [
            sent[d][14 + k // across : 15 + k // across, slots * (k % across) : slots * (k % across + 1)]
            for k in range(6)
        ]
        first = jnp.concatenate(first, axis=0)
        position, velocity = corrected(
            first[0:3],
            first[3:6],
            sent[d][0:3, 0:slots],
            sent[d][3:6, 0:slots],
            forces[d][0:3],
            forces[d][3:6],
        )
        ahead, speed = advance(position, velocity, forces[d][0:3], forces[d][3:6], fine_step)
        active = sent[d][7:8, 0:slots] > 0.5
        still = sent[d][8:14, 0:slots]
        again = jnp.where(active, jnp.concatenate([ahead, speed], axis=0), still)
        if d == 0:
            own = jnp.concatenate([again, jnp.zeros((2, slots), jnp.float32)], axis=0)
        later = jnp.concatenate([again, sent[d][8:14, slots:size]], axis=1)
        spread_sources(jnp.concatenate([later, sent[d][6:8, :]], axis=0), later_ref, d * chunks)
    target_ref = new_targets[0]
    spread_targets(own, target_ref)
    second = run_pairs(
        [(target_ref, None, (later_ref,), None)], slots, 4, True, partial_ref, sums_ref
    )[0]
    position, velocity = corrected(
        forces[0][0:3], forces[0][3:6], own[0:3], own[3:6], second[0:3], second[3:6]
    )
    new_rows = jnp.concatenate(
        [position, velocity, second[0:6], jnp.zeros((4, slots), jnp.float32)], axis=0
    )
    slot = lax.broadcasted_iota(jnp.int32, (slots, size), 0).astype(jnp.float32)
    chosen = jnp.where(slot == place_ref[0:1, :], 1.0, 0.0).astype(jnp.bfloat16)
    back = add_terms(jnp.dot(three_terms(new_rows), chosen, preferred_element_type=jnp.float32))
    out_ref[...] = jnp.where(place_ref[1:2, :] > 0.5, back[0:12], state_ref[...])


def direct_per_device(star_state, masses, phases, levels, active_list, active_count):
    del active_count
    size = star_state.shape[1]
    shards = lax.axis_size("src")
    slots = 2 * active_list.shape[0]
    whole = pl.BlockSpec(memory_space=pltpu.VMEM)
    message, place = pl.pallas_call(
        lambda *refs: prepare(slots, size * shards, *refs),
        out_shape=(
            jax.ShapeDtypeStruct((16, size), jnp.float32),
            jax.ShapeDtypeStruct((8, size), jnp.float32),
        ),
        in_specs=[pl.BlockSpec(memory_space=pltpu.HBM)] * 4,
        out_specs=(whole, whole),
        scratch_shapes=[
            pltpu.VMEM((12, size), jnp.float32),
            pltpu.VMEM((1, size), jnp.float32),
            pltpu.VMEM((1, size), jnp.float32),
            pltpu.VMEM((1, size), jnp.int32),
            pltpu.SemaphoreType.DMA((4,)),
        ],
        compiler_params=pltpu.CompilerParams(vmem_limit_bytes=16 * 2**20),
        name="prepare",
    )(
        *(
            pltpu.with_memory_space_constraint(x, pltpu.HBM)
            for x in (star_state, masses.reshape(1, size), phases.reshape(1, size), levels.reshape(1, size))
        )
    )
    sent = [message]
    for shift in range(1, shards):
        pairs = [(d, (d + shift) % shards) for d in range(shards)]
        sent.append(lax.ppermute(message, "src", pairs))

    limit = pltpu.CompilerParams(vmem_limit_bytes=16 * 2**20)
    source_shape = jax.ShapeDtypeStruct((7, size // 16, 128), jnp.float32)
    target_shape = jax.ShapeDtypeStruct((6, slots, 128), jnp.float32)
    sources, targets, sums = [], [], []
    known = 0
    stages = [min(2, shards - 1)] + [1] * (shards - 3)
    for fresh in stages:
        every = known + fresh
        outs = pl.pallas_call(
            functools.partial(meet, slots, known, fresh, 2),
            out_shape=[source_shape] * fresh + [target_shape] * (fresh + every),
            in_specs=[whole] * (fresh + 3 * known),
            out_specs=[whole] * (2 * fresh + every),
            compiler_params=limit,
            name=f"meet_{every}",
        )(*sent[known:every], *sources, *targets, *sums)
        sources += outs[:fresh]
        targets += outs[fresh : 2 * fresh]
        sums = list(outs[2 * fresh :])
        known = every
    together = 2
    rows = max(together * shards, 4) * 48
    return pl.pallas_call(
        functools.partial(finish, slots, known, shards - known, together),
        out_shape=jax.ShapeDtypeStruct((12, size), jnp.float32),
        in_specs=[whole] * (shards + 3 * known + 2),
        out_specs=whole,
        scratch_shapes=[pltpu.VMEM(source_shape.shape, jnp.float32)] * (shards - known)
        + [pltpu.VMEM(target_shape.shape, jnp.float32)] * (shards - known)
        + [
            pltpu.VMEM((7, shards * size // 16, 128), jnp.float32),
            pltpu.VMEM((rows, 128), jnp.float32),
            pltpu.VMEM((shards * (slots + 32), 8), jnp.float32),
        ],
        compiler_params=limit,
        name="finish",
    )(*sent, *sources, *targets, *sums, star_state, place)


def solution(mesh):
    in_specs = (
        P(None, ("groups", "src")),
        P(("groups", "src")),
        P(("groups", "src")),
        P(("groups", "src")),
        P(("groups", "src", "act")),
        P(("groups", "src", "act")),
    )
    out_specs = P(None, ("groups", "src"))
    few = 3 <= mesh.shape["src"] <= MAX_DIRECT
    return jax.shard_map(
        direct_per_device if few else gather_per_device,
        mesh=mesh,
        in_specs=in_specs,
        out_specs=out_specs,
        check_vma=False,
    )
```

```python
import functools

import jax
import jax.numpy as jnp
from jax import lax
from jax.experimental import pallas as pl
from jax.experimental.pallas import tpu as pltpu
from jax.sharding import PartitionSpec as P

LEVELS = 5
STEPS = 2
MAX_DIRECT = 8


soften_sq = 0.0004
fine_step = 0.03125


def predict(star_state, elapsed):
    interval = elapsed[None, :]
    position = star_state[0:3] + interval * (
        star_state[3:6] + interval * (0.5 * star_state[6:9] + interval * star_state[9:12] / 6.0)
    )
    velocity = star_state[3:6] + interval * (star_state[6:9] + 0.5 * interval * star_state[9:12])
    return jnp.concatenate([position, velocity], axis=0)


def pair_block(targets, sources):
    delta_pos = sources[0:3, None, :] - targets[0:3, :, None]
    delta_vel = sources[3:6, None, :] - targets[3:6, :, None]
    dist_sq = (
        delta_pos[0] * delta_pos[0]
        + delta_pos[1] * delta_pos[1]
        + delta_pos[2] * delta_pos[2]
        + soften_sq
    )
    inverse = lax.rsqrt(dist_sq)
    inv_sq = inverse * inverse
    weight = sources[6][None, :] * inverse * inv_sq
    radial = (
        (delta_pos[0] * delta_vel[0] + delta_pos[1] * delta_vel[1] + delta_pos[2] * delta_vel[2])
        * inv_sq
        * 3.0
    )
    acceleration = jnp.sum(weight[None] * delta_pos, axis=2)
    jerk_sum = jnp.sum(weight[None] * (delta_vel - radial[None] * delta_pos), axis=2)
    return jnp.concatenate([acceleration, jerk_sum], axis=0)


def over_sources(targets, sources):
    count_src = sources.shape[1]
    width = 512
    blocks = sources.reshape(7, count_src // width, width).transpose(1, 0, 2)

    def accumulate(running, portion):
        return (running + pair_block(targets, portion), None)

    init = jnp.zeros((6, targets.shape[1]), jnp.float32)
    running, unused = lax.scan(accumulate, init, blocks)
    return running


def corrected(acc_old, jerk_old, position, velocity, acc_new, jerk_new):
    snap_term = (-6.0 * (acc_old - acc_new) - fine_step * (4.0 * jerk_old + 2.0 * jerk_new)) / (
        fine_step * fine_step
    )
    crackle = (12.0 * (acc_old - acc_new) + 6.0 * fine_step * (jerk_old + jerk_new)) / (
        fine_step * fine_step * fine_step
    )
    new_position = position + fine_step**4 / 24.0 * snap_term + fine_step**5 / 120.0 * crackle
    new_velocity = velocity + fine_step**3 / 6.0 * snap_term + fine_step**4 / 24.0 * crackle
    return new_position, new_velocity


def correct(old_state, predicted_rows, forces):
    new_position, new_velocity = corrected(
        old_state[6:9],
        old_state[9:12],
        predicted_rows[0:3],
        predicted_rows[3:6],
        forces[0:3],
        forces[3:6],
    )
    return jnp.concatenate([new_position, new_velocity, forces], axis=0)


def gather_per_device(star_state, masses, phases, levels, active_list, active_count):
    shard_size = star_state.shape[1]
    total_stars = shard_size * lax.axis_size("src")
    weights = masses / total_stars
    slot_count = active_list.shape[0]
    live = jnp.arange(slot_count, dtype=jnp.int32) < active_count[0]
    write_index = jnp.where(live, active_list, shard_size)
    tick_count = jnp.left_shift(jnp.int32(1), LEVELS - 1 - levels).astype(jnp.float32)
    state_now = star_state
    for substep in range(STEPS):
        elapsed = (
            jnp.where(levels == LEVELS - 1, 1.0, phases * (tick_count - STEPS) + (substep + 1))
            * fine_step
        )
        predicted = predict(state_now, elapsed)
        sources = jnp.concatenate([predicted, weights[None, :]], axis=0)
        targets = predicted[:, active_list]
        forces = over_sources(targets, lax.all_gather(sources, "src", axis=1, tiled=True))
        new_state = correct(state_now[:, active_list], targets, forces)
        all_new, all_index = (
            lax.all_gather(new_state, "act", axis=1, tiled=True),
            lax.all_gather(write_index, "act", axis=0, tiled=True),
        )
        state_now = state_now.at[:, all_index].set(all_new, mode="drop")
    return state_now


def three_terms(x):
    high = x.astype(jnp.bfloat16)
    rest = x - high.astype(jnp.float32)
    middle = rest.astype(jnp.bfloat16)
    low = (rest - middle.astype(jnp.float32)).astype(jnp.bfloat16)
    return jnp.concatenate([high, middle, low], axis=0)


def add_terms(y):
    rows = y.shape[0] // 3
    return (y[0:rows] + y[rows : 2 * rows]) + y[2 * rows : 3 * rows]


def advance(position, velocity, acceleration, jerk, step):
    ahead = position + step * (velocity + step * (0.5 * acceleration + step * jerk / 6.0))
    speed = velocity + step * (acceleration + 0.5 * step * jerk)
    return ahead, speed


def prepare(slots, total_stars, *refs):
    out_ref, place_ref = refs[4:6]
    copies = [
        pltpu.make_async_copy(far, near, refs[10].at[k])
        for k, (far, near) in enumerate(zip(refs[0:4], refs[6:10]))
    ]
    for copy in copies:
        copy.start()
    for copy in copies:
        copy.wait()
    state_ref, mass_ref, phase_ref, level_ref = refs[6:10]
    size = state_ref.shape[1]
    level = level_ref[...]
    active = level == LEVELS - 1
    mask = jnp.where(active, 1.0, 0.0)
    blocks = size // 128
    grouped = jnp.concatenate(
        [mask[:, 128 * b : 128 * (b + 1)] for b in range(blocks)]
        + [jnp.zeros((16 - blocks, 128), jnp.float32)],
        axis=0,
    ).astype(jnp.bfloat16)
    lane_in = lax.broadcasted_iota(jnp.int32, (128, 256), 0)
    lane_out = lax.broadcasted_iota(jnp.int32, (128, 256), 1)
    counting = jnp.where((lane_in <= lane_out) | (lane_out >= 128), 1.0, 0.0).astype(jnp.bfloat16)
    counts = jnp.dot(grouped, counting, preferred_element_type=jnp.float32)
    so_far = []
    before = jnp.zeros((1, 128), jnp.float32)
    for b in range(blocks):
        so_far.append(counts[b : b + 1, 0:128] + before)
        before = before + counts[b : b + 1, 128:256]
    rank = jnp.concatenate(so_far, axis=1)
    total = jnp.concatenate([before] * blocks, axis=1)
    star = lax.broadcasted_iota(jnp.int32, (1, size), 1).astype(jnp.float32)
    place = jnp.where(active, rank - 1.0, total + star - rank)
    place_ref[0:1, :] = place
    place_ref[1:2, :] = mask
    place_ref[2:8, :] = jnp.zeros((6, size), jnp.float32)

    tick_count = jnp.left_shift(jnp.int32(1), LEVELS - 1 - level).astype(jnp.float32)
    offset = phase_ref[...] * (tick_count - STEPS)
    position, velocity = state_ref[0:3, :], state_ref[3:6, :]
    acceleration, jerk = state_ref[6:9, :], state_ref[9:12, :]
    rows = []
    for substep in range(STEPS):
        elapsed = jnp.where(active, 1.0, offset + (substep + 1)) * fine_step
        rows.extend(advance(position, velocity, acceleration, jerk, elapsed))
        if substep == 0:
            rows.append(mass_ref[...] / total_stars)
            rows.append(mask)
    rows.append(jnp.zeros((2, size), jnp.float32))
    rows.extend([acceleration, jerk, jnp.zeros((10, size), jnp.float32)])
    terms = three_terms(jnp.concatenate(rows, axis=0))
    slot = lax.broadcasted_iota(jnp.int32, (size, size), 0).astype(jnp.float32)
    chosen = jnp.where(slot == place, 1.0, 0.0).astype(jnp.bfloat16)
    moved = add_terms(
        lax.dot_general(
            terms, chosen, (((1,), (1,)), ((), ())), preferred_element_type=jnp.float32
        )
    )
    out_ref[...] = moved[0:16]
    across = size // slots
    for k in range(6):
        out_ref[14 + k // across : 15 + k // across, slots * (k % across) : slots * (k % across + 1)] = (
            moved[16 + k : 17 + k, 0:slots]
        )


def pair_terms(source, target, sums):
    sx, sy, sz, su, sv, sw, weight = source
    tx, ty, tz, tu, tv, tw = target
    dx, dy, dz = sx - tx, sy - ty, sz - tz
    du, dv, dw = su - tu, sv - tv, sw - tw
    inverse = lax.rsqrt(dx * dx + dy * dy + (dz * dz + soften_sq))
    inv_sq = inverse * inverse
    pull = weight * inverse * inv_sq
    radial = (dx * du + dy * dv + dz * dw) * (inv_sq * 3.0)
    ax, ay, az, jx, jy, jz = sums
    return (
        ax + pull * dx,
        ay + pull * dy,
        az + pull * dz,
        jx + pull * (du - radial * dx),
        jy + pull * (dv - radial * dy),
        jz + pull * (dw - radial * dz),
    )


def spread_sources(rows, spread_ref, first):
    for c in range(rows.shape[1] // 128):
        for r in range(7):
            spread_ref[r, 8 * (first + c) : 8 * (first + c + 1), :] = jnp.broadcast_to(
                rows[r : r + 1, 128 * c : 128 * (c + 1)], (8, 128)
            )


def spread_targets(rows, spread_ref):
    columns = jnp.transpose(rows)
    for r in range(6):
        spread_ref[r] = jnp.broadcast_to(columns[:, r : r + 1], (columns.shape[0], 128))


def run_pairs(groups, slots, start, count, together, finish, partial_ref, sums_ref):
    lead = 8 * together

    def reduce(place):
        for g in range(together):
            for j in range(len(groups)):
                for q in range(6):
                    row = ((g * len(groups) + j) * 6 + q) * 8
                    sums_ref[pl.ds(j * (slots + lead) + place + 8 * g, 8), q : q + 1] = jnp.sum(
                        partial_ref[row : row + 8, :], axis=1, keepdims=True
                    )

    def body(step, unused):
        base = pl.multiple_of(start + step * lead, 8)
        if finish:
            reduce(base)
        for g in range(together):
            here = pl.ds(base + 8 * g, 8)
            for j, (target_ref, before_ref, sources, after_ref) in enumerate(groups):
                target = [target_ref[r, here, :] for r in range(6)]
                if before_ref is None:
                    sums = (jnp.zeros((8, 128), jnp.float32),) * 6
                else:
                    sums = tuple(before_ref[q, here, :] for q in range(6))
                for source_ref in sources:
                    for c in range(source_ref.shape[1] // 8):
                        source = [source_ref[r, 8 * c : 8 * (c + 1), :] for r in range(7)]
                        sums = pair_terms(source, target, sums)
                for q in range(6):
                    if finish:
                        row = ((g * len(groups) + j) * 6 + q) * 8
                        partial_ref[row : row + 8, :] = sums[q]
                    else:
                        after_ref[q, here, :] = sums[q]
        return unused

    if finish:
        used = together * len(groups) * 48
        partial_ref[0:used, :] = jnp.zeros((used, 128), jnp.float32)
        if count < slots:
            sums_ref[...] = jnp.zeros_like(sums_ref)
    lax.fori_loop(0, count // lead, body, 0)
    if not finish:
        return None
    reduce(pl.multiple_of(start + count, 8))
    return [
        jnp.transpose(sums_ref[j * (slots + lead) + lead : (j + 1) * (slots + lead), :])
        for j in range(len(groups))
    ]


def pair_groups(sent, sources, targets, before, after, slots):
    for d in range(len(before), len(targets)):
        fresh = sent[d - len(before)]
        spread_sources(fresh[0:8, :], sources[d], 0)
        spread_targets(fresh[0:8, 0:slots], targets[d])
    groups = []
    for d in range(len(targets)):
        if d < len(before):
            groups.append((targets[d], before[d], sources[len(before) :], after[d]))
        else:
            groups.append((targets[d], None, sources, after[d]))
    return groups


def my_slots(slots, split):
    if not split:
        return 0, slots
    half = slots // 2
    return pl.multiple_of(lax.rem(lax.axis_index("act"), 2) * half, 8), half


def meet(slots, split, known, fresh, last, together, *refs):
    every = known + fresh
    sent, refs = refs[:fresh], refs[fresh:]
    old_sources, old_targets, before = refs[:known], refs[known : 2 * known], refs[2 * known : 3 * known]
    refs = refs[3 * known :]
    start, count = my_slots(slots, split)
    if last:
        forces_ref, refs = refs[0], refs[1:]
        after = (None,) * every
        partial_ref, sums_ref = refs[2 * fresh :]
    else:
        after = refs[2 * fresh :]
        partial_ref, sums_ref = None, None
    new_sources, new_targets = refs[:fresh], refs[fresh : 2 * fresh]
    groups = pair_groups(
        sent, old_sources + new_sources, old_targets + new_targets, before, after, slots
    )
    forces = run_pairs(groups, slots, start, count, together, last, partial_ref, sums_ref)
    if last:
        for d in range(every):
            forces_ref[:, d * slots : (d + 1) * slots] = forces[d]


def finish(slots, shards, parts, *refs):
    sent, refs = refs[:shards], refs[shards:]
    shares, refs = refs[:parts], refs[parts:]
    state_ref, place_ref, out_ref, later_ref, target_ref, partial_ref, sums_ref = refs
    size = state_ref.shape[1]
    across = size // slots
    chunks = size // 128
    forces = []
    for d in range(shards):
        share = [s[:, d * slots : (d + 1) * slots] for s in shares]
        forces.append(share[0] + share[1] if parts == 2 else share[0])
    for d in range(shards):
        first = [
            sent[d][14 + k // across : 15 + k // across, slots * (k % across) : slots * (k % across + 1)]
            for k in range(6)
        ]
        first = jnp.concatenate(first, axis=0)
        position, velocity = corrected(
            first[0:3],
            first[3:6],
            sent[d][0:3, 0:slots],
            sent[d][3:6, 0:slots],
            forces[d][0:3],
            forces[d][3:6],
        )
        ahead, speed = advance(position, velocity, forces[d][0:3], forces[d][3:6], fine_step)
        active = sent[d][7:8, 0:slots] > 0.5
        still = sent[d][8:14, 0:slots]
        again = jnp.where(active, jnp.concatenate([ahead, speed], axis=0), still)
        if d == 0:
            own = jnp.concatenate([again, jnp.zeros((2, slots), jnp.float32)], axis=0)
        later = jnp.concatenate([again, sent[d][8:14, slots:size]], axis=1)
        spread_sources(jnp.concatenate([later, sent[d][6:8, :]], axis=0), later_ref, d * chunks)
    spread_targets(own, target_ref)
    second = run_pairs(
        [(target_ref, None, (later_ref,), None)], slots, 0, slots, 4, True, partial_ref, sums_ref
    )[0]
    position, velocity = corrected(
        forces[0][0:3], forces[0][3:6], own[0:3], own[3:6], second[0:3], second[3:6]
    )
    new_rows = jnp.concatenate(
        [position, velocity, second[0:6], jnp.zeros((4, slots), jnp.float32)], axis=0
    )
    slot = lax.broadcasted_iota(jnp.int32, (slots, size), 0).astype(jnp.float32)
    chosen = jnp.where(slot == place_ref[0:1, :], 1.0, 0.0).astype(jnp.bfloat16)
    back = add_terms(jnp.dot(three_terms(new_rows), chosen, preferred_element_type=jnp.float32))
    out_ref[...] = jnp.where(place_ref[1:2, :] > 0.5, back[0:12], state_ref[...])


def direct_per_device(star_state, masses, phases, levels, active_list, active_count):
    del active_count
    size = star_state.shape[1]
    shards = lax.axis_size("src")
    slots = 2 * active_list.shape[0]
    whole = pl.BlockSpec(memory_space=pltpu.VMEM)
    message, place = pl.pallas_call(
        lambda *refs: prepare(slots, size * shards, *refs),
        out_shape=(
            jax.ShapeDtypeStruct((16, size), jnp.float32),
            jax.ShapeDtypeStruct((8, size), jnp.float32),
        ),
        in_specs=[pl.BlockSpec(memory_space=pltpu.HBM)] * 4,
        out_specs=(whole, whole),
        scratch_shapes=[
            pltpu.VMEM((12, size), jnp.float32),
            pltpu.VMEM((1, size), jnp.float32),
            pltpu.VMEM((1, size), jnp.float32),
            pltpu.VMEM((1, size), jnp.int32),
            pltpu.SemaphoreType.DMA((4,)),
        ],
        compiler_params=pltpu.CompilerParams(vmem_limit_bytes=16 * 2**20),
        name="prepare",
    )(
        *(
            pltpu.with_memory_space_constraint(x, pltpu.HBM)
            for x in (star_state, masses.reshape(1, size), phases.reshape(1, size), levels.reshape(1, size))
        )
    )
    sent = [message]
    for shift in range(1, shards):
        pairs = [(d, (d + shift) % shards) for d in range(shards)]
        sent.append(lax.ppermute(message, "src", pairs))

    limit = pltpu.CompilerParams(vmem_limit_bytes=16 * 2**20)
    owners = lax.axis_size("act")
    split = owners % 2 == 0
    source_shape = jax.ShapeDtypeStruct((7, size // 16, 128), jnp.float32)
    target_shape = jax.ShapeDtypeStruct((6, slots, 128), jnp.float32)
    together = 2
    sources, targets, sums = [], [], []
    known = 0
    for fresh in [2] + [1] * (shards - 2):
        every = known + fresh
        last = every == shards
        kept = [source_shape] * fresh + [target_shape] * fresh
        outs = pl.pallas_call(
            functools.partial(meet, slots, split, known, fresh, last, together),
            out_shape=(
                jax.ShapeDtypeStruct((8, shards * slots), jnp.float32)
                if last
                else kept + [target_shape] * every
            ),
            in_specs=[whole] * (fresh + 3 * known),
            out_specs=whole if last else [whole] * (2 * fresh + every),
            scratch_shapes=(
                [pltpu.VMEM(k.shape, k.dtype) for k in kept]
                + [
                    pltpu.VMEM((together * shards * 48, 128), jnp.float32),
                    pltpu.VMEM((shards * (slots + 8 * together), 8), jnp.float32),
                ]
                if last
                else []
            ),
            compiler_params=limit,
            name=f"meet_{every}",
        )(*sent[known:every], *sources, *targets, *sums)
        if last:
            break
        sources += outs[:fresh]
        targets += outs[fresh : 2 * fresh]
        sums = list(outs[2 * fresh :])
        known = every
    shares = [outs]
    if split:
        shares.append(lax.ppermute(outs, "act", [(i, i ^ 1) for i in range(owners)]))
    return pl.pallas_call(
        functools.partial(finish, slots, shards, len(shares)),
        out_shape=jax.ShapeDtypeStruct((12, size), jnp.float32),
        in_specs=[whole] * (shards + len(shares) + 2),
        out_specs=whole,
        scratch_shapes=[
            pltpu.VMEM((7, shards * size // 16, 128), jnp.float32),
            pltpu.VMEM(target_shape.shape, jnp.float32),
            pltpu.VMEM((4 * 48, 128), jnp.float32),
            pltpu.VMEM((slots + 32, 8), jnp.float32),
        ],
        compiler_params=limit,
        name="finish",
    )(*sent, *shares, star_state, place)


def solution(mesh):
    in_specs = (
        P(None, ("groups", "src")),
        P(("groups", "src")),
        P(("groups", "src")),
        P(("groups", "src")),
        P(("groups", "src", "act")),
        P(("groups", "src", "act")),
    )
    out_specs = P(None, ("groups", "src"))
    few = 2 <= mesh.shape["src"] <= MAX_DIRECT
    return jax.shard_map(
        direct_per_device if few else gather_per_device,
        mesh=mesh,
        in_specs=in_specs,
        out_specs=out_specs,
        check_vma=False,
    )
```

```python
import functools

import jax
import jax.numpy as jnp
from jax import lax
from jax.experimental import pallas as pl
from jax.experimental.pallas import tpu as pltpu
from jax.sharding import PartitionSpec as P

LEVELS = 5
STEPS = 2
MAX_DIRECT = 8


soften_sq = 0.0004
fine_step = 0.03125


def predict(star_state, elapsed):
    interval = elapsed[None, :]
    position = star_state[0:3] + interval * (
        star_state[3:6] + interval * (0.5 * star_state[6:9] + interval * star_state[9:12] / 6.0)
    )
    velocity = star_state[3:6] + interval * (star_state[6:9] + 0.5 * interval * star_state[9:12])
    return jnp.concatenate([position, velocity], axis=0)


def pair_block(targets, sources):
    delta_pos = sources[0:3, None, :] - targets[0:3, :, None]
    delta_vel = sources[3:6, None, :] - targets[3:6, :, None]
    dist_sq = (
        delta_pos[0] * delta_pos[0]
        + delta_pos[1] * delta_pos[1]
        + delta_pos[2] * delta_pos[2]
        + soften_sq
    )
    inverse = lax.rsqrt(dist_sq)
    inv_sq = inverse * inverse
    weight = sources[6][None, :] * inverse * inv_sq
    radial = (
        (delta_pos[0] * delta_vel[0] + delta_pos[1] * delta_vel[1] + delta_pos[2] * delta_vel[2])
        * inv_sq
        * 3.0
    )
    acceleration = jnp.sum(weight[None] * delta_pos, axis=2)
    jerk_sum = jnp.sum(weight[None] * (delta_vel - radial[None] * delta_pos), axis=2)
    return jnp.concatenate([acceleration, jerk_sum], axis=0)


def over_sources(targets, sources):
    count_src = sources.shape[1]
    width = 512
    blocks = sources.reshape(7, count_src // width, width).transpose(1, 0, 2)

    def accumulate(running, portion):
        return (running + pair_block(targets, portion), None)

    init = jnp.zeros((6, targets.shape[1]), jnp.float32)
    running, unused = lax.scan(accumulate, init, blocks)
    return running


def corrected(acc_old, jerk_old, position, velocity, acc_new, jerk_new):
    snap_term = (-6.0 * (acc_old - acc_new) - fine_step * (4.0 * jerk_old + 2.0 * jerk_new)) / (
        fine_step * fine_step
    )
    crackle = (12.0 * (acc_old - acc_new) + 6.0 * fine_step * (jerk_old + jerk_new)) / (
        fine_step * fine_step * fine_step
    )
    new_position = position + fine_step**4 / 24.0 * snap_term + fine_step**5 / 120.0 * crackle
    new_velocity = velocity + fine_step**3 / 6.0 * snap_term + fine_step**4 / 24.0 * crackle
    return new_position, new_velocity


def correct(old_state, predicted_rows, forces):
    new_position, new_velocity = corrected(
        old_state[6:9],
        old_state[9:12],
        predicted_rows[0:3],
        predicted_rows[3:6],
        forces[0:3],
        forces[3:6],
    )
    return jnp.concatenate([new_position, new_velocity, forces], axis=0)


def gather_per_device(star_state, masses, phases, levels, active_list, active_count):
    shard_size = star_state.shape[1]
    total_stars = shard_size * lax.axis_size("src")
    weights = masses / total_stars
    slot_count = active_list.shape[0]
    live = jnp.arange(slot_count, dtype=jnp.int32) < active_count[0]
    write_index = jnp.where(live, active_list, shard_size)
    tick_count = jnp.left_shift(jnp.int32(1), LEVELS - 1 - levels).astype(jnp.float32)
    state_now = star_state
    for substep in range(STEPS):
        elapsed = (
            jnp.where(levels == LEVELS - 1, 1.0, phases * (tick_count - STEPS) + (substep + 1))
            * fine_step
        )
        predicted = predict(state_now, elapsed)
        sources = jnp.concatenate([predicted, weights[None, :]], axis=0)
        targets = predicted[:, active_list]
        forces = over_sources(targets, lax.all_gather(sources, "src", axis=1, tiled=True))
        new_state = correct(state_now[:, active_list], targets, forces)
        all_new, all_index = (
            lax.all_gather(new_state, "act", axis=1, tiled=True),
            lax.all_gather(write_index, "act", axis=0, tiled=True),
        )
        state_now = state_now.at[:, all_index].set(all_new, mode="drop")
    return state_now


def three_terms(x):
    high = x.astype(jnp.bfloat16)
    rest = x - high.astype(jnp.float32)
    middle = rest.astype(jnp.bfloat16)
    low = (rest - middle.astype(jnp.float32)).astype(jnp.bfloat16)
    return jnp.concatenate([high, middle, low], axis=0)


def add_terms(y):
    rows = y.shape[0] // 3
    return (y[0:rows] + y[rows : 2 * rows]) + y[2 * rows : 3 * rows]


def advance(position, velocity, acceleration, jerk, step):
    ahead = position + step * (velocity + step * (0.5 * acceleration + step * jerk / 6.0))
    speed = velocity + step * (acceleration + 0.5 * step * jerk)
    return ahead, speed


def prepare(slots, total_stars, *refs):
    out_ref, place_ref = refs[4:6]
    copies = [
        pltpu.make_async_copy(far, near, refs[10].at[k])
        for k, (far, near) in enumerate(zip(refs[0:4], refs[6:10]))
    ]
    for copy in copies:
        copy.start()
    for copy in copies:
        copy.wait()
    state_ref, mass_ref, phase_ref, level_ref = refs[6:10]
    size = state_ref.shape[1]
    level = level_ref[...]
    active = level == LEVELS - 1
    mask = jnp.where(active, 1.0, 0.0)
    blocks = size // 128
    grouped = jnp.concatenate(
        [mask[:, 128 * b : 128 * (b + 1)] for b in range(blocks)]
        + [jnp.zeros((16 - blocks, 128), jnp.float32)],
        axis=0,
    ).astype(jnp.bfloat16)
    lane_in = lax.broadcasted_iota(jnp.int32, (128, 256), 0)
    lane_out = lax.broadcasted_iota(jnp.int32, (128, 256), 1)
    counting = jnp.where((lane_in <= lane_out) | (lane_out >= 128), 1.0, 0.0).astype(jnp.bfloat16)
    counts = jnp.dot(grouped, counting, preferred_element_type=jnp.float32)
    so_far = []
    before = jnp.zeros((1, 128), jnp.float32)
    for b in range(blocks):
        so_far.append(counts[b : b + 1, 0:128] + before)
        before = before + counts[b : b + 1, 128:256]
    rank = jnp.concatenate(so_far, axis=1)
    total = jnp.concatenate([before] * blocks, axis=1)
    star = lax.broadcasted_iota(jnp.int32, (1, size), 1).astype(jnp.float32)
    place = jnp.where(active, rank - 1.0, total + star - rank)
    place_ref[0:1, :] = place
    place_ref[1:2, :] = mask
    place_ref[2:8, :] = jnp.zeros((6, size), jnp.float32)

    tick_count = jnp.left_shift(jnp.int32(1), LEVELS - 1 - level).astype(jnp.float32)
    offset = phase_ref[...] * (tick_count - STEPS)
    position, velocity = state_ref[0:3, :], state_ref[3:6, :]
    acceleration, jerk = state_ref[6:9, :], state_ref[9:12, :]
    rows = []
    for substep in range(STEPS):
        elapsed = jnp.where(active, 1.0, offset + (substep + 1)) * fine_step
        rows.extend(advance(position, velocity, acceleration, jerk, elapsed))
        if substep == 0:
            rows.append(mass_ref[...] / total_stars)
            rows.append(mask)
    rows.append(jnp.zeros((2, size), jnp.float32))
    rows.extend([acceleration, jerk, jnp.zeros((10, size), jnp.float32)])
    terms = three_terms(jnp.concatenate(rows, axis=0))
    slot = lax.broadcasted_iota(jnp.int32, (size, size), 0).astype(jnp.float32)
    chosen = jnp.where(slot == place, 1.0, 0.0).astype(jnp.bfloat16)
    moved = add_terms(
        lax.dot_general(
            terms, chosen, (((1,), (1,)), ((), ())), preferred_element_type=jnp.float32
        )
    )
    out_ref[...] = moved[0:16]
    across = size // slots
    for k in range(6):
        out_ref[14 + k // across : 15 + k // across, slots * (k % across) : slots * (k % across + 1)] = (
            moved[16 + k : 17 + k, 0:slots]
        )


def pair_terms(source, target, sums):
    sx, sy, sz, su, sv, sw, weight = source
    tx, ty, tz, tu, tv, tw = target
    dx, dy, dz = sx - tx, sy - ty, sz - tz
    du, dv, dw = su - tu, sv - tv, sw - tw
    inverse = lax.rsqrt(dx * dx + dy * dy + (dz * dz + soften_sq))
    inv_sq = inverse * inverse
    pull = weight * inverse * inv_sq
    radial = (dx * du + dy * dv + dz * dw) * (inv_sq * 3.0)
    ax, ay, az, jx, jy, jz = sums
    return (
        ax + pull * dx,
        ay + pull * dy,
        az + pull * dz,
        jx + pull * (du - radial * dx),
        jy + pull * (dv - radial * dy),
        jz + pull * (dw - radial * dz),
    )


def spread_sources(rows, spread_ref, first):
    for c in range(rows.shape[1] // 128):
        for r in range(7):
            spread_ref[r, 8 * (first + c) : 8 * (first + c + 1), :] = jnp.broadcast_to(
                rows[r : r + 1, 128 * c : 128 * (c + 1)], (8, 128)
            )


def spread_targets(rows, spread_ref, start, count):
    columns = jnp.transpose(rows)
    for r in range(6):
        spread_ref[r, start : start + count, :] = jnp.broadcast_to(
            columns[start : start + count, r : r + 1], (count, 128)
        )


def run_pairs(groups, slots, start, count, together, finish, partial_ref, sums_ref):
    lead = 8 * together

    def reduce(place):
        for g in range(together):
            for j in range(len(groups)):
                for q in range(6):
                    row = ((g * len(groups) + j) * 6 + q) * 8
                    sums_ref[pl.ds(j * (slots + lead) + place + 8 * g, 8), q : q + 1] = jnp.sum(
                        partial_ref[row : row + 8, :], axis=1, keepdims=True
                    )

    def body(step, unused):
        base = pl.multiple_of(start + step * lead, 8)
        if finish:
            reduce(base)
        for g in range(together):
            here = pl.ds(base + 8 * g, 8)
            for j, (target_ref, columns_ref, before_ref, sources, after_ref) in enumerate(groups):
                if columns_ref is None:
                    target = [target_ref[r, here, :] for r in range(6)]
                else:
                    columns = columns_ref[here, :]
                    target = [jnp.broadcast_to(columns[:, r : r + 1], (8, 128)) for r in range(6)]
                    if target_ref is not None:
                        for r in range(6):
                            target_ref[r, here, :] = target[r]
                if before_ref is None:
                    sums = (jnp.zeros((8, 128), jnp.float32),) * 6
                else:
                    sums = tuple(before_ref[q, here, :] for q in range(6))
                for source_ref in sources:
                    for c in range(source_ref.shape[1] // 8):
                        source = [source_ref[r, 8 * c : 8 * (c + 1), :] for r in range(7)]
                        sums = pair_terms(source, target, sums)
                for q in range(6):
                    if finish:
                        row = ((g * len(groups) + j) * 6 + q) * 8
                        partial_ref[row : row + 8, :] = sums[q]
                    else:
                        after_ref[q, here, :] = sums[q]
        return unused

    if finish:
        used = together * len(groups) * 48
        partial_ref[0:used, :] = jnp.zeros((used, 128), jnp.float32)
        if count < slots:
            sums_ref[...] = jnp.zeros_like(sums_ref)
    lax.fori_loop(0, count // lead, body, 0)
    if not finish:
        return None
    reduce(pl.multiple_of(start + count, 8))
    return [
        jnp.transpose(sums_ref[j * (slots + lead) + lead : (j + 1) * (slots + lead), :])
        for j in range(len(groups))
    ]


def meet(slots, shares, known, fresh, last, together, *refs):
    every = known + fresh
    sent, refs = refs[:fresh], refs[fresh:]
    old_sources, old_targets, before = refs[:known], refs[known : 2 * known], refs[2 * known : 3 * known]
    refs = refs[3 * known :]
    forces_ref = columns_ref = partial_ref = sums_ref = None
    if last:
        forces_ref, refs = refs[0], refs[1:]
        new_sources, refs = refs[:fresh], refs[fresh:]
        new_targets = (None,) * fresh
        after = (None,) * every
        columns_ref, partial_ref, sums_ref = refs
    else:
        new_sources, new_targets, after = refs[:fresh], refs[fresh : 2 * fresh], refs[2 * fresh : 2 * fresh + every]
        columns_ref = refs[2 * fresh + every]
    sources = old_sources + new_sources

    def run(start, count):
        groups = []
        for d in range(known):
            groups.append((old_targets[d], None, before[d], new_sources, after[d]))
        for d in range(fresh):
            spread_sources(sent[d][0:8, :], new_sources[d], 0)
            in_loop = None
            if known:
                in_loop = columns_ref
                columns_ref[...] = jnp.transpose(sent[d][0:8, 0:slots])
            else:
                spread_targets(sent[d][0:8, 0:slots], new_targets[d], start, count)
            groups.append((new_targets[d], in_loop, None, sources, after[known + d]))
        forces = run_pairs(groups, slots, start, count, together, last, partial_ref, sums_ref)
        if last:
            for d in range(every):
                forces_ref[:, d * slots : (d + 1) * slots] = forces[d]

    if len(shares) == 1:
        run(0, slots)
        return
    member = lax.rem(lax.axis_index("act"), len(shares))
    for m in range(len(shares)):

        @pl.when(member == m)
        def _():
            run(sum(shares[:m]), shares[m])


def finish(slots, shards, parts, *refs):
    sent, refs = refs[:shards], refs[shards:]
    shares, refs = refs[:parts], refs[parts:]
    state_ref, place_ref, out_ref, later_ref, target_ref, partial_ref, sums_ref = refs
    size = state_ref.shape[1]
    across = size // slots
    chunks = size // 128
    forces = []
    for d in range(shards):
        share = [s[:, d * slots : (d + 1) * slots] for s in shares]
        forces.append(share[0] + share[1] if parts == 2 else share[0])
    for d in range(shards):
        first = [
            sent[d][14 + k // across : 15 + k // across, slots * (k % across) : slots * (k % across + 1)]
            for k in range(6)
        ]
        first = jnp.concatenate(first, axis=0)
        position, velocity = corrected(
            first[0:3],
            first[3:6],
            sent[d][0:3, 0:slots],
            sent[d][3:6, 0:slots],
            forces[d][0:3],
            forces[d][3:6],
        )
        ahead, speed = advance(position, velocity, forces[d][0:3], forces[d][3:6], fine_step)
        active = sent[d][7:8, 0:slots] > 0.5
        still = sent[d][8:14, 0:slots]
        again = jnp.where(active, jnp.concatenate([ahead, speed], axis=0), still)
        if d == 0:
            own = jnp.concatenate([again, jnp.zeros((2, slots), jnp.float32)], axis=0)
        later = jnp.concatenate([again, sent[d][8:14, slots:size]], axis=1)
        spread_sources(jnp.concatenate([later, sent[d][6:8, :]], axis=0), later_ref, d * chunks)
    spread_targets(own, target_ref, 0, slots)
    second = run_pairs(
        [(target_ref, None, None, (later_ref,), None)], slots, 0, slots, 4, True, partial_ref, sums_ref
    )[0]
    position, velocity = corrected(
        forces[0][0:3], forces[0][3:6], own[0:3], own[3:6], second[0:3], second[3:6]
    )
    new_rows = jnp.concatenate(
        [position, velocity, second[0:6], jnp.zeros((4, slots), jnp.float32)], axis=0
    )
    slot = lax.broadcasted_iota(jnp.int32, (slots, size), 0).astype(jnp.float32)
    chosen = jnp.where(slot == place_ref[0:1, :], 1.0, 0.0).astype(jnp.bfloat16)
    back = add_terms(jnp.dot(three_terms(new_rows), chosen, preferred_element_type=jnp.float32))
    out_ref[...] = jnp.where(place_ref[1:2, :] > 0.5, back[0:12], state_ref[...])


def direct_per_device(star_state, masses, phases, levels, active_list, active_count):
    del active_count
    size = star_state.shape[1]
    shards = lax.axis_size("src")
    slots = 2 * active_list.shape[0]
    whole = pl.BlockSpec(memory_space=pltpu.VMEM)
    message, place = pl.pallas_call(
        lambda *refs: prepare(slots, size * shards, *refs),
        out_shape=(
            jax.ShapeDtypeStruct((16, size), jnp.float32),
            jax.ShapeDtypeStruct((8, size), jnp.float32),
        ),
        in_specs=[pl.BlockSpec(memory_space=pltpu.HBM)] * 4,
        out_specs=(whole, whole),
        scratch_shapes=[
            pltpu.VMEM((12, size), jnp.float32),
            pltpu.VMEM((1, size), jnp.float32),
            pltpu.VMEM((1, size), jnp.float32),
            pltpu.VMEM((1, size), jnp.int32),
            pltpu.SemaphoreType.DMA((4,)),
        ],
        compiler_params=pltpu.CompilerParams(vmem_limit_bytes=16 * 2**20),
        name="prepare",
    )(
        *(
            pltpu.with_memory_space_constraint(x, pltpu.HBM)
            for x in (star_state, masses.reshape(1, size), phases.reshape(1, size), levels.reshape(1, size))
        )
    )
    sent = [message]
    for shift in range(1, shards):
        pairs = [(d, (d + shift) % shards) for d in range(shards)]
        sent.append(lax.ppermute(message, "src", pairs))

    limit = pltpu.CompilerParams(vmem_limit_bytes=16 * 2**20)
    owners = lax.axis_size("act")
    shares = (slots,)
    if owners % 2 == 0:
        first_share = slots * 3 // 8 // 16 * 16
        shares = (first_share, slots - first_share)
    source_shape = jax.ShapeDtypeStruct((7, size // 16, 128), jnp.float32)
    target_shape = jax.ShapeDtypeStruct((6, slots, 128), jnp.float32)
    together = 2
    sources, targets, sums = [], [], []
    known = 0
    for fresh in [2] + [1] * (shards - 2):
        every = known + fresh
        last = every == shards
        kept = [source_shape] * fresh + [target_shape] * fresh
        outs = pl.pallas_call(
            functools.partial(meet, slots, shares, known, fresh, last, together),
            out_shape=(
                jax.ShapeDtypeStruct((8, shards * slots), jnp.float32)
                if last
                else kept + [target_shape] * every
            ),
            in_specs=[whole] * (fresh + 3 * known),
            out_specs=whole if last else [whole] * (2 * fresh + every),
            scratch_shapes=(
                [
                    pltpu.VMEM(source_shape.shape, jnp.float32),
                    pltpu.VMEM((slots, 8), jnp.float32),
                    pltpu.VMEM((together * shards * 48, 128), jnp.float32),
                    pltpu.VMEM((shards * (slots + 8 * together), 8), jnp.float32),
                ]
                if last
                else [pltpu.VMEM((slots, 8), jnp.float32)]
            ),
            compiler_params=limit,
            name=f"meet_{every}",
        )(*sent[known:every], *sources, *targets, *sums)
        if last:
            break
        sources += outs[:fresh]
        targets += outs[fresh : 2 * fresh]
        sums = list(outs[2 * fresh :])
        known = every
    parts = [outs]
    if len(shares) == 2:
        parts.append(lax.ppermute(outs, "act", [(i, i ^ 1) for i in range(owners)]))
    return pl.pallas_call(
        functools.partial(finish, slots, shards, len(parts)),
        out_shape=jax.ShapeDtypeStruct((12, size), jnp.float32),
        in_specs=[whole] * (shards + len(parts) + 2),
        out_specs=whole,
        scratch_shapes=[
            pltpu.VMEM((7, shards * size // 16, 128), jnp.float32),
            pltpu.VMEM(target_shape.shape, jnp.float32),
            pltpu.VMEM((4 * 48, 128), jnp.float32),
            pltpu.VMEM((slots + 32, 8), jnp.float32),
        ],
        compiler_params=limit,
        name="finish",
    )(*sent, *parts, star_state, place)


def solution(mesh):
    in_specs = (
        P(None, ("groups", "src")),
        P(("groups", "src")),
        P(("groups", "src")),
        P(("groups", "src")),
        P(("groups", "src", "act")),
        P(("groups", "src", "act")),
    )
    out_specs = P(None, ("groups", "src"))
    few = 3 <= mesh.shape["src"] <= MAX_DIRECT
    return jax.shard_map(
        direct_per_device if few else gather_per_device,
        mesh=mesh,
        in_specs=in_specs,
        out_specs=out_specs,
        check_vma=False,
    )
```

```python
import functools

import jax
import jax.numpy as jnp
from jax import lax
from jax.experimental import pallas as pl
from jax.experimental.pallas import tpu as pltpu
from jax.sharding import PartitionSpec as P

LEVELS = 5
STEPS = 2
MAX_DIRECT = 8


soften_sq = 0.0004
fine_step = 0.03125


def predict(star_state, elapsed):
    interval = elapsed[None, :]
    position = star_state[0:3] + interval * (
        star_state[3:6] + interval * (0.5 * star_state[6:9] + interval * star_state[9:12] / 6.0)
    )
    velocity = star_state[3:6] + interval * (star_state[6:9] + 0.5 * interval * star_state[9:12])
    return jnp.concatenate([position, velocity], axis=0)


def pair_block(targets, sources):
    delta_pos = sources[0:3, None, :] - targets[0:3, :, None]
    delta_vel = sources[3:6, None, :] - targets[3:6, :, None]
    dist_sq = (
        delta_pos[0] * delta_pos[0]
        + delta_pos[1] * delta_pos[1]
        + delta_pos[2] * delta_pos[2]
        + soften_sq
    )
    inverse = lax.rsqrt(dist_sq)
    inv_sq = inverse * inverse
    weight = sources[6][None, :] * inverse * inv_sq
    radial = (
        (delta_pos[0] * delta_vel[0] + delta_pos[1] * delta_vel[1] + delta_pos[2] * delta_vel[2])
        * inv_sq
        * 3.0
    )
    acceleration = jnp.sum(weight[None] * delta_pos, axis=2)
    jerk_sum = jnp.sum(weight[None] * (delta_vel - radial[None] * delta_pos), axis=2)
    return jnp.concatenate([acceleration, jerk_sum], axis=0)


def over_sources(targets, sources):
    count_src = sources.shape[1]
    width = 512
    blocks = sources.reshape(7, count_src // width, width).transpose(1, 0, 2)

    def accumulate(running, portion):
        return (running + pair_block(targets, portion), None)

    init = jnp.zeros((6, targets.shape[1]), jnp.float32)
    running, unused = lax.scan(accumulate, init, blocks)
    return running


def corrected(acc_old, jerk_old, position, velocity, acc_new, jerk_new):
    snap_term = (-6.0 * (acc_old - acc_new) - fine_step * (4.0 * jerk_old + 2.0 * jerk_new)) / (
        fine_step * fine_step
    )
    crackle = (12.0 * (acc_old - acc_new) + 6.0 * fine_step * (jerk_old + jerk_new)) / (
        fine_step * fine_step * fine_step
    )
    new_position = position + fine_step**4 / 24.0 * snap_term + fine_step**5 / 120.0 * crackle
    new_velocity = velocity + fine_step**3 / 6.0 * snap_term + fine_step**4 / 24.0 * crackle
    return new_position, new_velocity


def correct(old_state, predicted_rows, forces):
    new_position, new_velocity = corrected(
        old_state[6:9],
        old_state[9:12],
        predicted_rows[0:3],
        predicted_rows[3:6],
        forces[0:3],
        forces[3:6],
    )
    return jnp.concatenate([new_position, new_velocity, forces], axis=0)


def gather_per_device(star_state, masses, phases, levels, active_list, active_count):
    shard_size = star_state.shape[1]
    total_stars = shard_size * lax.axis_size("src")
    weights = masses / total_stars
    slot_count = active_list.shape[0]
    live = jnp.arange(slot_count, dtype=jnp.int32) < active_count[0]
    write_index = jnp.where(live, active_list, shard_size)
    tick_count = jnp.left_shift(jnp.int32(1), LEVELS - 1 - levels).astype(jnp.float32)
    state_now = star_state
    for substep in range(STEPS):
        elapsed = (
            jnp.where(levels == LEVELS - 1, 1.0, phases * (tick_count - STEPS) + (substep + 1))
            * fine_step
        )
        predicted = predict(state_now, elapsed)
        sources = jnp.concatenate([predicted, weights[None, :]], axis=0)
        targets = predicted[:, active_list]
        forces = over_sources(targets, lax.all_gather(sources, "src", axis=1, tiled=True))
        new_state = correct(state_now[:, active_list], targets, forces)
        all_new, all_index = (
            lax.all_gather(new_state, "act", axis=1, tiled=True),
            lax.all_gather(write_index, "act", axis=0, tiled=True),
        )
        state_now = state_now.at[:, all_index].set(all_new, mode="drop")
    return state_now


def three_terms(x):
    high = x.astype(jnp.bfloat16)
    rest = x - high.astype(jnp.float32)
    middle = rest.astype(jnp.bfloat16)
    low = (rest - middle.astype(jnp.float32)).astype(jnp.bfloat16)
    return jnp.concatenate([high, middle, low], axis=0)


def add_terms(y):
    rows = y.shape[0] // 3
    return (y[0:rows] + y[rows : 2 * rows]) + y[2 * rows : 3 * rows]


def advance(position, velocity, acceleration, jerk, step):
    ahead = position + step * (velocity + step * (0.5 * acceleration + step * jerk / 6.0))
    speed = velocity + step * (acceleration + 0.5 * step * jerk)
    return ahead, speed


def prepare(slots, total_stars, *refs):
    out_ref, place_ref = refs[4:6]
    copies = [
        pltpu.make_async_copy(far, near, refs[10].at[k])
        for k, (far, near) in enumerate(zip(refs[0:4], refs[6:10]))
    ]
    for copy in copies:
        copy.start()
    for copy in copies:
        copy.wait()
    state_ref, mass_ref, phase_ref, level_ref = refs[6:10]
    size = state_ref.shape[1]
    level = level_ref[...]
    active = level == LEVELS - 1
    mask = jnp.where(active, 1.0, 0.0)
    blocks = size // 128
    grouped = jnp.concatenate(
        [mask[:, 128 * b : 128 * (b + 1)] for b in range(blocks)]
        + [jnp.zeros((16 - blocks, 128), jnp.float32)],
        axis=0,
    ).astype(jnp.bfloat16)
    lane_in = lax.broadcasted_iota(jnp.int32, (128, 256), 0)
    lane_out = lax.broadcasted_iota(jnp.int32, (128, 256), 1)
    counting = jnp.where((lane_in <= lane_out) | (lane_out >= 128), 1.0, 0.0).astype(jnp.bfloat16)
    counts = jnp.dot(grouped, counting, preferred_element_type=jnp.float32)
    so_far = []
    before = jnp.zeros((1, 128), jnp.float32)
    for b in range(blocks):
        so_far.append(counts[b : b + 1, 0:128] + before)
        before = before + counts[b : b + 1, 128:256]
    rank = jnp.concatenate(so_far, axis=1)
    total = jnp.concatenate([before] * blocks, axis=1)
    star = lax.broadcasted_iota(jnp.int32, (1, size), 1).astype(jnp.float32)
    place = jnp.where(active, rank - 1.0, total + star - rank)
    place_ref[0:1, :] = place
    place_ref[1:2, :] = mask
    place_ref[2:8, :] = jnp.zeros((6, size), jnp.float32)

    tick_count = jnp.left_shift(jnp.int32(1), LEVELS - 1 - level).astype(jnp.float32)
    offset = phase_ref[...] * (tick_count - STEPS)
    position, velocity = state_ref[0:3, :], state_ref[3:6, :]
    acceleration, jerk = state_ref[6:9, :], state_ref[9:12, :]
    rows = []
    for substep in range(STEPS):
        elapsed = jnp.where(active, 1.0, offset + (substep + 1)) * fine_step
        rows.extend(advance(position, velocity, acceleration, jerk, elapsed))
        if substep == 0:
            rows.append(mass_ref[...] / total_stars)
            rows.append(mask)
    rows.append(jnp.zeros((2, size), jnp.float32))
    rows.extend([acceleration, jerk, jnp.zeros((10, size), jnp.float32)])
    terms = three_terms(jnp.concatenate(rows, axis=0))
    slot = lax.broadcasted_iota(jnp.int32, (size, size), 0).astype(jnp.float32)
    chosen = jnp.where(slot == place, 1.0, 0.0).astype(jnp.bfloat16)
    moved = add_terms(
        lax.dot_general(
            terms, chosen, (((1,), (1,)), ((), ())), preferred_element_type=jnp.float32
        )
    )
    out_ref[...] = moved[0:16]
    across = size // slots
    for k in range(6):
        out_ref[14 + k // across : 15 + k // across, slots * (k % across) : slots * (k % across + 1)] = (
            moved[16 + k : 17 + k, 0:slots]
        )


def pair_terms(source, target, sums):
    sx, sy, sz, su, sv, sw, weight = source
    tx, ty, tz, tu, tv, tw = target
    dx, dy, dz = sx - tx, sy - ty, sz - tz
    du, dv, dw = su - tu, sv - tv, sw - tw
    inverse = lax.rsqrt(dx * dx + dy * dy + (dz * dz + soften_sq))
    inv_sq = inverse * inverse
    pull = weight * inverse * inv_sq
    radial = (dx * du + dy * dv + dz * dw) * (inv_sq * 3.0)
    ax, ay, az, jx, jy, jz = sums
    return (
        ax + pull * dx,
        ay + pull * dy,
        az + pull * dz,
        jx + pull * (du - radial * dx),
        jy + pull * (dv - radial * dy),
        jz + pull * (dw - radial * dz),
    )


def spread_sources(rows, spread_ref, first):
    for c in range(rows.shape[1] // 128):
        for r in range(7):
            spread_ref[r, 8 * (first + c) : 8 * (first + c + 1), :] = jnp.broadcast_to(
                rows[r : r + 1, 128 * c : 128 * (c + 1)], (8, 128)
            )


def spread_targets(rows, spread_ref, start, count):
    columns = jnp.transpose(rows)
    for r in range(6):
        spread_ref[r, start : start + count, :] = jnp.broadcast_to(
            columns[start : start + count, r : r + 1], (count, 128)
        )


def run_pairs(groups, slots, start, count, together, finish, partial_ref, sums_ref):
    lead = 8 * together

    def reduce(place):
        for g in range(together):
            for j in range(len(groups)):
                for q in range(6):
                    row = ((g * len(groups) + j) * 6 + q) * 8
                    sums_ref[pl.ds(j * (slots + lead) + place + 8 * g, 8), q : q + 1] = jnp.sum(
                        partial_ref[row : row + 8, :], axis=1, keepdims=True
                    )

    def body(step, unused):
        base = pl.multiple_of(start + step * lead, 8)
        if finish:
            reduce(base)
        for g in range(together):
            here = pl.ds(base + 8 * g, 8)
            for j, (target_ref, columns_ref, before_ref, sources, after_ref) in enumerate(groups):
                if columns_ref is None:
                    target = [target_ref[r, here, :] for r in range(6)]
                else:
                    columns = columns_ref[here, :]
                    target = [jnp.broadcast_to(columns[:, r : r + 1], (8, 128)) for r in range(6)]
                    if target_ref is not None:
                        for r in range(6):
                            target_ref[r, here, :] = target[r]
                if before_ref is None:
                    sums = (jnp.zeros((8, 128), jnp.float32),) * 6
                else:
                    sums = tuple(before_ref[q, here, :] for q in range(6))
                for source_ref in sources:
                    for c in range(source_ref.shape[1] // 8):
                        source = [source_ref[r, 8 * c : 8 * (c + 1), :] for r in range(7)]
                        sums = pair_terms(source, target, sums)
                for q in range(6):
                    if finish:
                        row = ((g * len(groups) + j) * 6 + q) * 8
                        partial_ref[row : row + 8, :] = sums[q]
                    else:
                        after_ref[q, here, :] = sums[q]
        return unused

    if finish:
        used = together * len(groups) * 48
        partial_ref[0:used, :] = jnp.zeros((used, 128), jnp.float32)
        if count < slots:
            sums_ref[...] = jnp.zeros_like(sums_ref)
    lax.fori_loop(0, count // lead, body, 0)
    if not finish:
        return None
    reduce(pl.multiple_of(start + count, 8))
    return [
        jnp.transpose(sums_ref[j * (slots + lead) + lead : (j + 1) * (slots + lead), :])
        for j in range(len(groups))
    ]


def meet(slots, shares, known, fresh, last, *refs):
    every = known + fresh
    sent, refs = refs[:fresh], refs[fresh:]
    old_sources, old_targets, before = refs[:known], refs[known : 2 * known], refs[2 * known : 3 * known]
    refs = refs[3 * known :]
    own_ref = forces_ref = own_partial = own_sums = partial_ref = sums_ref = None
    if last:
        own_ref, forces_ref, refs = refs[0], refs[1], refs[2:]
        new_sources, refs = refs[:fresh], refs[fresh:]
        new_targets = (None,) * fresh
        after = (None,) * every
        columns_ref, own_partial, own_sums, partial_ref, sums_ref = refs
    else:
        new_sources, new_targets, after = refs[:fresh], refs[fresh : 2 * fresh], refs[2 * fresh : 2 * fresh + every]
        columns_ref = refs[2 * fresh + every]
    sources = old_sources + new_sources

    for d in range(fresh):
        spread_sources(sent[d][0:8, :], new_sources[d], 0)
        if known + d > 0:
            columns_ref[...] = jnp.transpose(sent[d][0:8, 0:slots])
    if known == 0:
        spread_targets(sent[0][0:8, 0:slots], new_targets[0], 0, slots)
        own = (new_targets[0], None, None, sources, after[0])
    else:
        own = (old_targets[0], None, before[0], new_sources, after[0])
    own = run_pairs([own], slots, 0, slots, 4 if known == 0 else 8, last, own_partial, own_sums)
    if last:
        own_ref[...] = own[0]

    def run(start, count):
        groups = []
        for d in range(1, known):
            groups.append((old_targets[d], None, before[d], new_sources, after[d]))
        for d in range(max(known, 1), every):
            groups.append((new_targets[d - known], columns_ref, None, sources, after[d]))
        together = 4 if known == 0 else 2
        forces = run_pairs(groups, slots, start, count, together, last, partial_ref, sums_ref)
        if last:
            for d in range(1, every):
                forces_ref[:, (d - 1) * slots : d * slots] = forces[d - 1]

    if len(shares) == 1:
        run(0, slots)
        return
    member = lax.rem(lax.axis_index("act"), len(shares))
    for m in range(len(shares)):

        @pl.when(member == m)
        def _():
            run(sum(shares[:m]), shares[m])


def first_step(slots, sent, forces):
    size = sent.shape[1]
    across = size // slots
    old = [
        sent[14 + k // across : 15 + k // across, slots * (k % across) : slots * (k % across + 1)]
        for k in range(6)
    ]
    old = jnp.concatenate(old, axis=0)
    position, velocity = corrected(
        old[0:3], old[3:6], sent[0:3, 0:slots], sent[3:6, 0:slots], forces[0:3], forces[3:6]
    )
    ahead, speed = advance(position, velocity, forces[0:3], forces[3:6], fine_step)
    active = sent[7:8, 0:slots] > 0.5
    return jnp.where(active, jnp.concatenate([ahead, speed], axis=0), sent[8:14, 0:slots])


def meet_still(slots, shards, *refs):
    sent, refs = refs[:shards], refs[shards:]
    own_ref, again_ref, target_ref, after_ref, still_ref = refs
    size = sent[0].shape[1]
    chunks = size // 128
    first = slots // 128
    again = first_step(slots, sent[0], own_ref[...])
    again = jnp.concatenate([again, jnp.zeros((2, slots), jnp.float32)], axis=0)
    again_ref[...] = again
    for d in range(shards):
        rows = jnp.concatenate([sent[d][8:14, slots:size], sent[d][6:8, slots:size]], axis=0)
        spread_sources(rows, still_ref, d * (chunks - first))
    spread_targets(again, target_ref, 0, slots)
    run_pairs(
        [(target_ref, None, None, (still_ref,), after_ref)], slots, 0, slots, 4, False, None, None
    )


def finish(slots, shards, parts, *refs):
    sent, refs = refs[:shards], refs[shards:]
    shares, refs = refs[:parts], refs[parts:]
    own_ref, again_ref, target_ref, before_ref, state_ref, place_ref, out_ref = refs[:7]
    later_ref, partial_ref, sums_ref = refs[7:]
    size = state_ref.shape[1]
    first = slots // 128
    own = again_ref[...]
    for d in range(shards):
        if d == 0:
            again = own[0:6]
        else:
            share = [s[:, (d - 1) * slots : d * slots] for s in shares]
            again = first_step(
                slots, sent[d], share[0] + share[1] if parts == 2 else share[0]
            )
        rows = jnp.concatenate([again, sent[d][6:8, 0:slots]], axis=0)
        spread_sources(rows, later_ref, d * first)
    second = run_pairs(
        [(target_ref, None, before_ref, (later_ref,), None)],
        slots,
        0,
        slots,
        8,
        True,
        partial_ref,
        sums_ref,
    )[0]
    before = own_ref[...]
    position, velocity = corrected(
        before[0:3], before[3:6], own[0:3], own[3:6], second[0:3], second[3:6]
    )
    new_rows = jnp.concatenate(
        [position, velocity, second[0:6], jnp.zeros((4, slots), jnp.float32)], axis=0
    )
    slot = lax.broadcasted_iota(jnp.int32, (slots, size), 0).astype(jnp.float32)
    chosen = jnp.where(slot == place_ref[0:1, :], 1.0, 0.0).astype(jnp.bfloat16)
    back = add_terms(jnp.dot(three_terms(new_rows), chosen, preferred_element_type=jnp.float32))
    out_ref[...] = jnp.where(place_ref[1:2, :] > 0.5, back[0:12], state_ref[...])


def direct_per_device(star_state, masses, phases, levels, active_list, active_count):
    del active_count
    size = star_state.shape[1]
    shards = lax.axis_size("src")
    slots = 2 * active_list.shape[0]
    whole = pl.BlockSpec(memory_space=pltpu.VMEM)
    message, place = pl.pallas_call(
        lambda *refs: prepare(slots, size * shards, *refs),
        out_shape=(
            jax.ShapeDtypeStruct((16, size), jnp.float32),
            jax.ShapeDtypeStruct((8, size), jnp.float32),
        ),
        in_specs=[pl.BlockSpec(memory_space=pltpu.HBM)] * 4,
        out_specs=(whole, whole),
        scratch_shapes=[
            pltpu.VMEM((12, size), jnp.float32),
            pltpu.VMEM((1, size), jnp.float32),
            pltpu.VMEM((1, size), jnp.float32),
            pltpu.VMEM((1, size), jnp.int32),
            pltpu.SemaphoreType.DMA((4,)),
        ],
        compiler_params=pltpu.CompilerParams(vmem_limit_bytes=16 * 2**20),
        name="prepare",
    )(
        *(
            pltpu.with_memory_space_constraint(x, pltpu.HBM)
            for x in (star_state, masses.reshape(1, size), phases.reshape(1, size), levels.reshape(1, size))
        )
    )
    sent = [message]
    for shift in range(1, shards):
        pairs = [(d, (d + shift) % shards) for d in range(shards)]
        sent.append(lax.ppermute(message, "src", pairs))

    limit = pltpu.CompilerParams(vmem_limit_bytes=16 * 2**20)
    owners = lax.axis_size("act")
    shares = (slots,)
    if owners % 2 == 0:
        first_share = slots // 4 // 32 * 32
        shares = (first_share, slots - first_share)
    source_shape = jax.ShapeDtypeStruct((7, size // 16, 128), jnp.float32)
    target_shape = jax.ShapeDtypeStruct((6, slots, 128), jnp.float32)
    own_shape = jax.ShapeDtypeStruct((8, slots), jnp.float32)
    columns = pltpu.VMEM((slots, 8), jnp.float32)
    sources, targets, sums = [], [], []
    known = 0
    for fresh in [2] + [1] * (shards - 2):
        every = known + fresh
        last = every == shards
        if last:
            out_shape = (own_shape, jax.ShapeDtypeStruct((8, (shards - 1) * slots), jnp.float32))
            scratch = [
                pltpu.VMEM(source_shape.shape, jnp.float32),
                columns,
                pltpu.VMEM((8 * 48, 128), jnp.float32),
                pltpu.VMEM((slots + 64, 8), jnp.float32),
                pltpu.VMEM((2 * (shards - 1) * 48, 128), jnp.float32),
                pltpu.VMEM(((shards - 1) * (slots + 16), 8), jnp.float32),
            ]
        else:
            out_shape = [source_shape] * fresh + [target_shape] * (fresh + every)
            scratch = [columns]
        outs = pl.pallas_call(
            functools.partial(meet, slots, shares, known, fresh, last),
            out_shape=out_shape,
            in_specs=[whole] * (fresh + 3 * known),
            out_specs=(whole, whole) if last else [whole] * (2 * fresh + every),
            scratch_shapes=scratch,
            compiler_params=limit,
            name=f"meet_{every}",
        )(*sent[known:every], *sources, *targets, *sums)
        if last:
            break
        sources += outs[:fresh]
        targets += outs[fresh : 2 * fresh]
        sums = list(outs[2 * fresh :])
        known = every
    own, part = outs
    parts = [part]
    if len(shares) == 2:
        parts.append(lax.ppermute(part, "act", [(i, i ^ 1) for i in range(owners)]))
    first = slots // 128
    again, target, still = pl.pallas_call(
        functools.partial(meet_still, slots, shards),
        out_shape=(own_shape, target_shape, target_shape),
        in_specs=[whole] * (shards + 1),
        out_specs=(whole,) * 3,
        scratch_shapes=[pltpu.VMEM((7, shards * (size // 128 - first) * 8, 128), jnp.float32)],
        compiler_params=limit,
        name="meet_still",
    )(*sent, own)
    return pl.pallas_call(
        functools.partial(finish, slots, shards, len(parts)),
        out_shape=jax.ShapeDtypeStruct((12, size), jnp.float32),
        in_specs=[whole] * (shards + len(parts) + 6),
        out_specs=whole,
        scratch_shapes=[
            pltpu.VMEM((7, shards * first * 8, 128), jnp.float32),
            pltpu.VMEM((8 * 48, 128), jnp.float32),
            pltpu.VMEM((slots + 64, 8), jnp.float32),
        ],
        compiler_params=limit,
        name="finish",
    )(*sent, *parts, own, again, target, still, star_state, place)


def solution(mesh):
    in_specs = (
        P(None, ("groups", "src")),
        P(("groups", "src")),
        P(("groups", "src")),
        P(("groups", "src")),
        P(("groups", "src", "act")),
        P(("groups", "src", "act")),
    )
    out_specs = P(None, ("groups", "src"))
    few = 3 <= mesh.shape["src"] <= MAX_DIRECT
    return jax.shard_map(
        direct_per_device if few else gather_per_device,
        mesh=mesh,
        in_specs=in_specs,
        out_specs=out_specs,
        check_vma=False,
    )
```

```python
import functools

import jax
import jax.numpy as jnp
from jax import lax
from jax.experimental import pallas as pl
from jax.experimental.pallas import tpu as pltpu
from jax.sharding import PartitionSpec as P

LEVELS = 5
STEPS = 2
MAX_DIRECT = 8


soften_sq = 0.0004
fine_step = 0.03125


def predict(star_state, elapsed):
    interval = elapsed[None, :]
    position = star_state[0:3] + interval * (
        star_state[3:6] + interval * (0.5 * star_state[6:9] + interval * star_state[9:12] / 6.0)
    )
    velocity = star_state[3:6] + interval * (star_state[6:9] + 0.5 * interval * star_state[9:12])
    return jnp.concatenate([position, velocity], axis=0)


def pair_block(targets, sources):
    delta_pos = sources[0:3, None, :] - targets[0:3, :, None]
    delta_vel = sources[3:6, None, :] - targets[3:6, :, None]
    dist_sq = (
        delta_pos[0] * delta_pos[0]
        + delta_pos[1] * delta_pos[1]
        + delta_pos[2] * delta_pos[2]
        + soften_sq
    )
    inverse = lax.rsqrt(dist_sq)
    inv_sq = inverse * inverse
    weight = sources[6][None, :] * inverse * inv_sq
    radial = (
        (delta_pos[0] * delta_vel[0] + delta_pos[1] * delta_vel[1] + delta_pos[2] * delta_vel[2])
        * inv_sq
        * 3.0
    )
    acceleration = jnp.sum(weight[None] * delta_pos, axis=2)
    jerk_sum = jnp.sum(weight[None] * (delta_vel - radial[None] * delta_pos), axis=2)
    return jnp.concatenate([acceleration, jerk_sum], axis=0)


def over_sources(targets, sources):
    count_src = sources.shape[1]
    width = 512
    blocks = sources.reshape(7, count_src // width, width).transpose(1, 0, 2)

    def accumulate(running, portion):
        return (running + pair_block(targets, portion), None)

    init = jnp.zeros((6, targets.shape[1]), jnp.float32)
    running, unused = lax.scan(accumulate, init, blocks)
    return running


def corrected(acc_old, jerk_old, position, velocity, acc_new, jerk_new):
    snap_term = (-6.0 * (acc_old - acc_new) - fine_step * (4.0 * jerk_old + 2.0 * jerk_new)) / (
        fine_step * fine_step
    )
    crackle = (12.0 * (acc_old - acc_new) + 6.0 * fine_step * (jerk_old + jerk_new)) / (
        fine_step * fine_step * fine_step
    )
    new_position = position + fine_step**4 / 24.0 * snap_term + fine_step**5 / 120.0 * crackle
    new_velocity = velocity + fine_step**3 / 6.0 * snap_term + fine_step**4 / 24.0 * crackle
    return new_position, new_velocity


def correct(old_state, predicted_rows, forces):
    new_position, new_velocity = corrected(
        old_state[6:9],
        old_state[9:12],
        predicted_rows[0:3],
        predicted_rows[3:6],
        forces[0:3],
        forces[3:6],
    )
    return jnp.concatenate([new_position, new_velocity, forces], axis=0)


def gather_per_device(star_state, masses, phases, levels, active_list, active_count):
    shard_size = star_state.shape[1]
    total_stars = shard_size * lax.axis_size("src")
    weights = masses / total_stars
    slot_count = active_list.shape[0]
    live = jnp.arange(slot_count, dtype=jnp.int32) < active_count[0]
    write_index = jnp.where(live, active_list, shard_size)
    tick_count = jnp.left_shift(jnp.int32(1), LEVELS - 1 - levels).astype(jnp.float32)
    state_now = star_state
    for substep in range(STEPS):
        elapsed = (
            jnp.where(levels == LEVELS - 1, 1.0, phases * (tick_count - STEPS) + (substep + 1))
            * fine_step
        )
        predicted = predict(state_now, elapsed)
        sources = jnp.concatenate([predicted, weights[None, :]], axis=0)
        targets = predicted[:, active_list]
        forces = over_sources(targets, lax.all_gather(sources, "src", axis=1, tiled=True))
        new_state = correct(state_now[:, active_list], targets, forces)
        all_new, all_index = (
            lax.all_gather(new_state, "act", axis=1, tiled=True),
            lax.all_gather(write_index, "act", axis=0, tiled=True),
        )
        state_now = state_now.at[:, all_index].set(all_new, mode="drop")
    return state_now


def three_terms(x):
    high = x.astype(jnp.bfloat16)
    rest = x - high.astype(jnp.float32)
    middle = rest.astype(jnp.bfloat16)
    low = (rest - middle.astype(jnp.float32)).astype(jnp.bfloat16)
    return jnp.concatenate([high, middle, low], axis=0)


def add_terms(y):
    rows = y.shape[0] // 3
    return (y[0:rows] + y[rows : 2 * rows]) + y[2 * rows : 3 * rows]


def advance(position, velocity, acceleration, jerk, step):
    ahead = position + step * (velocity + step * (0.5 * acceleration + step * jerk / 6.0))
    speed = velocity + step * (acceleration + 0.5 * step * jerk)
    return ahead, speed


def prepare(slots, total_stars, *refs):
    out_ref, place_ref = refs[4:6]
    copies = [
        pltpu.make_async_copy(far, near, refs[10].at[k])
        for k, (far, near) in enumerate(zip(refs[0:4], refs[6:10]))
    ]
    for copy in copies:
        copy.start()
    for copy in copies:
        copy.wait()
    state_ref, mass_ref, phase_ref, level_ref = refs[6:10]
    size = state_ref.shape[1]
    level = level_ref[...]
    active = level == LEVELS - 1
    mask = jnp.where(active, 1.0, 0.0)
    blocks = size // 128
    grouped = jnp.concatenate(
        [mask[:, 128 * b : 128 * (b + 1)] for b in range(blocks)]
        + [jnp.zeros((16 - blocks, 128), jnp.float32)],
        axis=0,
    ).astype(jnp.bfloat16)
    lane_in = lax.broadcasted_iota(jnp.int32, (128, 256), 0)
    lane_out = lax.broadcasted_iota(jnp.int32, (128, 256), 1)
    counting = jnp.where((lane_in <= lane_out) | (lane_out >= 128), 1.0, 0.0).astype(jnp.bfloat16)
    counts = jnp.dot(grouped, counting, preferred_element_type=jnp.float32)
    so_far = []
    before = jnp.zeros((1, 128), jnp.float32)
    for b in range(blocks):
        so_far.append(counts[b : b + 1, 0:128] + before)
        before = before + counts[b : b + 1, 128:256]
    rank = jnp.concatenate(so_far, axis=1)
    total = jnp.concatenate([before] * blocks, axis=1)
    star = lax.broadcasted_iota(jnp.int32, (1, size), 1).astype(jnp.float32)
    place = jnp.where(active, rank - 1.0, total + star - rank)
    place_ref[0:1, :] = place
    place_ref[1:2, :] = mask
    place_ref[2:8, :] = jnp.zeros((6, size), jnp.float32)

    tick_count = jnp.left_shift(jnp.int32(1), LEVELS - 1 - level).astype(jnp.float32)
    offset = phase_ref[...] * (tick_count - STEPS)
    position, velocity = state_ref[0:3, :], state_ref[3:6, :]
    acceleration, jerk = state_ref[6:9, :], state_ref[9:12, :]
    rows = []
    for substep in range(STEPS):
        elapsed = jnp.where(active, 1.0, offset + (substep + 1)) * fine_step
        rows.extend(advance(position, velocity, acceleration, jerk, elapsed))
        if substep == 0:
            rows.append(mass_ref[...] / total_stars)
            rows.append(mask)
    rows.append(jnp.zeros((2, size), jnp.float32))
    rows.extend([acceleration, jerk, jnp.zeros((10, size), jnp.float32)])
    terms = three_terms(jnp.concatenate(rows, axis=0))
    slot = lax.broadcasted_iota(jnp.int32, (size, size), 0).astype(jnp.float32)
    chosen = jnp.where(slot == place, 1.0, 0.0).astype(jnp.bfloat16)
    moved = add_terms(
        lax.dot_general(
            terms, chosen, (((1,), (1,)), ((), ())), preferred_element_type=jnp.float32
        )
    )
    out_ref[...] = moved[0:16]
    across = size // slots
    for k in range(6):
        out_ref[14 + k // across : 15 + k // across, slots * (k % across) : slots * (k % across + 1)] = (
            moved[16 + k : 17 + k, 0:slots]
        )


def pair_terms(source, target, sums):
    sx, sy, sz, su, sv, sw, weight = source
    tx, ty, tz, tu, tv, tw = target
    dx, dy, dz = sx - tx, sy - ty, sz - tz
    du, dv, dw = su - tu, sv - tv, sw - tw
    inverse = lax.rsqrt(dx * dx + dy * dy + (dz * dz + soften_sq))
    inv_sq = inverse * inverse
    pull = weight * inverse * inv_sq
    radial = (dx * du + dy * dv + dz * dw) * (inv_sq * 3.0)
    ax, ay, az, jx, jy, jz = sums
    return (
        ax + pull * dx,
        ay + pull * dy,
        az + pull * dz,
        jx + pull * (du - radial * dx),
        jy + pull * (dv - radial * dy),
        jz + pull * (dw - radial * dz),
    )


def spread_sources(rows, spread_ref, first):
    for c in range(rows.shape[1] // 128):
        for r in range(7):
            spread_ref[r, 8 * (first + c) : 8 * (first + c + 1), :] = jnp.broadcast_to(
                rows[r : r + 1, 128 * c : 128 * (c + 1)], (8, 128)
            )


def spread_targets(rows, spread_ref, start, count):
    columns = jnp.transpose(rows)
    for r in range(6):
        spread_ref[r, start : start + count, :] = jnp.broadcast_to(
            columns[start : start + count, r : r + 1], (count, 128)
        )


def run_pairs(groups, slots, start, count, together, finish, partial_ref, sums_ref):
    lead = 8 * together
    stride = slots + lead

    def reduce(place, many):
        for g in range(many):
            for j in range(len(groups)):
                for q in range(6):
                    row = ((g * len(groups) + j) * 6 + q) * 8
                    sums_ref[pl.ds(j * stride + place + 8 * g, 8), q : q + 1] = jnp.sum(
                        partial_ref[row : row + 8, :], axis=1, keepdims=True
                    )

    def block(base, many):
        for g in range(many):
            here = pl.ds(base + 8 * g, 8)
            for j, (target_ref, columns_ref, before_ref, sources, after_ref) in enumerate(groups):
                if columns_ref is None:
                    target = [target_ref[r, here, :] for r in range(6)]
                else:
                    columns = columns_ref[here, :]
                    target = [jnp.broadcast_to(columns[:, r : r + 1], (8, 128)) for r in range(6)]
                    if target_ref is not None:
                        for r in range(6):
                            target_ref[r, here, :] = target[r]
                if before_ref is None:
                    sums = (jnp.zeros((8, 128), jnp.float32),) * 6
                else:
                    sums = tuple(before_ref[q, here, :] for q in range(6))
                for source_ref in sources:
                    for c in range(source_ref.shape[1] // 8):
                        source = [source_ref[r, 8 * c : 8 * (c + 1), :] for r in range(7)]
                        sums = pair_terms(source, target, sums)
                for q in range(6):
                    if finish:
                        row = ((g * len(groups) + j) * 6 + q) * 8
                        partial_ref[row : row + 8, :] = sums[q]
                    else:
                        after_ref[q, here, :] = sums[q]

    def body(step, unused):
        base = pl.multiple_of(start + step * lead, 8)
        if finish:
            reduce(base, together)
        block(base, together)
        return unused

    if finish:
        used = together * len(groups) * 48
        partial_ref[0:used, :] = jnp.zeros((used, 128), jnp.float32)
        if count < slots:
            sums_ref[...] = jnp.zeros_like(sums_ref)
    steps = count // lead
    lax.fori_loop(0, steps, body, 0)
    rest = (count - steps * lead) // 8
    end = start + steps * lead
    if finish:
        reduce(end, together)
    if rest:
        block(end, rest)
        if finish:
            reduce(end + lead, rest)
    if not finish:
        return None
    return [
        jnp.transpose(sums_ref[j * stride + lead : (j + 1) * stride, :])
        for j in range(len(groups))
    ]


def meet(slots, shares, known, fresh, last, *refs):
    every = known + fresh
    sent, refs = refs[:fresh], refs[fresh:]
    old_sources, old_targets, before = refs[:known], refs[known : 2 * known], refs[2 * known : 3 * known]
    refs = refs[3 * known :]
    own_ref = forces_ref = own_partial = own_sums = partial_ref = sums_ref = None
    if last:
        own_ref, forces_ref, refs = refs[0], refs[1], refs[2:]
        new_sources, refs = refs[:fresh], refs[fresh:]
        new_targets = (None,) * fresh
        after = (None,) * every
        columns_ref, own_partial, own_sums, partial_ref, sums_ref = refs
    else:
        new_sources, new_targets, after = refs[:fresh], refs[fresh : 2 * fresh], refs[2 * fresh : 2 * fresh + every]
        columns_ref = refs[2 * fresh + every]
    sources = old_sources + new_sources

    for d in range(fresh):
        spread_sources(sent[d][0:8, :], new_sources[d], 0)
        if known + d > 0:
            columns_ref[...] = jnp.transpose(sent[d][0:8, 0:slots])
    if known == 0:
        spread_targets(sent[0][0:8, 0:slots], new_targets[0], 0, slots)
        own = (new_targets[0], None, None, sources, after[0])
    else:
        own = (old_targets[0], None, before[0], new_sources, after[0])
    own = run_pairs([own], slots, 0, slots, 4 if known == 0 else 8, last, own_partial, own_sums)
    if last:
        own_ref[...] = own[0]

    def run(start, count):
        groups = []
        for d in range(1, known):
            groups.append((old_targets[d], None, before[d], new_sources, after[d]))
        for d in range(max(known, 1), every):
            groups.append((new_targets[d - known], columns_ref, None, sources, after[d]))
        together = 4 if known == 0 else 2
        forces = run_pairs(groups, slots, start, count, together, last, partial_ref, sums_ref)
        if last:
            for d in range(1, every):
                forces_ref[:, (d - 1) * slots : d * slots] = forces[d - 1]

    if len(shares) == 1:
        run(0, slots)
        return
    member = lax.rem(lax.axis_index("act"), len(shares))
    for m in range(len(shares)):

        @pl.when(member == m)
        def _():
            run(sum(shares[:m]), shares[m])


def first_step(slots, sent, forces):
    size = sent.shape[1]
    across = size // slots
    old = [
        sent[14 + k // across : 15 + k // across, slots * (k % across) : slots * (k % across + 1)]
        for k in range(6)
    ]
    old = jnp.concatenate(old, axis=0)
    position, velocity = corrected(
        old[0:3], old[3:6], sent[0:3, 0:slots], sent[3:6, 0:slots], forces[0:3], forces[3:6]
    )
    ahead, speed = advance(position, velocity, forces[0:3], forces[3:6], fine_step)
    active = sent[7:8, 0:slots] > 0.5
    return jnp.where(active, jnp.concatenate([ahead, speed], axis=0), sent[8:14, 0:slots])


def meet_still(slots, shards, *refs):
    sent, refs = refs[:shards], refs[shards:]
    own_ref, again_ref, target_ref, after_ref, still_ref = refs
    size = sent[0].shape[1]
    chunks = size // 128
    first = slots // 128
    again = first_step(slots, sent[0], own_ref[...])
    again = jnp.concatenate([again, jnp.zeros((2, slots), jnp.float32)], axis=0)
    again_ref[...] = again
    for d in range(shards):
        rows = jnp.concatenate([sent[d][8:14, slots:size], sent[d][6:8, slots:size]], axis=0)
        spread_sources(rows, still_ref, d * (chunks - first))
    spread_targets(again, target_ref, 0, slots)
    run_pairs(
        [(target_ref, None, None, (still_ref,), after_ref)], slots, 0, slots, 4, False, None, None
    )


def finish(slots, shards, parts, *refs):
    sent, refs = refs[:shards], refs[shards:]
    shares, refs = refs[:parts], refs[parts:]
    own_ref, again_ref, target_ref, before_ref, state_ref, place_ref, out_ref = refs[:7]
    later_ref, partial_ref, sums_ref = refs[7:]
    size = state_ref.shape[1]
    first = slots // 128
    own = again_ref[...]
    for d in range(shards):
        if d == 0:
            again = own[0:6]
        else:
            share = [s[:, (d - 1) * slots : d * slots] for s in shares]
            again = first_step(
                slots, sent[d], share[0] + share[1] if parts == 2 else share[0]
            )
        rows = jnp.concatenate([again, sent[d][6:8, 0:slots]], axis=0)
        spread_sources(rows, later_ref, d * first)
    second = run_pairs(
        [(target_ref, None, before_ref, (later_ref,), None)],
        slots,
        0,
        slots,
        8,
        True,
        partial_ref,
        sums_ref,
    )[0]
    before = own_ref[...]
    position, velocity = corrected(
        before[0:3], before[3:6], own[0:3], own[3:6], second[0:3], second[3:6]
    )
    new_rows = jnp.concatenate(
        [position, velocity, second[0:6], jnp.zeros((4, slots), jnp.float32)], axis=0
    )
    slot = lax.broadcasted_iota(jnp.int32, (slots, size), 0).astype(jnp.float32)
    chosen = jnp.where(slot == place_ref[0:1, :], 1.0, 0.0).astype(jnp.bfloat16)
    back = add_terms(jnp.dot(three_terms(new_rows), chosen, preferred_element_type=jnp.float32))
    out_ref[...] = jnp.where(place_ref[1:2, :] > 0.5, back[0:12], state_ref[...])


def direct_per_device(star_state, masses, phases, levels, active_list, active_count):
    del active_count
    size = star_state.shape[1]
    shards = lax.axis_size("src")
    slots = 2 * active_list.shape[0]
    whole = pl.BlockSpec(memory_space=pltpu.VMEM)
    message, place = pl.pallas_call(
        lambda *refs: prepare(slots, size * shards, *refs),
        out_shape=(
            jax.ShapeDtypeStruct((16, size), jnp.float32),
            jax.ShapeDtypeStruct((8, size), jnp.float32),
        ),
        in_specs=[pl.BlockSpec(memory_space=pltpu.HBM)] * 4,
        out_specs=(whole, whole),
        scratch_shapes=[
            pltpu.VMEM((12, size), jnp.float32),
            pltpu.VMEM((1, size), jnp.float32),
            pltpu.VMEM((1, size), jnp.float32),
            pltpu.VMEM((1, size), jnp.int32),
            pltpu.SemaphoreType.DMA((4,)),
        ],
        compiler_params=pltpu.CompilerParams(vmem_limit_bytes=16 * 2**20),
        name="prepare",
    )(
        *(
            pltpu.with_memory_space_constraint(x, pltpu.HBM)
            for x in (star_state, masses.reshape(1, size), phases.reshape(1, size), levels.reshape(1, size))
        )
    )
    sent = [message]
    for shift in range(1, shards):
        pairs = [(d, (d + shift) % shards) for d in range(shards)]
        sent.append(lax.ppermute(message, "src", pairs))

    limit = pltpu.CompilerParams(vmem_limit_bytes=16 * 2**20)
    owners = lax.axis_size("act")
    shares = (slots,)
    if owners % 2 == 0:
        first_share = slots * 7 // 16 // 8 * 8
        shares = (first_share, slots - first_share)
    source_shape = jax.ShapeDtypeStruct((7, size // 16, 128), jnp.float32)
    target_shape = jax.ShapeDtypeStruct((6, slots, 128), jnp.float32)
    own_shape = jax.ShapeDtypeStruct((8, slots), jnp.float32)
    columns = pltpu.VMEM((slots, 8), jnp.float32)
    sources, targets, sums = [], [], []
    known = 0
    for fresh in [2] + [1] * (shards - 2):
        every = known + fresh
        last = every == shards
        if last:
            out_shape = (own_shape, jax.ShapeDtypeStruct((8, (shards - 1) * slots), jnp.float32))
            scratch = [
                pltpu.VMEM(source_shape.shape, jnp.float32),
                columns,
                pltpu.VMEM((8 * 48, 128), jnp.float32),
                pltpu.VMEM((slots + 64, 8), jnp.float32),
                pltpu.VMEM((2 * (shards - 1) * 48, 128), jnp.float32),
                pltpu.VMEM(((shards - 1) * (slots + 16), 8), jnp.float32),
            ]
        else:
            out_shape = [source_shape] * fresh + [target_shape] * (fresh + every)
            scratch = [columns]
        outs = pl.pallas_call(
            functools.partial(meet, slots, shares, known, fresh, last),
            out_shape=out_shape,
            in_specs=[whole] * (fresh + 3 * known),
            out_specs=(whole, whole) if last else [whole] * (2 * fresh + every),
            scratch_shapes=scratch,
            compiler_params=limit,
            name=f"meet_{every}",
        )(*sent[known:every], *sources, *targets, *sums)
        if last:
            break
        sources += outs[:fresh]
        targets += outs[fresh : 2 * fresh]
        sums = list(outs[2 * fresh :])
        known = every
    own, part = outs
    parts = [part]
    if len(shares) == 2:
        parts.append(lax.ppermute(part, "act", [(i, i ^ 1) for i in range(owners)]))
    first = slots // 128
    again, target, still = pl.pallas_call(
        functools.partial(meet_still, slots, shards),
        out_shape=(own_shape, target_shape, target_shape),
        in_specs=[whole] * (shards + 1),
        out_specs=(whole,) * 3,
        scratch_shapes=[pltpu.VMEM((7, shards * (size // 128 - first) * 8, 128), jnp.float32)],
        compiler_params=limit,
        name="meet_still",
    )(*sent, own)
    return pl.pallas_call(
        functools.partial(finish, slots, shards, len(parts)),
        out_shape=jax.ShapeDtypeStruct((12, size), jnp.float32),
        in_specs=[whole] * (shards + len(parts) + 6),
        out_specs=whole,
        scratch_shapes=[
            pltpu.VMEM((7, shards * first * 8, 128), jnp.float32),
            pltpu.VMEM((8 * 48, 128), jnp.float32),
            pltpu.VMEM((slots + 64, 8), jnp.float32),
        ],
        compiler_params=limit,
        name="finish",
    )(*sent, *parts, own, again, target, still, star_state, place)


def solution(mesh):
    in_specs = (
        P(None, ("groups", "src")),
        P(("groups", "src")),
        P(("groups", "src")),
        P(("groups", "src")),
        P(("groups", "src", "act")),
        P(("groups", "src", "act")),
    )
    out_specs = P(None, ("groups", "src"))
    few = 3 <= mesh.shape["src"] <= MAX_DIRECT
    return jax.shard_map(
        direct_per_device if few else gather_per_device,
        mesh=mesh,
        in_specs=in_specs,
        out_specs=out_specs,
        check_vma=False,
    )
```

```python
import functools

import jax
import jax.numpy as jnp
from jax import lax
from jax.experimental import pallas as pl
from jax.experimental.pallas import tpu as pltpu
from jax.sharding import PartitionSpec as P

LEVELS = 5
STEPS = 2
MAX_DIRECT = 8


soften_sq = 0.0004
fine_step = 0.03125


def predict(star_state, elapsed):
    interval = elapsed[None, :]
    position = star_state[0:3] + interval * (
        star_state[3:6] + interval * (0.5 * star_state[6:9] + interval * star_state[9:12] / 6.0)
    )
    velocity = star_state[3:6] + interval * (star_state[6:9] + 0.5 * interval * star_state[9:12])
    return jnp.concatenate([position, velocity], axis=0)


def pair_block(targets, sources):
    delta_pos = sources[0:3, None, :] - targets[0:3, :, None]
    delta_vel = sources[3:6, None, :] - targets[3:6, :, None]
    dist_sq = (
        delta_pos[0] * delta_pos[0]
        + delta_pos[1] * delta_pos[1]
        + delta_pos[2] * delta_pos[2]
        + soften_sq
    )
    inverse = lax.rsqrt(dist_sq)
    inv_sq = inverse * inverse
    weight = sources[6][None, :] * inverse * inv_sq
    radial = (
        (delta_pos[0] * delta_vel[0] + delta_pos[1] * delta_vel[1] + delta_pos[2] * delta_vel[2])
        * inv_sq
        * 3.0
    )
    acceleration = jnp.sum(weight[None] * delta_pos, axis=2)
    jerk_sum = jnp.sum(weight[None] * (delta_vel - radial[None] * delta_pos), axis=2)
    return jnp.concatenate([acceleration, jerk_sum], axis=0)


def over_sources(targets, sources):
    count_src = sources.shape[1]
    width = 512
    blocks = sources.reshape(7, count_src // width, width).transpose(1, 0, 2)

    def accumulate(running, portion):
        return (running + pair_block(targets, portion), None)

    init = jnp.zeros((6, targets.shape[1]), jnp.float32)
    running, unused = lax.scan(accumulate, init, blocks)
    return running


def corrected(acc_old, jerk_old, position, velocity, acc_new, jerk_new):
    snap_term = (-6.0 * (acc_old - acc_new) - fine_step * (4.0 * jerk_old + 2.0 * jerk_new)) / (
        fine_step * fine_step
    )
    crackle = (12.0 * (acc_old - acc_new) + 6.0 * fine_step * (jerk_old + jerk_new)) / (
        fine_step * fine_step * fine_step
    )
    new_position = position + fine_step**4 / 24.0 * snap_term + fine_step**5 / 120.0 * crackle
    new_velocity = velocity + fine_step**3 / 6.0 * snap_term + fine_step**4 / 24.0 * crackle
    return new_position, new_velocity


def correct(old_state, predicted_rows, forces):
    new_position, new_velocity = corrected(
        old_state[6:9],
        old_state[9:12],
        predicted_rows[0:3],
        predicted_rows[3:6],
        forces[0:3],
        forces[3:6],
    )
    return jnp.concatenate([new_position, new_velocity, forces], axis=0)


def gather_per_device(star_state, masses, phases, levels, active_list, active_count):
    shard_size = star_state.shape[1]
    total_stars = shard_size * lax.axis_size("src")
    weights = masses / total_stars
    slot_count = active_list.shape[0]
    live = jnp.arange(slot_count, dtype=jnp.int32) < active_count[0]
    write_index = jnp.where(live, active_list, shard_size)
    tick_count = jnp.left_shift(jnp.int32(1), LEVELS - 1 - levels).astype(jnp.float32)
    state_now = star_state
    for substep in range(STEPS):
        elapsed = (
            jnp.where(levels == LEVELS - 1, 1.0, phases * (tick_count - STEPS) + (substep + 1))
            * fine_step
        )
        predicted = predict(state_now, elapsed)
        sources = jnp.concatenate([predicted, weights[None, :]], axis=0)
        targets = predicted[:, active_list]
        forces = over_sources(targets, lax.all_gather(sources, "src", axis=1, tiled=True))
        new_state = correct(state_now[:, active_list], targets, forces)
        all_new, all_index = (
            lax.all_gather(new_state, "act", axis=1, tiled=True),
            lax.all_gather(write_index, "act", axis=0, tiled=True),
        )
        state_now = state_now.at[:, all_index].set(all_new, mode="drop")
    return state_now


def three_terms(x):
    high = x.astype(jnp.bfloat16)
    rest = x - high.astype(jnp.float32)
    middle = rest.astype(jnp.bfloat16)
    low = (rest - middle.astype(jnp.float32)).astype(jnp.bfloat16)
    return jnp.concatenate([high, middle, low], axis=0)


def add_terms(y):
    rows = y.shape[0] // 3
    return (y[0:rows] + y[rows : 2 * rows]) + y[2 * rows : 3 * rows]


def advance(position, velocity, acceleration, jerk, step):
    ahead = position + step * (velocity + step * (0.5 * acceleration + step * jerk / 6.0))
    speed = velocity + step * (acceleration + 0.5 * step * jerk)
    return ahead, speed


def prepare(slots, total_stars, *refs):
    out_ref, place_ref = refs[4:6]
    copies = [
        pltpu.make_async_copy(far, near, refs[10].at[k])
        for k, (far, near) in enumerate(zip(refs[0:4], refs[6:10]))
    ]
    for copy in copies:
        copy.start()
    for copy in copies:
        copy.wait()
    state_ref, mass_ref, phase_ref, level_ref = refs[6:10]
    size = state_ref.shape[1]
    level = level_ref[...]
    active = level == LEVELS - 1
    mask = jnp.where(active, 1.0, 0.0)
    blocks = size // 128
    grouped = jnp.concatenate(
        [mask[:, 128 * b : 128 * (b + 1)] for b in range(blocks)]
        + [jnp.zeros((16 - blocks, 128), jnp.float32)],
        axis=0,
    ).astype(jnp.bfloat16)
    lane_in = lax.broadcasted_iota(jnp.int32, (128, 256), 0)
    lane_out = lax.broadcasted_iota(jnp.int32, (128, 256), 1)
    counting = jnp.where((lane_in <= lane_out) | (lane_out >= 128), 1.0, 0.0).astype(jnp.bfloat16)
    counts = jnp.dot(grouped, counting, preferred_element_type=jnp.float32)
    so_far = []
    before = jnp.zeros((1, 128), jnp.float32)
    for b in range(blocks):
        so_far.append(counts[b : b + 1, 0:128] + before)
        before = before + counts[b : b + 1, 128:256]
    rank = jnp.concatenate(so_far, axis=1)
    total = jnp.concatenate([before] * blocks, axis=1)
    star = lax.broadcasted_iota(jnp.int32, (1, size), 1).astype(jnp.float32)
    place = jnp.where(active, rank - 1.0, total + star - rank)
    place_ref[0:1, :] = place
    place_ref[1:2, :] = mask
    place_ref[2:8, :] = jnp.zeros((6, size), jnp.float32)

    tick_count = jnp.left_shift(jnp.int32(1), LEVELS - 1 - level).astype(jnp.float32)
    offset = phase_ref[...] * (tick_count - STEPS)
    position, velocity = state_ref[0:3, :], state_ref[3:6, :]
    acceleration, jerk = state_ref[6:9, :], state_ref[9:12, :]
    rows = []
    for substep in range(STEPS):
        elapsed = jnp.where(active, 1.0, offset + (substep + 1)) * fine_step
        rows.extend(advance(position, velocity, acceleration, jerk, elapsed))
        if substep == 0:
            rows.append(mass_ref[...] / total_stars)
            rows.append(mask)
    rows.append(jnp.zeros((2, size), jnp.float32))
    rows.extend([acceleration, jerk, jnp.zeros((10, size), jnp.float32)])
    terms = three_terms(jnp.concatenate(rows, axis=0))
    slot = lax.broadcasted_iota(jnp.int32, (size, size), 0).astype(jnp.float32)
    chosen = jnp.where(slot == place, 1.0, 0.0).astype(jnp.bfloat16)
    moved = add_terms(
        lax.dot_general(
            terms, chosen, (((1,), (1,)), ((), ())), preferred_element_type=jnp.float32
        )
    )
    out_ref[...] = moved[0:16]
    across = size // slots
    for k in range(6):
        out_ref[14 + k // across : 15 + k // across, slots * (k % across) : slots * (k % across + 1)] = (
            moved[16 + k : 17 + k, 0:slots]
        )


def pair_terms(source, target, sums):
    sx, sy, sz, su, sv, sw, weight = source
    tx, ty, tz, tu, tv, tw = target
    dx, dy, dz = sx - tx, sy - ty, sz - tz
    du, dv, dw = su - tu, sv - tv, sw - tw
    inverse = lax.rsqrt(dx * dx + dy * dy + (dz * dz + soften_sq))
    inv_sq = inverse * inverse
    pull = weight * inverse * inv_sq
    radial = (dx * du + dy * dv + dz * dw) * (inv_sq * 3.0)
    ax, ay, az, jx, jy, jz = sums
    return (
        ax + pull * dx,
        ay + pull * dy,
        az + pull * dz,
        jx + pull * (du - radial * dx),
        jy + pull * (dv - radial * dy),
        jz + pull * (dw - radial * dz),
    )


def spread_sources(rows, spread_ref, first):
    for c in range(rows.shape[1] // 128):
        for r in range(7):
            spread_ref[r, 8 * (first + c) : 8 * (first + c + 1), :] = jnp.broadcast_to(
                rows[r : r + 1, 128 * c : 128 * (c + 1)], (8, 128)
            )


def spread_targets(rows, spread_ref, start, count):
    columns = jnp.transpose(rows)
    for r in range(6):
        spread_ref[r, start : start + count, :] = jnp.broadcast_to(
            columns[start : start + count, r : r + 1], (count, 128)
        )


def run_pairs(groups, slots, start, count, together, finish, partial_ref, sums_ref):
    lead = 8 * together
    stride = slots + lead

    def reduce(place, many):
        for g in range(many):
            for j in range(len(groups)):
                for q in range(6):
                    row = ((g * len(groups) + j) * 6 + q) * 8
                    sums_ref[pl.ds(j * stride + place + 8 * g, 8), q : q + 1] = jnp.sum(
                        partial_ref[row : row + 8, :], axis=1, keepdims=True
                    )

    def block(base, many):
        for g in range(many):
            here = pl.ds(base + 8 * g, 8)
            for j, (target_ref, columns_ref, before_ref, sources, after_ref) in enumerate(groups):
                if columns_ref is None:
                    target = [target_ref[r, here, :] for r in range(6)]
                else:
                    columns = columns_ref[here, :]
                    target = [jnp.broadcast_to(columns[:, r : r + 1], (8, 128)) for r in range(6)]
                    if target_ref is not None:
                        for r in range(6):
                            target_ref[r, here, :] = target[r]
                if before_ref is None:
                    sums = (jnp.zeros((8, 128), jnp.float32),) * 6
                else:
                    sums = tuple(before_ref[q, here, :] for q in range(6))
                for source_ref in sources:
                    for c in range(source_ref.shape[1] // 8):
                        source = [source_ref[r, 8 * c : 8 * (c + 1), :] for r in range(7)]
                        sums = pair_terms(source, target, sums)
                for q in range(6):
                    if finish:
                        row = ((g * len(groups) + j) * 6 + q) * 8
                        partial_ref[row : row + 8, :] = sums[q]
                    else:
                        after_ref[q, here, :] = sums[q]

    def body(step, unused):
        base = pl.multiple_of(start + step * lead, 8)
        if finish:
            reduce(base, together)
        block(base, together)
        return unused

    if finish:
        used = together * len(groups) * 48
        partial_ref[0:used, :] = jnp.zeros((used, 128), jnp.float32)
        if count < slots:
            sums_ref[...] = jnp.zeros_like(sums_ref)
    steps = count // lead
    lax.fori_loop(0, steps, body, 0)
    rest = (count - steps * lead) // 8
    end = start + steps * lead
    if finish:
        reduce(end, together)
    if rest:
        block(end, rest)
        if finish:
            reduce(end + lead, rest)
    if not finish:
        return None
    return [
        jnp.transpose(sums_ref[j * stride + lead : (j + 1) * stride, :])
        for j in range(len(groups))
    ]


def meet(slots, shares, known, fresh, last, *refs):
    every = known + fresh
    sent, refs = refs[:fresh], refs[fresh:]
    old_sources, old_targets, before = refs[:known], refs[known : 2 * known], refs[2 * known : 3 * known]
    refs = refs[3 * known :]
    own_ref = forces_ref = own_partial = own_sums = partial_ref = sums_ref = None
    if last:
        own_ref, forces_ref, refs = refs[0], refs[1], refs[2:]
        new_sources, refs = refs[:fresh], refs[fresh:]
        new_targets = (None,) * fresh
        after = (None,) * every
        columns_ref, own_partial, own_sums, partial_ref, sums_ref = refs
    else:
        new_sources, new_targets, after = refs[:fresh], refs[fresh : 2 * fresh], refs[2 * fresh : 2 * fresh + every]
        columns_ref = refs[2 * fresh + every]
    sources = old_sources + new_sources

    for d in range(fresh):
        spread_sources(sent[d][0:8, :], new_sources[d], 0)
        if known + d > 0:
            columns_ref[...] = jnp.transpose(sent[d][0:8, 0:slots])
    if known == 0:
        spread_targets(sent[0][0:8, 0:slots], new_targets[0], 0, slots)
        own = (new_targets[0], None, None, sources, after[0])
    else:
        own = (old_targets[0], None, before[0], new_sources, after[0])
    own = run_pairs([own], slots, 0, slots, 4 if known == 0 else 8, last, own_partial, own_sums)
    if last:
        own_ref[...] = own[0]

    def run(start, count):
        groups = []
        for d in range(1, known):
            groups.append((old_targets[d], None, before[d], new_sources, after[d]))
        for d in range(max(known, 1), every):
            groups.append((new_targets[d - known], columns_ref, None, sources, after[d]))
        together = 4 if known == 0 else 2
        forces = run_pairs(groups, slots, start, count, together, last, partial_ref, sums_ref)
        if last:
            for d in range(1, every):
                forces_ref[:, (d - 1) * slots : d * slots] = forces[d - 1]

    if len(shares) == 1:
        run(0, slots)
        return
    member = lax.rem(lax.axis_index("act"), len(shares))
    for m in range(len(shares)):

        @pl.when(member == m)
        def _():
            run(sum(shares[:m]), shares[m])


def first_step(slots, sent, forces):
    size = sent.shape[1]
    across = size // slots
    old = [
        sent[14 + k // across : 15 + k // across, slots * (k % across) : slots * (k % across + 1)]
        for k in range(6)
    ]
    old = jnp.concatenate(old, axis=0)
    position, velocity = corrected(
        old[0:3], old[3:6], sent[0:3, 0:slots], sent[3:6, 0:slots], forces[0:3], forces[3:6]
    )
    ahead, speed = advance(position, velocity, forces[0:3], forces[3:6], fine_step)
    active = sent[7:8, 0:slots] > 0.5
    return jnp.where(active, jnp.concatenate([ahead, speed], axis=0), sent[8:14, 0:slots])


def meet_still(slots, shards, *refs):
    sent, refs = refs[:shards], refs[shards:]
    own_ref, again_ref, target_ref, after_ref, still_ref = refs
    size = sent[0].shape[1]
    chunks = size // 128
    first = slots // 128
    again = first_step(slots, sent[0], own_ref[...])
    again = jnp.concatenate([again, jnp.zeros((2, slots), jnp.float32)], axis=0)
    again_ref[...] = again
    for d in range(shards):
        rows = jnp.concatenate([sent[d][8:14, slots:size], sent[d][6:8, slots:size]], axis=0)
        spread_sources(rows, still_ref, d * (chunks - first))
    spread_targets(again, target_ref, 0, slots)
    run_pairs(
        [(target_ref, None, None, (still_ref,), after_ref)], slots, 0, slots, 4, False, None, None
    )


def finish(slots, shards, parts, *refs):
    sent, refs = refs[:shards], refs[shards:]
    shares, refs = refs[:parts], refs[parts:]
    own_ref, again_ref, target_ref, before_ref, state_ref, place_ref, out_ref = refs[:7]
    later_ref, partial_ref, sums_ref = refs[7:]
    size = state_ref.shape[1]
    first = slots // 128
    own = again_ref[...]
    for d in range(shards):
        if d == 0:
            again = own[0:6]
        else:
            share = [s[:, (d - 1) * slots : d * slots] for s in shares]
            again = first_step(
                slots, sent[d], share[0] + share[1] if parts == 2 else share[0]
            )
        rows = jnp.concatenate([again, sent[d][6:8, 0:slots]], axis=0)
        spread_sources(rows, later_ref, d * first)
    second = run_pairs(
        [(target_ref, None, before_ref, (later_ref,), None)],
        slots,
        0,
        slots,
        8,
        True,
        partial_ref,
        sums_ref,
    )[0]
    before = own_ref[...]
    position, velocity = corrected(
        before[0:3], before[3:6], own[0:3], own[3:6], second[0:3], second[3:6]
    )
    new_rows = jnp.concatenate(
        [position, velocity, second[0:6], jnp.zeros((4, slots), jnp.float32)], axis=0
    )
    slot = lax.broadcasted_iota(jnp.int32, (slots, size), 0).astype(jnp.float32)
    chosen = jnp.where(slot == place_ref[0:1, :], 1.0, 0.0).astype(jnp.bfloat16)
    back = add_terms(jnp.dot(three_terms(new_rows), chosen, preferred_element_type=jnp.float32))
    out_ref[...] = jnp.where(place_ref[1:2, :] > 0.5, back[0:12], state_ref[...])


def direct_per_device(star_state, masses, phases, levels, active_list, active_count):
    del active_count
    size = star_state.shape[1]
    shards = lax.axis_size("src")
    slots = 2 * active_list.shape[0]
    whole = pl.BlockSpec(memory_space=pltpu.VMEM)
    message, place = pl.pallas_call(
        lambda *refs: prepare(slots, size * shards, *refs),
        out_shape=(
            jax.ShapeDtypeStruct((16, size), jnp.float32),
            jax.ShapeDtypeStruct((8, size), jnp.float32),
        ),
        in_specs=[pl.BlockSpec(memory_space=pltpu.HBM)] * 4,
        out_specs=(whole, whole),
        scratch_shapes=[
            pltpu.VMEM((12, size), jnp.float32),
            pltpu.VMEM((1, size), jnp.float32),
            pltpu.VMEM((1, size), jnp.float32),
            pltpu.VMEM((1, size), jnp.int32),
            pltpu.SemaphoreType.DMA((4,)),
        ],
        compiler_params=pltpu.CompilerParams(vmem_limit_bytes=16 * 2**20),
        name="prepare",
    )(
        *(
            pltpu.with_memory_space_constraint(x, pltpu.HBM)
            for x in (star_state, masses.reshape(1, size), phases.reshape(1, size), levels.reshape(1, size))
        )
    )
    sent = [message]
    for shift in range(1, shards):
        pairs = [(d, (d + shift) % shards) for d in range(shards)]
        sent.append(lax.ppermute(message, "src", pairs))

    limit = pltpu.CompilerParams(vmem_limit_bytes=16 * 2**20)
    owners = lax.axis_size("act")
    shares = (slots,)
    if owners % 2 == 0:
        first_share = slots * 3 // 8 // 16 * 16
        shares = (first_share, slots - first_share)
    source_shape = jax.ShapeDtypeStruct((7, size // 16, 128), jnp.float32)
    target_shape = jax.ShapeDtypeStruct((6, slots, 128), jnp.float32)
    own_shape = jax.ShapeDtypeStruct((8, slots), jnp.float32)
    columns = pltpu.VMEM((slots, 8), jnp.float32)
    sources, targets, sums = [], [], []
    known = 0
    for fresh in [2] + [1] * (shards - 2):
        every = known + fresh
        last = every == shards
        if last:
            out_shape = (own_shape, jax.ShapeDtypeStruct((8, (shards - 1) * slots), jnp.float32))
            scratch = [
                pltpu.VMEM(source_shape.shape, jnp.float32),
                columns,
                pltpu.VMEM((8 * 48, 128), jnp.float32),
                pltpu.VMEM((slots + 64, 8), jnp.float32),
                pltpu.VMEM((2 * (shards - 1) * 48, 128), jnp.float32),
                pltpu.VMEM(((shards - 1) * (slots + 16), 8), jnp.float32),
            ]
        else:
            out_shape = [source_shape] * fresh + [target_shape] * (fresh + every)
            scratch = [columns]
        outs = pl.pallas_call(
            functools.partial(meet, slots, shares, known, fresh, last),
            out_shape=out_shape,
            in_specs=[whole] * (fresh + 3 * known),
            out_specs=(whole, whole) if last else [whole] * (2 * fresh + every),
            scratch_shapes=scratch,
            compiler_params=limit,
            name=f"meet_{every}",
        )(*sent[known:every], *sources, *targets, *sums)
        if last:
            break
        sources += outs[:fresh]
        targets += outs[fresh : 2 * fresh]
        sums = list(outs[2 * fresh :])
        known = every
    own, part = outs
    parts = [part]
    if len(shares) == 2:
        parts.append(lax.ppermute(part, "act", [(i, i ^ 1) for i in range(owners)]))
    first = slots // 128
    again, target, still = pl.pallas_call(
        functools.partial(meet_still, slots, shards),
        out_shape=(own_shape, target_shape, target_shape),
        in_specs=[whole] * (shards + 1),
        out_specs=(whole,) * 3,
        scratch_shapes=[pltpu.VMEM((7, shards * (size // 128 - first) * 8, 128), jnp.float32)],
        compiler_params=limit,
        name="meet_still",
    )(*sent, own)
    return pl.pallas_call(
        functools.partial(finish, slots, shards, len(parts)),
        out_shape=jax.ShapeDtypeStruct((12, size), jnp.float32),
        in_specs=[whole] * (shards + len(parts) + 6),
        out_specs=whole,
        scratch_shapes=[
            pltpu.VMEM((7, shards * first * 8, 128), jnp.float32),
            pltpu.VMEM((8 * 48, 128), jnp.float32),
            pltpu.VMEM((slots + 64, 8), jnp.float32),
        ],
        compiler_params=limit,
        name="finish",
    )(*sent, *parts, own, again, target, still, star_state, place)


def solution(mesh):
    in_specs = (
        P(None, ("groups", "src")),
        P(("groups", "src")),
        P(("groups", "src")),
        P(("groups", "src")),
        P(("groups", "src", "act")),
        P(("groups", "src", "act")),
    )
    out_specs = P(None, ("groups", "src"))
    few = 3 <= mesh.shape["src"] <= MAX_DIRECT
    return jax.shard_map(
        direct_per_device if few else gather_per_device,
        mesh=mesh,
        in_specs=in_specs,
        out_specs=out_specs,
        check_vma=False,
    )
```

```python
import functools

import jax
import jax.numpy as jnp
from jax import lax
from jax.experimental import pallas as pl
from jax.experimental.pallas import tpu as pltpu
from jax.sharding import PartitionSpec as P


LEVELS = 5
STEPS = 2
MAX_DIRECT = 8


soften_sq = 0.0004
fine_step = 0.03125


def predict(star_state, elapsed):
    interval = elapsed[None, :]
    position = star_state[0:3] + interval * (
        star_state[3:6] + interval * (0.5 * star_state[6:9] + interval * star_state[9:12] / 6.0)
    )
    velocity = star_state[3:6] + interval * (star_state[6:9] + 0.5 * interval * star_state[9:12])
    return jnp.concatenate([position, velocity], axis=0)


def pair_block(targets, sources):
    delta_pos = sources[0:3, None, :] - targets[0:3, :, None]
    delta_vel = sources[3:6, None, :] - targets[3:6, :, None]
    dist_sq = (
        delta_pos[0] * delta_pos[0]
        + delta_pos[1] * delta_pos[1]
        + delta_pos[2] * delta_pos[2]
        + soften_sq
    )
    inverse = lax.rsqrt(dist_sq)
    inv_sq = inverse * inverse
    weight = sources[6][None, :] * inverse * inv_sq
    radial = (
        (delta_pos[0] * delta_vel[0] + delta_pos[1] * delta_vel[1] + delta_pos[2] * delta_vel[2])
        * inv_sq
        * 3.0
    )
    acceleration = jnp.sum(weight[None] * delta_pos, axis=2)
    jerk_sum = jnp.sum(weight[None] * (delta_vel - radial[None] * delta_pos), axis=2)
    return jnp.concatenate([acceleration, jerk_sum], axis=0)


def over_sources(targets, sources):
    count_src = sources.shape[1]
    width = 512
    blocks = sources.reshape(7, count_src // width, width).transpose(1, 0, 2)

    def accumulate(running, portion):
        return (running + pair_block(targets, portion), None)

    init = jnp.zeros((6, targets.shape[1]), jnp.float32)
    running, _ = lax.scan(accumulate, init, blocks)
    return running


def corrected(acc_old, jerk_old, position, velocity, acc_new, jerk_new):
    snap_term = (-6.0 * (acc_old - acc_new) - fine_step * (4.0 * jerk_old + 2.0 * jerk_new)) / (
        fine_step * fine_step
    )
    crackle = (12.0 * (acc_old - acc_new) + 6.0 * fine_step * (jerk_old + jerk_new)) / (
        fine_step * fine_step * fine_step
    )
    new_position = position + fine_step**4 / 24.0 * snap_term + fine_step**5 / 120.0 * crackle
    new_velocity = velocity + fine_step**3 / 6.0 * snap_term + fine_step**4 / 24.0 * crackle
    return new_position, new_velocity


def correct(old_state, predicted_rows, forces):
    new_position, new_velocity = corrected(
        old_state[6:9],
        old_state[9:12],
        predicted_rows[0:3],
        predicted_rows[3:6],
        forces[0:3],
        forces[3:6],
    )
    return jnp.concatenate([new_position, new_velocity, forces], axis=0)


def gather_per_device(star_state, masses, phases, levels, active_list, active_count):
    shard_size = star_state.shape[1]
    total_stars = shard_size * lax.axis_size("src")
    weights = masses / total_stars
    slot_count = active_list.shape[0]
    live = jnp.arange(slot_count, dtype=jnp.int32) < active_count[0]
    write_index = jnp.where(live, active_list, shard_size)
    tick_count = jnp.left_shift(jnp.int32(1), LEVELS - 1 - levels).astype(jnp.float32)
    state_now = star_state
    for substep in range(STEPS):
        elapsed = (
            jnp.where(levels == LEVELS - 1, 1.0, phases * (tick_count - STEPS) + (substep + 1))
            * fine_step
        )
        predicted = predict(state_now, elapsed)
        sources = jnp.concatenate([predicted, weights[None, :]], axis=0)
        targets = predicted[:, active_list]
        forces = over_sources(targets, lax.all_gather(sources, "src", axis=1, tiled=True))
        new_state = correct(state_now[:, active_list], targets, forces)
        all_new, all_index = (
            lax.all_gather(new_state, "act", axis=1, tiled=True),
            lax.all_gather(write_index, "act", axis=0, tiled=True),
        )
        state_now = state_now.at[:, all_index].set(all_new, mode="drop")
    return state_now


def three_terms(x):
    high = x.astype(jnp.bfloat16)
    rest = x - high.astype(jnp.float32)
    middle = rest.astype(jnp.bfloat16)
    low = (rest - middle.astype(jnp.float32)).astype(jnp.bfloat16)
    return jnp.concatenate([high, middle, low], axis=0)


def add_terms(y):
    rows = y.shape[0] // 3
    return (y[0:rows] + y[rows : 2 * rows]) + y[2 * rows : 3 * rows]


def advance(position, velocity, acceleration, jerk, step):
    ahead = position + step * (velocity + step * (0.5 * acceleration + step * jerk / 6.0))
    speed = velocity + step * (acceleration + 0.5 * step * jerk)
    return ahead, speed


def prepare(slots, total_stars, *refs):
    out_ref, place_ref = refs[4:6]
    copies = [
        pltpu.make_async_copy(far, near, refs[10].at[k])
        for k, (far, near) in enumerate(zip(refs[0:4], refs[6:10]))
    ]
    for copy in copies:
        copy.start()
    for copy in copies:
        copy.wait()
    state_ref, mass_ref, phase_ref, level_ref = refs[6:10]
    size = state_ref.shape[1]
    level = level_ref[...]
    active = level == LEVELS - 1
    mask = jnp.where(active, 1.0, 0.0)
    blocks = size // 128
    grouped = jnp.concatenate(
        [mask[:, 128 * b : 128 * (b + 1)] for b in range(blocks)]
        + [jnp.zeros((16 - blocks, 128), jnp.float32)],
        axis=0,
    ).astype(jnp.bfloat16)
    lane_in = lax.broadcasted_iota(jnp.int32, (128, 256), 0)
    lane_out = lax.broadcasted_iota(jnp.int32, (128, 256), 1)
    counting = jnp.where((lane_in <= lane_out) | (lane_out >= 128), 1.0, 0.0).astype(jnp.bfloat16)
    counts = jnp.dot(grouped, counting, preferred_element_type=jnp.float32)
    so_far = []
    before = jnp.zeros((1, 128), jnp.float32)
    for b in range(blocks):
        so_far.append(counts[b : b + 1, 0:128] + before)
        before = before + counts[b : b + 1, 128:256]
    rank = jnp.concatenate(so_far, axis=1)
    total = jnp.concatenate([before] * blocks, axis=1)
    star = lax.broadcasted_iota(jnp.int32, (1, size), 1).astype(jnp.float32)
    place = jnp.where(active, rank - 1.0, total + star - rank)
    place_ref[0:1, :] = place
    place_ref[1:2, :] = mask
    place_ref[2:8, :] = jnp.zeros((6, size), jnp.float32)

    tick_count = jnp.left_shift(jnp.int32(1), LEVELS - 1 - level).astype(jnp.float32)
    offset = phase_ref[...] * (tick_count - STEPS)
    position, velocity = state_ref[0:3, :], state_ref[3:6, :]
    acceleration, jerk = state_ref[6:9, :], state_ref[9:12, :]
    rows = []
    for substep in range(STEPS):
        elapsed = jnp.where(active, 1.0, offset + (substep + 1)) * fine_step
        rows.extend(advance(position, velocity, acceleration, jerk, elapsed))
        if substep == 0:
            rows.append(mass_ref[...] / total_stars)
            rows.append(mask)
    rows.append(jnp.zeros((2, size), jnp.float32))
    rows.extend([acceleration, jerk, jnp.zeros((10, size), jnp.float32)])
    terms = three_terms(jnp.concatenate(rows, axis=0))
    slot = lax.broadcasted_iota(jnp.int32, (size, size), 0).astype(jnp.float32)
    chosen = jnp.where(slot == place, 1.0, 0.0).astype(jnp.bfloat16)
    moved = add_terms(
        lax.dot_general(
            terms, chosen, (((1,), (1,)), ((), ())), preferred_element_type=jnp.float32
        )
    )
    out_ref[...] = moved[0:16]
    across = size // slots
    for k in range(6):
        out_ref[14 + k // across : 15 + k // across, slots * (k % across) : slots * (k % across + 1)] = (
            moved[16 + k : 17 + k, 0:slots]
        )


def pair_terms(source, target, sums):
    sx, sy, sz, su, sv, sw, weight = source
    tx, ty, tz, tu, tv, tw = target
    dx, dy, dz = sx - tx, sy - ty, sz - tz
    du, dv, dw = su - tu, sv - tv, sw - tw
    inverse = lax.rsqrt(dx * dx + dy * dy + (dz * dz + soften_sq))
    inv_sq = inverse * inverse
    pull = weight * inverse * inv_sq
    radial = (dx * du + dy * dv + dz * dw) * (inv_sq * 3.0)
    ax, ay, az, jx, jy, jz = sums
    return (
        ax + pull * dx,
        ay + pull * dy,
        az + pull * dz,
        jx + pull * (du - radial * dx),
        jy + pull * (dv - radial * dy),
        jz + pull * (dw - radial * dz),
    )


def spread_sources(rows, spread_ref, first):
    for c in range(rows.shape[1] // 128):
        for r in range(7):
            spread_ref[r, 8 * (first + c) : 8 * (first + c + 1), :] = jnp.broadcast_to(
                rows[r : r + 1, 128 * c : 128 * (c + 1)], (8, 128)
            )


def spread_targets(rows, spread_ref, start, count):
    columns = jnp.transpose(rows)
    for r in range(6):
        spread_ref[r, start : start + count, :] = jnp.broadcast_to(
            columns[start : start + count, r : r + 1], (count, 128)
        )


def run_pairs(groups, slots, start, count, together, finish, partial_ref, sums_ref):
    lead = 8 * together
    stride = slots + lead

    def reduce(place, many):
        for g in range(many):
            for j in range(len(groups)):
                for q in range(6):
                    row = ((g * len(groups) + j) * 6 + q) * 8
                    sums_ref[pl.ds(j * stride + place + 8 * g, 8), q : q + 1] = jnp.sum(
                        partial_ref[row : row + 8, :], axis=1, keepdims=True
                    )

    def block(base, many):
        for g in range(many):
            here = pl.ds(base + 8 * g, 8)
            for j, (target_ref, columns_ref, before_ref, sources, after_ref) in enumerate(groups):
                if columns_ref is None:
                    target = [target_ref[r, here, :] for r in range(6)]
                else:
                    columns = columns_ref[here, :]
                    target = [jnp.broadcast_to(columns[:, r : r + 1], (8, 128)) for r in range(6)]
                    if target_ref is not None:
                        for r in range(6):
                            target_ref[r, here, :] = target[r]
                if before_ref is None:
                    sums = (jnp.zeros((8, 128), jnp.float32),) * 6
                else:
                    sums = tuple(before_ref[q, here, :] for q in range(6))
                for source_ref in sources:
                    for c in range(source_ref.shape[1] // 8):
                        source = [source_ref[r, 8 * c : 8 * (c + 1), :] for r in range(7)]
                        sums = pair_terms(source, target, sums)
                for q in range(6):
                    if finish:
                        row = ((g * len(groups) + j) * 6 + q) * 8
                        partial_ref[row : row + 8, :] = sums[q]
                    else:
                        after_ref[q, here, :] = sums[q]

    def body(step, unused):
        base = pl.multiple_of(start + step * lead, 8)
        if finish:
            reduce(base, together)
        block(base, together)
        return unused

    if finish:
        used = together * len(groups) * 48
        partial_ref[0:used, :] = jnp.zeros((used, 128), jnp.float32)
        if count < slots:
            sums_ref[...] = jnp.zeros_like(sums_ref)
    steps = count // lead
    lax.fori_loop(0, steps, body, 0)
    rest = (count - steps * lead) // 8
    end = start + steps * lead
    if finish:
        reduce(end, together)
    if rest:
        block(end, rest)
        if finish:
            reduce(end + lead, rest)
    if not finish:
        return None
    return [
        jnp.transpose(sums_ref[j * stride + lead : (j + 1) * stride, :])
        for j in range(len(groups))
    ]


def on_member(shares, run):
    if len(shares) == 1:
        run(0, shares[0])
        return
    member = lax.rem(lax.axis_index("act"), len(shares))
    for m in range(len(shares)):

        @pl.when(member == m)
        def _():
            run(sum(shares[:m]), shares[m])


def meet(slots, shares, known, fresh, *refs):
    every = known + fresh
    sent, refs = refs[:fresh], refs[fresh:]
    old_sources, old_targets, before = refs[:known], refs[known : 2 * known], refs[2 * known : 3 * known]
    refs = refs[3 * known :]
    new_sources, new_targets, after = refs[:fresh], refs[fresh : 2 * fresh], refs[2 * fresh : 2 * fresh + every]
    columns_ref = refs[2 * fresh + every]
    sources = old_sources + new_sources

    def run(start, count):
        groups = []
        for d in range(known):
            groups.append((old_targets[d], None, before[d], new_sources, after[d]))
        for d in range(fresh):
            spread_sources(sent[d][0:8, :], new_sources[d], 0)
            in_loop = None
            if known:
                in_loop = columns_ref
                columns_ref[...] = jnp.transpose(sent[d][0:8, 0:slots])
            else:
                spread_targets(sent[d][0:8, 0:slots], new_targets[d], start, count)
            groups.append((new_targets[d], in_loop, None, sources, after[known + d]))
        run_pairs(groups, slots, start, count, 2, False, None, None)

    on_member(shares, run)


def meet_own(slots, shares, sent_ref, target_ref, before_ref, source_ref, own_ref, *scratch):
    spread_sources(sent_ref[0:8, :], source_ref, 0)

    def run(start, count):
        group = (target_ref, None, before_ref, (source_ref,), None)
        own_ref[...] = run_pairs(
            [group], slots, start, count, count // 8, True, scratch[0], scratch[1]
        )[0]

    on_member(shares, run)


def meet_rest(slots, shares, known, sent_ref, source_ref, *refs):
    sources, targets, before = refs[:known], refs[known : 2 * known - 1], refs[2 * known - 1 : 3 * known - 2]
    forces_ref, columns_ref, partial_ref, sums_ref = refs[3 * known - 2 :]
    columns_ref[...] = jnp.transpose(sent_ref[0:8, 0:slots])

    def run(start, count):
        groups = [(t, None, b, (source_ref,), None) for t, b in zip(targets, before)]
        groups.append((None, columns_ref, None, sources + (source_ref,), None))
        forces = run_pairs(groups, slots, start, count, 2, True, partial_ref, sums_ref)
        for d in range(known):
            forces_ref[:, d * slots : (d + 1) * slots] = forces[d]

    on_member(shares, run)


def first_step(slots, sent, forces):
    size = sent.shape[1]
    across = size // slots
    old = [
        sent[14 + k // across : 15 + k // across, slots * (k % across) : slots * (k % across + 1)]
        for k in range(6)
    ]
    old = jnp.concatenate(old, axis=0)
    position, velocity = corrected(
        old[0:3], old[3:6], sent[0:3, 0:slots], sent[3:6, 0:slots], forces[0:3], forces[3:6]
    )
    ahead, speed = advance(position, velocity, forces[0:3], forces[3:6], fine_step)
    active = sent[7:8, 0:slots] > 0.5
    return jnp.where(active, jnp.concatenate([ahead, speed], axis=0), sent[8:14, 0:slots])


def meet_still(slots, shards, parts, *refs):
    sent, refs = refs[:shards], refs[shards:]
    shares, refs = refs[:parts], refs[parts:]
    own_ref, again_ref, target_ref, after_ref, still_ref = refs
    own_ref[...] = shares[0][...] + shares[1][...] if parts == 2 else shares[0][...]
    size = sent[0].shape[1]
    chunks = size // 128
    first = slots // 128
    again = first_step(slots, sent[0], own_ref[...])
    again = jnp.concatenate([again, jnp.zeros((2, slots), jnp.float32)], axis=0)
    again_ref[...] = again
    for d in range(shards):
        rows = jnp.concatenate([sent[d][8:14, slots:size], sent[d][6:8, slots:size]], axis=0)
        spread_sources(rows, still_ref, d * (chunks - first))
    spread_targets(again, target_ref, 0, slots)
    run_pairs(
        [(target_ref, None, None, (still_ref,), after_ref)], slots, 0, slots, 4, False, None, None
    )


def finish(slots, shards, parts, *refs):
    sent, refs = refs[:shards], refs[shards:]
    shares, refs = refs[:parts], refs[parts:]
    own_ref, again_ref, target_ref, before_ref, state_ref, place_ref, out_ref = refs[:7]
    later_ref, partial_ref, sums_ref = refs[7:]
    size = state_ref.shape[1]
    first = slots // 128
    own = again_ref[...]
    for d in range(shards):
        if d == 0:
            again = own[0:6]
        else:
            share = [s[:, (d - 1) * slots : d * slots] for s in shares]
            again = first_step(
                slots, sent[d], share[0] + share[1] if parts == 2 else share[0]
            )
        rows = jnp.concatenate([again, sent[d][6:8, 0:slots]], axis=0)
        spread_sources(rows, later_ref, d * first)
    second = run_pairs(
        [(target_ref, None, before_ref, (later_ref,), None)],
        slots,
        0,
        slots,
        8,
        True,
        partial_ref,
        sums_ref,
    )[0]
    before = own_ref[...]
    position, velocity = corrected(
        before[0:3], before[3:6], own[0:3], own[3:6], second[0:3], second[3:6]
    )
    new_rows = jnp.concatenate(
        [position, velocity, second[0:6], jnp.zeros((4, slots), jnp.float32)], axis=0
    )
    slot = lax.broadcasted_iota(jnp.int32, (slots, size), 0).astype(jnp.float32)
    chosen = jnp.where(slot == place_ref[0:1, :], 1.0, 0.0).astype(jnp.bfloat16)
    back = add_terms(jnp.dot(three_terms(new_rows), chosen, preferred_element_type=jnp.float32))
    out_ref[...] = jnp.where(place_ref[1:2, :] > 0.5, back[0:12], state_ref[...])


def direct_per_device(star_state, masses, phases, levels, active_list, active_count):
    del active_count
    size = star_state.shape[1]
    shards = lax.axis_size("src")
    slots = 2 * active_list.shape[0]
    whole = pl.BlockSpec(memory_space=pltpu.VMEM)
    message, place = pl.pallas_call(
        lambda *refs: prepare(slots, size * shards, *refs),
        out_shape=(
            jax.ShapeDtypeStruct((16, size), jnp.float32),
            jax.ShapeDtypeStruct((8, size), jnp.float32),
        ),
        in_specs=[pl.BlockSpec(memory_space=pltpu.HBM)] * 4,
        out_specs=(whole, whole),
        scratch_shapes=[
            pltpu.VMEM((12, size), jnp.float32),
            pltpu.VMEM((1, size), jnp.float32),
            pltpu.VMEM((1, size), jnp.float32),
            pltpu.VMEM((1, size), jnp.int32),
            pltpu.SemaphoreType.DMA((4,)),
        ],
        compiler_params=pltpu.CompilerParams(vmem_limit_bytes=16 * 2**20),
        name="prepare",
    )(
        *(
            pltpu.with_memory_space_constraint(x, pltpu.HBM)
            for x in (star_state, masses.reshape(1, size), phases.reshape(1, size), levels.reshape(1, size))
        )
    )
    sent = [message]
    for shift in range(1, shards):
        pairs = [(d, (d + shift) % shards) for d in range(shards)]
        sent.append(lax.ppermute(message, "src", pairs))

    limit = pltpu.CompilerParams(vmem_limit_bytes=16 * 2**20)
    owners = lax.axis_size("act")
    shares = (slots,)
    if owners % 2 == 0:
        first_share = slots * 3 // 8 // 16 * 16
        shares = (first_share, slots - first_share)
    parts = len(shares)

    def with_other(part):
        if parts == 1:
            return [part]
        return [part, lax.ppermute(part, "act", [(i, i ^ 1) for i in range(owners)])]

    def call(body, operands, out_shape, scratch=(), pairs=0):
        cost = pl.CostEstimate(flops=41 * pairs, bytes_accessed=0, transcendentals=pairs)
        return pl.pallas_call(
            body,
            out_shape=out_shape,
            in_specs=[whole] * len(operands),
            out_specs=jax.tree.map(lambda _: whole, out_shape),
            scratch_shapes=list(scratch),
            compiler_params=limit,
            cost_estimate=cost if pairs else None,
        )(*operands)

    def rows(shape):
        return pltpu.VMEM(shape, jnp.float32)

    source_shape = jax.ShapeDtypeStruct((7, size // 16, 128), jnp.float32)
    target_shape = jax.ShapeDtypeStruct((6, slots, 128), jnp.float32)
    own_shape = jax.ShapeDtypeStruct((8, slots), jnp.float32)
    sources, targets, sums = [], [], []
    known = 0
    for fresh in [2] + [1] * (shards - 3):
        every = known + fresh
        outs = call(
            functools.partial(meet, slots, shares, known, fresh),
            [*sent[known:every], *sources, *targets, *sums],
            [source_shape] * fresh + [target_shape] * (fresh + every),
            [rows((slots, 8))],
        )
        sources += outs[:fresh]
        targets += outs[fresh : 2 * fresh]
        sums = list(outs[2 * fresh :])
        known = every
    source, own = call(
        functools.partial(meet_own, slots, shares),
        [sent[known], targets[0], sums[0]],
        (source_shape, own_shape),
        [rows((max(shares) * 6, 128)), rows((slots + max(shares), 8))],
    )
    own = with_other(own)
    forces = call(
        functools.partial(meet_rest, slots, shares, known),
        [sent[known], source, *sources, *targets[1:], *sums[1:]],
        jax.ShapeDtypeStruct((8, known * slots), jnp.float32),
        [rows((slots, 8)), rows((2 * known * 48, 128)), rows((known * (slots + 16), 8))],
        2 * known * max(shares) * size,
    )
    forces = with_other(forces)
    first = slots // 128
    own, again, target, still = call(
        functools.partial(meet_still, slots, shards, parts),
        [*sent, *own],
        (own_shape, own_shape, target_shape, target_shape),
        [rows((7, shards * (size // 128 - first) * 8, 128))],
        slots * shards * (size - slots),
    )
    return call(
        functools.partial(finish, slots, shards, parts),
        [*sent, *forces, own, again, target, still, star_state, place],
        jax.ShapeDtypeStruct((12, size), jnp.float32),
        [rows((7, shards * first * 8, 128)), rows((8 * 48, 128)), rows((slots + 64, 8))],
    )


def solution(mesh):
    in_specs = (
        P(None, ("groups", "src")),
        P(("groups", "src")),
        P(("groups", "src")),
        P(("groups", "src")),
        P(("groups", "src", "act")),
        P(("groups", "src", "act")),
    )
    out_specs = P(None, ("groups", "src"))
    few = 3 <= mesh.shape["src"] <= MAX_DIRECT
    return jax.shard_map(
        direct_per_device if few else gather_per_device,
        mesh=mesh,
        in_specs=in_specs,
        out_specs=out_specs,
        check_vma=False,
    )
```

```python
import functools

import jax
import jax.numpy as jnp
from jax import lax
from jax.experimental import pallas as pl
from jax.experimental.pallas import tpu as pltpu
from jax.sharding import PartitionSpec as P


LEVELS = 5
STEPS = 2
MAX_DIRECT = 8


soften_sq = 0.0004
fine_step = 0.03125


def predict(star_state, elapsed):
    interval = elapsed[None, :]
    position = star_state[0:3] + interval * (
        star_state[3:6] + interval * (0.5 * star_state[6:9] + interval * star_state[9:12] / 6.0)
    )
    velocity = star_state[3:6] + interval * (star_state[6:9] + 0.5 * interval * star_state[9:12])
    return jnp.concatenate([position, velocity], axis=0)


def pair_block(targets, sources):
    delta_pos = sources[0:3, None, :] - targets[0:3, :, None]
    delta_vel = sources[3:6, None, :] - targets[3:6, :, None]
    dist_sq = (
        delta_pos[0] * delta_pos[0]
        + delta_pos[1] * delta_pos[1]
        + delta_pos[2] * delta_pos[2]
        + soften_sq
    )
    inverse = lax.rsqrt(dist_sq)
    inv_sq = inverse * inverse
    weight = sources[6][None, :] * inverse * inv_sq
    radial = (
        (delta_pos[0] * delta_vel[0] + delta_pos[1] * delta_vel[1] + delta_pos[2] * delta_vel[2])
        * inv_sq
        * 3.0
    )
    acceleration = jnp.sum(weight[None] * delta_pos, axis=2)
    jerk_sum = jnp.sum(weight[None] * (delta_vel - radial[None] * delta_pos), axis=2)
    return jnp.concatenate([acceleration, jerk_sum], axis=0)


def over_sources(targets, sources):
    count_src = sources.shape[1]
    width = 512
    blocks = sources.reshape(7, count_src // width, width).transpose(1, 0, 2)

    def accumulate(running, portion):
        return (running + pair_block(targets, portion), None)

    init = jnp.zeros((6, targets.shape[1]), jnp.float32)
    running, _ = lax.scan(accumulate, init, blocks)
    return running


def corrected(acc_old, jerk_old, position, velocity, acc_new, jerk_new):
    snap_term = (-6.0 * (acc_old - acc_new) - fine_step * (4.0 * jerk_old + 2.0 * jerk_new)) / (
        fine_step * fine_step
    )
    crackle = (12.0 * (acc_old - acc_new) + 6.0 * fine_step * (jerk_old + jerk_new)) / (
        fine_step * fine_step * fine_step
    )
    new_position = position + fine_step**4 / 24.0 * snap_term + fine_step**5 / 120.0 * crackle
    new_velocity = velocity + fine_step**3 / 6.0 * snap_term + fine_step**4 / 24.0 * crackle
    return new_position, new_velocity


def correct(old_state, predicted_rows, forces):
    new_position, new_velocity = corrected(
        old_state[6:9],
        old_state[9:12],
        predicted_rows[0:3],
        predicted_rows[3:6],
        forces[0:3],
        forces[3:6],
    )
    return jnp.concatenate([new_position, new_velocity, forces], axis=0)


def gather_per_device(star_state, masses, phases, levels, active_list, active_count):
    shard_size = star_state.shape[1]
    total_stars = shard_size * lax.axis_size("src")
    weights = masses / total_stars
    slot_count = active_list.shape[0]
    live = jnp.arange(slot_count, dtype=jnp.int32) < active_count[0]
    write_index = jnp.where(live, active_list, shard_size)
    tick_count = jnp.left_shift(jnp.int32(1), LEVELS - 1 - levels).astype(jnp.float32)
    state_now = star_state
    for substep in range(STEPS):
        elapsed = (
            jnp.where(levels == LEVELS - 1, 1.0, phases * (tick_count - STEPS) + (substep + 1))
            * fine_step
        )
        predicted = predict(state_now, elapsed)
        sources = jnp.concatenate([predicted, weights[None, :]], axis=0)
        targets = predicted[:, active_list]
        forces = over_sources(targets, lax.all_gather(sources, "src", axis=1, tiled=True))
        new_state = correct(state_now[:, active_list], targets, forces)
        all_new, all_index = (
            lax.all_gather(new_state, "act", axis=1, tiled=True),
            lax.all_gather(write_index, "act", axis=0, tiled=True),
        )
        state_now = state_now.at[:, all_index].set(all_new, mode="drop")
    return state_now


def three_terms(x):
    high = x.astype(jnp.bfloat16)
    rest = x - high.astype(jnp.float32)
    middle = rest.astype(jnp.bfloat16)
    low = (rest - middle.astype(jnp.float32)).astype(jnp.bfloat16)
    return jnp.concatenate([high, middle, low], axis=0)


def add_terms(y):
    rows = y.shape[0] // 3
    return (y[0:rows] + y[rows : 2 * rows]) + y[2 * rows : 3 * rows]


def advance(position, velocity, acceleration, jerk, step):
    ahead = position + step * (velocity + step * (0.5 * acceleration + step * jerk / 6.0))
    speed = velocity + step * (acceleration + 0.5 * step * jerk)
    return ahead, speed


def prepare(slots, total_stars, *refs):
    out_ref, place_ref = refs[4:6]
    copies = [
        pltpu.make_async_copy(far, near, refs[10].at[k])
        for k, (far, near) in enumerate(zip(refs[0:4], refs[6:10]))
    ]
    for copy in copies:
        copy.start()
    for copy in copies:
        copy.wait()
    state_ref, mass_ref, phase_ref, level_ref = refs[6:10]
    size = state_ref.shape[1]
    level = level_ref[...]
    active = level == LEVELS - 1
    mask = jnp.where(active, 1.0, 0.0)
    blocks = size // 128
    grouped = jnp.concatenate(
        [mask[:, 128 * b : 128 * (b + 1)] for b in range(blocks)]
        + [jnp.zeros((16 - blocks, 128), jnp.float32)],
        axis=0,
    ).astype(jnp.bfloat16)
    lane_in = lax.broadcasted_iota(jnp.int32, (128, 256), 0)
    lane_out = lax.broadcasted_iota(jnp.int32, (128, 256), 1)
    counting = jnp.where((lane_in <= lane_out) | (lane_out >= 128), 1.0, 0.0).astype(jnp.bfloat16)
    counts = jnp.dot(grouped, counting, preferred_element_type=jnp.float32)
    so_far = []
    before = jnp.zeros((1, 128), jnp.float32)
    for b in range(blocks):
        so_far.append(counts[b : b + 1, 0:128] + before)
        before = before + counts[b : b + 1, 128:256]
    rank = jnp.concatenate(so_far, axis=1)
    total = jnp.concatenate([before] * blocks, axis=1)
    star = lax.broadcasted_iota(jnp.int32, (1, size), 1).astype(jnp.float32)
    place = jnp.where(active, rank - 1.0, total + star - rank)
    place_ref[0:1, :] = place
    place_ref[1:2, :] = mask
    place_ref[2:8, :] = jnp.zeros((6, size), jnp.float32)

    tick_count = jnp.left_shift(jnp.int32(1), LEVELS - 1 - level).astype(jnp.float32)
    offset = phase_ref[...] * (tick_count - STEPS)
    position, velocity = state_ref[0:3, :], state_ref[3:6, :]
    acceleration, jerk = state_ref[6:9, :], state_ref[9:12, :]
    rows = []
    for substep in range(STEPS):
        elapsed = jnp.where(active, 1.0, offset + (substep + 1)) * fine_step
        rows.extend(advance(position, velocity, acceleration, jerk, elapsed))
        if substep == 0:
            rows.append(mass_ref[...] / total_stars)
            rows.append(mask)
    rows.append(jnp.zeros((2, size), jnp.float32))
    rows.extend([acceleration, jerk, jnp.zeros((10, size), jnp.float32)])
    terms = three_terms(jnp.concatenate(rows, axis=0))
    slot = lax.broadcasted_iota(jnp.int32, (size, size), 0).astype(jnp.float32)
    chosen = jnp.where(slot == place, 1.0, 0.0).astype(jnp.bfloat16)
    moved = add_terms(
        lax.dot_general(
            terms, chosen, (((1,), (1,)), ((), ())), preferred_element_type=jnp.float32
        )
    )
    out_ref[...] = moved[0:16]
    across = size // slots
    for k in range(6):
        out_ref[14 + k // across : 15 + k // across, slots * (k % across) : slots * (k % across + 1)] = (
            moved[16 + k : 17 + k, 0:slots]
        )


def pair_terms(source, target, sums):
    sx, sy, sz, su, sv, sw, weight = source
    tx, ty, tz, tu, tv, tw = target
    dx, dy, dz = sx - tx, sy - ty, sz - tz
    du, dv, dw = su - tu, sv - tv, sw - tw
    inverse = lax.rsqrt(dx * dx + dy * dy + (dz * dz + soften_sq))
    inv_sq = inverse * inverse
    pull = weight * inverse * inv_sq
    radial = (dx * du + dy * dv + dz * dw) * (inv_sq * 3.0)
    ax, ay, az, jx, jy, jz = sums
    return (
        ax + pull * dx,
        ay + pull * dy,
        az + pull * dz,
        jx + pull * (du - radial * dx),
        jy + pull * (dv - radial * dy),
        jz + pull * (dw - radial * dz),
    )


def spread_sources(rows, spread_ref, first):
    for c in range(rows.shape[1] // 128):
        for r in range(7):
            spread_ref[r, 8 * (first + c) : 8 * (first + c + 1), :] = jnp.broadcast_to(
                rows[r : r + 1, 128 * c : 128 * (c + 1)], (8, 128)
            )


def spread_targets(rows, spread_ref, start, count):
    columns = jnp.transpose(rows)
    for r in range(6):
        spread_ref[r, start : start + count, :] = jnp.broadcast_to(
            columns[start : start + count, r : r + 1], (count, 128)
        )


def run_pairs(groups, slots, start, count, together, finish, partial_ref, sums_ref):
    lead = 8 * together
    stride = slots + lead

    def reduce(place, many):
        for g in range(many):
            for j in range(len(groups)):
                for q in range(6):
                    row = ((g * len(groups) + j) * 6 + q) * 8
                    sums_ref[pl.ds(j * stride + place + 8 * g, 8), q : q + 1] = jnp.sum(
                        partial_ref[row : row + 8, :], axis=1, keepdims=True
                    )

    def block(base, many):
        for g in range(many):
            here = pl.ds(base + 8 * g, 8)
            for j, (target_ref, columns_ref, before_ref, sources, after_ref) in enumerate(groups):
                if columns_ref is None:
                    target = [target_ref[r, here, :] for r in range(6)]
                else:
                    columns = columns_ref[here, :]
                    target = [jnp.broadcast_to(columns[:, r : r + 1], (8, 128)) for r in range(6)]
                    if target_ref is not None:
                        for r in range(6):
                            target_ref[r, here, :] = target[r]
                if before_ref is None:
                    sums = (jnp.zeros((8, 128), jnp.float32),) * 6
                else:
                    sums = tuple(before_ref[q, here, :] for q in range(6))
                for source_ref in sources:
                    for c in range(source_ref.shape[1] // 8):
                        source = [source_ref[r, 8 * c : 8 * (c + 1), :] for r in range(7)]
                        sums = pair_terms(source, target, sums)
                for q in range(6):
                    if finish:
                        row = ((g * len(groups) + j) * 6 + q) * 8
                        partial_ref[row : row + 8, :] = sums[q]
                    else:
                        after_ref[q, here, :] = sums[q]

    def body(step, unused):
        base = pl.multiple_of(start + step * lead, 8)
        if finish:
            reduce(base, together)
        block(base, together)
        return unused

    if finish:
        used = together * len(groups) * 48
        partial_ref[0:used, :] = jnp.zeros((used, 128), jnp.float32)
        if count < slots:
            sums_ref[...] = jnp.zeros_like(sums_ref)
    steps = count // lead
    lax.fori_loop(0, steps, body, 0)
    rest = (count - steps * lead) // 8
    end = start + steps * lead
    if finish:
        reduce(end, together)
    if rest:
        block(end, rest)
        if finish:
            reduce(end + lead, rest)
    if not finish:
        return None
    return [
        jnp.transpose(sums_ref[j * stride + lead : (j + 1) * stride, :])
        for j in range(len(groups))
    ]


def on_member(shares, run):
    member = lax.rem(lax.axis_index("act"), len(shares))
    for m in range(len(shares)):

        @pl.when(member == m)
        def _():
            run(sum(shares[:m]), shares[m])


def meet(slots, shares, known, fresh, *refs):
    every = known + fresh
    sent, refs = refs[:fresh], refs[fresh:]
    old_sources, old_targets, before = refs[:known], refs[known : 2 * known], refs[2 * known : 3 * known]
    refs = refs[3 * known :]
    new_sources, new_targets, after = refs[:fresh], refs[fresh : 2 * fresh], refs[2 * fresh : 2 * fresh + every]
    columns_ref = refs[2 * fresh + every]
    sources = old_sources + new_sources

    def run(start, count):
        groups = []
        for d in range(known):
            groups.append((old_targets[d], None, before[d], new_sources, after[d]))
        for d in range(fresh):
            spread_sources(sent[d][0:8, :], new_sources[d], 0)
            in_loop = None
            if known:
                in_loop = columns_ref
                columns_ref[...] = jnp.transpose(sent[d][0:8, 0:slots])
            else:
                spread_targets(sent[d][0:8, 0:slots], new_targets[d], start, count)
            groups.append((new_targets[d], in_loop, None, sources, after[known + d]))
        run_pairs(groups, slots, start, count, 2, False, None, None)

    on_member(shares, run)


def meet_own(slots, shares, sent_ref, own_target, own_before, *refs):
    known = len(refs) - 9
    sources = refs[:known]
    source_ref, own_ref, late_ref, target_ref, own_partial, own_sums, partial_ref, sums_ref, _ = refs[known:]
    spread_sources(sent_ref[0:8, :], source_ref, 0)

    def own(start, count):
        group = (own_target, None, own_before, (source_ref,), None)
        own_ref[...] = run_pairs(
            [group], slots, start, count, count // 8, True, own_partial, own_sums
        )[0]

    def late():
        group = (target_ref, None, None, sources + (source_ref,), None)
        late_ref[...] = run_pairs([group], slots, 0, slots, 4, True, partial_ref, sums_ref)[0]

    member = lax.rem(lax.axis_index("act"), 2)

    @pl.when(member == 0)
    def _():
        late_ref[...] = jnp.zeros_like(late_ref)
        own(0, shares[0])

    @pl.when(member == 1)
    def _():
        spread_targets(sent_ref[0:8, 0:slots], target_ref, 0, slots)
        own(shares[0], shares[1])
        late()


def meet_rest(slots, shares, source_ref, late_ref, *refs):
    known = (len(refs) - 3) // 2
    targets, before = refs[:known], refs[known : 2 * known]
    forces_ref, partial_ref, sums_ref = refs[2 * known :]

    def run(start, count):
        groups = [(t, None, b, (source_ref,), None) for t, b in zip(targets, before)]
        forces = run_pairs(groups, slots, start, count, 4, True, partial_ref, sums_ref)
        for d in range(known):
            forces_ref[:, d * slots : (d + 1) * slots] = forces[d]

    on_member(shares, run)
    forces_ref[:, known * slots : (known + 1) * slots] = late_ref[...]


def first_step(slots, sent, forces):
    size = sent.shape[1]
    across = size // slots
    old = [
        sent[14 + k // across : 15 + k // across, slots * (k % across) : slots * (k % across + 1)]
        for k in range(6)
    ]
    old = jnp.concatenate(old, axis=0)
    position, velocity = corrected(
        old[0:3], old[3:6], sent[0:3, 0:slots], sent[3:6, 0:slots], forces[0:3], forces[3:6]
    )
    ahead, speed = advance(position, velocity, forces[0:3], forces[3:6], fine_step)
    active = sent[7:8, 0:slots] > 0.5
    return jnp.where(active, jnp.concatenate([ahead, speed], axis=0), sent[8:14, 0:slots])


def meet_still(slots, shards, parts, *refs):
    sent, refs = refs[:shards], refs[shards:]
    shares, refs = refs[:parts], refs[parts:]
    own_ref, again_ref, target_ref, after_ref, still_ref = refs
    own_ref[...] = shares[0][...] + shares[1][...] if parts == 2 else shares[0][...]
    size = sent[0].shape[1]
    chunks = size // 128
    first = slots // 128
    again = first_step(slots, sent[0], own_ref[...])
    again = jnp.concatenate([again, jnp.zeros((2, slots), jnp.float32)], axis=0)
    again_ref[...] = again
    for d in range(shards):
        rows = jnp.concatenate([sent[d][8:14, slots:size], sent[d][6:8, slots:size]], axis=0)
        spread_sources(rows, still_ref, d * (chunks - first))
    spread_targets(again, target_ref, 0, slots)
    run_pairs(
        [(target_ref, None, None, (still_ref,), after_ref)], slots, 0, slots, 4, False, None, None
    )


def finish(slots, shards, parts, *refs):
    sent, refs = refs[:shards], refs[shards:]
    shares, refs = refs[:parts], refs[parts:]
    own_ref, again_ref, target_ref, before_ref, state_ref, place_ref, out_ref = refs[:7]
    later_ref, partial_ref, sums_ref = refs[7:]
    size = state_ref.shape[1]
    first = slots // 128
    own = again_ref[...]
    for d in range(shards):
        if d == 0:
            again = own[0:6]
        else:
            share = [s[:, (d - 1) * slots : d * slots] for s in shares]
            again = first_step(
                slots, sent[d], share[0] + share[1] if parts == 2 else share[0]
            )
        rows = jnp.concatenate([again, sent[d][6:8, 0:slots]], axis=0)
        spread_sources(rows, later_ref, d * first)
    second = run_pairs(
        [(target_ref, None, before_ref, (later_ref,), None)],
        slots,
        0,
        slots,
        8,
        True,
        partial_ref,
        sums_ref,
    )[0]
    before = own_ref[...]
    position, velocity = corrected(
        before[0:3], before[3:6], own[0:3], own[3:6], second[0:3], second[3:6]
    )
    new_rows = jnp.concatenate(
        [position, velocity, second[0:6], jnp.zeros((4, slots), jnp.float32)], axis=0
    )
    slot = lax.broadcasted_iota(jnp.int32, (slots, size), 0).astype(jnp.float32)
    chosen = jnp.where(slot == place_ref[0:1, :], 1.0, 0.0).astype(jnp.bfloat16)
    back = add_terms(jnp.dot(three_terms(new_rows), chosen, preferred_element_type=jnp.float32))
    out_ref[...] = jnp.where(place_ref[1:2, :] > 0.5, back[0:12], state_ref[...])


def direct_per_device(star_state, masses, phases, levels, active_list, active_count):
    del active_count
    size = star_state.shape[1]
    shards = lax.axis_size("src")
    slots = 2 * active_list.shape[0]
    whole = pl.BlockSpec(memory_space=pltpu.VMEM)
    message, place = pl.pallas_call(
        lambda *refs: prepare(slots, size * shards, *refs),
        out_shape=(
            jax.ShapeDtypeStruct((16, size), jnp.float32),
            jax.ShapeDtypeStruct((8, size), jnp.float32),
        ),
        in_specs=[pl.BlockSpec(memory_space=pltpu.HBM)] * 4,
        out_specs=(whole, whole),
        scratch_shapes=[
            pltpu.VMEM((12, size), jnp.float32),
            pltpu.VMEM((1, size), jnp.float32),
            pltpu.VMEM((1, size), jnp.float32),
            pltpu.VMEM((1, size), jnp.int32),
            pltpu.SemaphoreType.DMA((4,)),
        ],
        compiler_params=pltpu.CompilerParams(vmem_limit_bytes=16 * 2**20),
        name="prepare",
    )(
        *(
            pltpu.with_memory_space_constraint(x, pltpu.HBM)
            for x in (star_state, masses.reshape(1, size), phases.reshape(1, size), levels.reshape(1, size))
        )
    )
    sent = [message]
    for shift in range(1, shards):
        pairs = [(d, (d + shift) % shards) for d in range(shards)]
        sent.append(lax.ppermute(message, "src", pairs))

    limit = pltpu.CompilerParams(vmem_limit_bytes=16 * 2**20)
    owners = lax.axis_size("act")
    shares = (slots // 2, slots - slots // 2)
    parts = len(shares)

    def with_other(part):
        return [part, lax.ppermute(part, "act", [(i, i ^ 1) for i in range(owners)])]

    def call(body, operands, out_shape, scratch=(), pairs=0):
        cost = pl.CostEstimate(flops=41 * pairs, bytes_accessed=0, transcendentals=pairs)
        return pl.pallas_call(
            body,
            out_shape=out_shape,
            in_specs=[whole] * len(operands),
            out_specs=jax.tree.map(lambda _: whole, out_shape),
            scratch_shapes=list(scratch),
            compiler_params=limit,
            cost_estimate=cost if pairs else None,
        )(*operands)

    def rows(shape):
        return pltpu.VMEM(shape, jnp.float32)

    source_shape = jax.ShapeDtypeStruct((7, size // 16, 128), jnp.float32)
    target_shape = jax.ShapeDtypeStruct((6, slots, 128), jnp.float32)
    own_shape = jax.ShapeDtypeStruct((8, slots), jnp.float32)
    sources, targets, sums = [], [], []
    known = 0
    for fresh in [2] + [1] * (shards - 3):
        every = known + fresh
        outs = call(
            functools.partial(meet, slots, shares, known, fresh),
            [*sent[known:every], *sources, *targets, *sums],
            [source_shape] * fresh + [target_shape] * (fresh + every),
            [rows((slots, 8))],
        )
        sources += outs[:fresh]
        targets += outs[fresh : 2 * fresh]
        sums = list(outs[2 * fresh :])
        known = every
    source, own, late = call(
        functools.partial(meet_own, slots, shares),
        [sent[known], targets[0], sums[0], *sources],
        (source_shape, own_shape, own_shape),
        [
            rows(target_shape.shape),
            rows((max(shares) * 6, 128)),
            rows((slots + max(shares), 8)),
            rows((4 * 48, 128)),
            rows((slots + 32, 8)),
            rows((slots, 8)),
        ],
    )
    others = known - 1
    own = with_other(own)
    forces = call(
        functools.partial(meet_rest, slots, shares),
        [source, late, *targets[1:], *sums[1:]],
        jax.ShapeDtypeStruct((8, known * slots), jnp.float32),
        [rows((4 * others * 48, 128)), rows((others * (slots + 32), 8))],
        others * max(shares) * size,
    )
    forces = with_other(forces)
    first = slots // 128
    own, again, target, still = call(
        functools.partial(meet_still, slots, shards, parts),
        [*sent, *own],
        (own_shape, own_shape, target_shape, target_shape),
        [rows((7, shards * (size // 128 - first) * 8, 128))],
        slots * shards * (size - slots),
    )
    return call(
        functools.partial(finish, slots, shards, parts),
        [*sent, *forces, own, again, target, still, star_state, place],
        jax.ShapeDtypeStruct((12, size), jnp.float32),
        [rows((7, shards * first * 8, 128)), rows((8 * 48, 128)), rows((slots + 64, 8))],
    )


def solution(mesh):
    in_specs = (
        P(None, ("groups", "src")),
        P(("groups", "src")),
        P(("groups", "src")),
        P(("groups", "src")),
        P(("groups", "src", "act")),
        P(("groups", "src", "act")),
    )
    out_specs = P(None, ("groups", "src"))
    few = 3 <= mesh.shape["src"] <= MAX_DIRECT and mesh.shape["act"] % 2 == 0
    return jax.shard_map(
        direct_per_device if few else gather_per_device,
        mesh=mesh,
        in_specs=in_specs,
        out_specs=out_specs,
        check_vma=False,
    )
```

```python
import functools

import jax
import jax.numpy as jnp
from jax import lax
from jax.experimental import pallas as pl
from jax.experimental.pallas import tpu as pltpu
from jax.sharding import PartitionSpec as P


LEVELS = 5
STEPS = 2
MAX_DIRECT = 8


soften_sq = 0.0004
fine_step = 0.03125


def predict(star_state, elapsed):
    interval = elapsed[None, :]
    position = star_state[0:3] + interval * (
        star_state[3:6] + interval * (0.5 * star_state[6:9] + interval * star_state[9:12] / 6.0)
    )
    velocity = star_state[3:6] + interval * (star_state[6:9] + 0.5 * interval * star_state[9:12])
    return jnp.concatenate([position, velocity], axis=0)


def pair_block(targets, sources):
    delta_pos = sources[0:3, None, :] - targets[0:3, :, None]
    delta_vel = sources[3:6, None, :] - targets[3:6, :, None]
    dist_sq = (
        delta_pos[0] * delta_pos[0]
        + delta_pos[1] * delta_pos[1]
        + delta_pos[2] * delta_pos[2]
        + soften_sq
    )
    inverse = lax.rsqrt(dist_sq)
    inv_sq = inverse * inverse
    weight = sources[6][None, :] * inverse * inv_sq
    radial = (
        (delta_pos[0] * delta_vel[0] + delta_pos[1] * delta_vel[1] + delta_pos[2] * delta_vel[2])
        * inv_sq
        * 3.0
    )
    acceleration = jnp.sum(weight[None] * delta_pos, axis=2)
    jerk_sum = jnp.sum(weight[None] * (delta_vel - radial[None] * delta_pos), axis=2)
    return jnp.concatenate([acceleration, jerk_sum], axis=0)


def over_sources(targets, sources):
    count_src = sources.shape[1]
    width = 512
    blocks = sources.reshape(7, count_src // width, width).transpose(1, 0, 2)

    def accumulate(running, portion):
        return (running + pair_block(targets, portion), None)

    init = jnp.zeros((6, targets.shape[1]), jnp.float32)
    running, _ = lax.scan(accumulate, init, blocks)
    return running


def corrected(acc_old, jerk_old, position, velocity, acc_new, jerk_new):
    snap_term = (-6.0 * (acc_old - acc_new) - fine_step * (4.0 * jerk_old + 2.0 * jerk_new)) / (
        fine_step * fine_step
    )
    crackle = (12.0 * (acc_old - acc_new) + 6.0 * fine_step * (jerk_old + jerk_new)) / (
        fine_step * fine_step * fine_step
    )
    new_position = position + fine_step**4 / 24.0 * snap_term + fine_step**5 / 120.0 * crackle
    new_velocity = velocity + fine_step**3 / 6.0 * snap_term + fine_step**4 / 24.0 * crackle
    return new_position, new_velocity


def correct(old_state, predicted_rows, forces):
    new_position, new_velocity = corrected(
        old_state[6:9],
        old_state[9:12],
        predicted_rows[0:3],
        predicted_rows[3:6],
        forces[0:3],
        forces[3:6],
    )
    return jnp.concatenate([new_position, new_velocity, forces], axis=0)


def gather_per_device(star_state, masses, phases, levels, active_list, active_count):
    shard_size = star_state.shape[1]
    total_stars = shard_size * lax.axis_size("src")
    weights = masses / total_stars
    slot_count = active_list.shape[0]
    live = jnp.arange(slot_count, dtype=jnp.int32) < active_count[0]
    write_index = jnp.where(live, active_list, shard_size)
    tick_count = jnp.left_shift(jnp.int32(1), LEVELS - 1 - levels).astype(jnp.float32)
    state_now = star_state
    for substep in range(STEPS):
        elapsed = (
            jnp.where(levels == LEVELS - 1, 1.0, phases * (tick_count - STEPS) + (substep + 1))
            * fine_step
        )
        predicted = predict(state_now, elapsed)
        sources = jnp.concatenate([predicted, weights[None, :]], axis=0)
        targets = predicted[:, active_list]
        forces = over_sources(targets, lax.all_gather(sources, "src", axis=1, tiled=True))
        new_state = correct(state_now[:, active_list], targets, forces)
        all_new, all_index = (
            lax.all_gather(new_state, "act", axis=1, tiled=True),
            lax.all_gather(write_index, "act", axis=0, tiled=True),
        )
        state_now = state_now.at[:, all_index].set(all_new, mode="drop")
    return state_now


def three_terms(x):
    high = x.astype(jnp.bfloat16)
    rest = x - high.astype(jnp.float32)
    middle = rest.astype(jnp.bfloat16)
    low = (rest - middle.astype(jnp.float32)).astype(jnp.bfloat16)
    return jnp.concatenate([high, middle, low], axis=0)


def add_terms(y):
    rows = y.shape[0] // 3
    return (y[0:rows] + y[rows : 2 * rows]) + y[2 * rows : 3 * rows]


def advance(position, velocity, acceleration, jerk, step):
    ahead = position + step * (velocity + step * (0.5 * acceleration + step * jerk / 6.0))
    speed = velocity + step * (acceleration + 0.5 * step * jerk)
    return ahead, speed


def prepare(slots, total_stars, *refs):
    out_ref, place_ref = refs[4:6]
    copies = [
        pltpu.make_async_copy(far, near, refs[10].at[k])
        for k, (far, near) in enumerate(zip(refs[0:4], refs[6:10]))
    ]
    for copy in copies:
        copy.start()
    for copy in copies:
        copy.wait()
    state_ref, mass_ref, phase_ref, level_ref = refs[6:10]
    size = state_ref.shape[1]
    level = level_ref[...]
    active = level == LEVELS - 1
    mask = jnp.where(active, 1.0, 0.0)
    blocks = size // 128
    grouped = jnp.concatenate(
        [mask[:, 128 * b : 128 * (b + 1)] for b in range(blocks)]
        + [jnp.zeros((16 - blocks, 128), jnp.float32)],
        axis=0,
    ).astype(jnp.bfloat16)
    lane_in = lax.broadcasted_iota(jnp.int32, (128, 256), 0)
    lane_out = lax.broadcasted_iota(jnp.int32, (128, 256), 1)
    counting = jnp.where((lane_in <= lane_out) | (lane_out >= 128), 1.0, 0.0).astype(jnp.bfloat16)
    counts = jnp.dot(grouped, counting, preferred_element_type=jnp.float32)
    so_far = []
    before = jnp.zeros((1, 128), jnp.float32)
    for b in range(blocks):
        so_far.append(counts[b : b + 1, 0:128] + before)
        before = before + counts[b : b + 1, 128:256]
    rank = jnp.concatenate(so_far, axis=1)
    total = jnp.concatenate([before] * blocks, axis=1)
    star = lax.broadcasted_iota(jnp.int32, (1, size), 1).astype(jnp.float32)
    place = jnp.where(active, rank - 1.0, total + star - rank)
    place_ref[0:1, :] = place
    place_ref[1:2, :] = mask
    place_ref[2:8, :] = jnp.zeros((6, size), jnp.float32)

    tick_count = jnp.left_shift(jnp.int32(1), LEVELS - 1 - level).astype(jnp.float32)
    offset = phase_ref[...] * (tick_count - STEPS)
    position, velocity = state_ref[0:3, :], state_ref[3:6, :]
    acceleration, jerk = state_ref[6:9, :], state_ref[9:12, :]
    rows = []
    for substep in range(STEPS):
        elapsed = jnp.where(active, 1.0, offset + (substep + 1)) * fine_step
        rows.extend(advance(position, velocity, acceleration, jerk, elapsed))
        if substep == 0:
            rows.append(mass_ref[...] / total_stars)
            rows.append(mask)
    rows.append(jnp.zeros((2, size), jnp.float32))
    rows.extend([acceleration, jerk, jnp.zeros((10, size), jnp.float32)])
    terms = three_terms(jnp.concatenate(rows, axis=0))
    slot = lax.broadcasted_iota(jnp.int32, (size, size), 0).astype(jnp.float32)
    chosen = jnp.where(slot == place, 1.0, 0.0).astype(jnp.bfloat16)
    moved = add_terms(
        lax.dot_general(
            terms, chosen, (((1,), (1,)), ((), ())), preferred_element_type=jnp.float32
        )
    )
    out_ref[...] = moved[0:16]
    across = size // slots
    for k in range(6):
        out_ref[14 + k // across : 15 + k // across, slots * (k % across) : slots * (k % across + 1)] = (
            moved[16 + k : 17 + k, 0:slots]
        )


def pair_terms(source, target, sums):
    sx, sy, sz, su, sv, sw, weight = source
    tx, ty, tz, tu, tv, tw = target
    dx, dy, dz = sx - tx, sy - ty, sz - tz
    du, dv, dw = su - tu, sv - tv, sw - tw
    inverse = lax.rsqrt(dx * dx + dy * dy + (dz * dz + soften_sq))
    inv_sq = inverse * inverse
    pull = weight * inverse * inv_sq
    radial = (dx * du + dy * dv + dz * dw) * (inv_sq * 3.0)
    ax, ay, az, jx, jy, jz = sums
    return (
        ax + pull * dx,
        ay + pull * dy,
        az + pull * dz,
        jx + pull * (du - radial * dx),
        jy + pull * (dv - radial * dy),
        jz + pull * (dw - radial * dz),
    )


def spread_sources(rows, spread_ref, first):
    for c in range(rows.shape[1] // 128):
        for r in range(7):
            spread_ref[r, 8 * (first + c) : 8 * (first + c + 1), :] = jnp.broadcast_to(
                rows[r : r + 1, 128 * c : 128 * (c + 1)], (8, 128)
            )


def spread_targets(rows, spread_ref, start, count):
    columns = jnp.transpose(rows)
    for r in range(6):
        spread_ref[r, start : start + count, :] = jnp.broadcast_to(
            columns[start : start + count, r : r + 1], (count, 128)
        )


def run_pairs(groups, slots, start, count, together, finish, partial_ref, sums_ref):
    lead = 8 * together
    stride = slots + lead

    def reduce(place, many):
        for g in range(many):
            for j in range(len(groups)):
                for q in range(6):
                    row = ((g * len(groups) + j) * 6 + q) * 8
                    sums_ref[pl.ds(j * stride + place + 8 * g, 8), q : q + 1] = jnp.sum(
                        partial_ref[row : row + 8, :], axis=1, keepdims=True
                    )

    def block(base, many):
        for g in range(many):
            here = pl.ds(base + 8 * g, 8)
            for j, (target_ref, columns_ref, before_ref, sources, after_ref) in enumerate(groups):
                if columns_ref is None:
                    target = [target_ref[r, here, :] for r in range(6)]
                else:
                    columns = columns_ref[here, :]
                    target = [jnp.broadcast_to(columns[:, r : r + 1], (8, 128)) for r in range(6)]
                    if target_ref is not None:
                        for r in range(6):
                            target_ref[r, here, :] = target[r]
                if before_ref is None:
                    sums = (jnp.zeros((8, 128), jnp.float32),) * 6
                else:
                    sums = tuple(before_ref[q, here, :] for q in range(6))
                for source_ref in sources:
                    for c in range(source_ref.shape[1] // 8):
                        source = [source_ref[r, 8 * c : 8 * (c + 1), :] for r in range(7)]
                        sums = pair_terms(source, target, sums)
                for q in range(6):
                    if finish:
                        row = ((g * len(groups) + j) * 6 + q) * 8
                        partial_ref[row : row + 8, :] = sums[q]
                    else:
                        after_ref[q, here, :] = sums[q]

    def body(step, unused):
        base = pl.multiple_of(start + step * lead, 8)
        if finish:
            reduce(base, together)
        block(base, together)
        return unused

    if finish:
        used = together * len(groups) * 48
        partial_ref[0:used, :] = jnp.zeros((used, 128), jnp.float32)
        if count < slots:
            sums_ref[...] = jnp.zeros_like(sums_ref)
    steps = count // lead
    lax.fori_loop(0, steps, body, 0)
    rest = (count - steps * lead) // 8
    end = start + steps * lead
    if finish:
        reduce(end, together)
    if rest:
        block(end, rest)
        if finish:
            reduce(end + lead, rest)
    if not finish:
        return None
    return [
        jnp.transpose(sums_ref[j * stride + lead : (j + 1) * stride, :])
        for j in range(len(groups))
    ]


def on_member(shares, run):
    member = lax.rem(lax.axis_index("act"), len(shares))
    for m in range(len(shares)):

        @pl.when(member == m)
        def _():
            run(sum(shares[:m]), shares[m])


def meet(slots, shares, known, fresh, *refs):
    every = known + fresh
    sent, refs = refs[:fresh], refs[fresh:]
    old_sources, old_targets, before = refs[:known], refs[known : 2 * known], refs[2 * known : 3 * known]
    refs = refs[3 * known :]
    new_sources, new_targets, after = refs[:fresh], refs[fresh : 2 * fresh], refs[2 * fresh : 2 * fresh + every]
    columns_ref = refs[2 * fresh + every]
    sources = old_sources + new_sources

    def run(start, count):
        groups = []
        for d in range(known):
            groups.append((old_targets[d], None, before[d], new_sources, after[d]))
        for d in range(fresh):
            spread_sources(sent[d][0:8, :], new_sources[d], 0)
            in_loop = None
            if known:
                in_loop = columns_ref
                columns_ref[...] = jnp.transpose(sent[d][0:8, 0:slots])
            else:
                spread_targets(sent[d][0:8, 0:slots], new_targets[d], start, count)
            groups.append((new_targets[d], in_loop, None, sources, after[known + d]))
        run_pairs(groups, slots, start, count, 2, False, None, None)

    on_member(shares, run)


def meet_own(slots, shares, early, sent_ref, own_target, own_before, *refs):
    known = len(refs) - 8
    sources = refs[:known]
    source_ref, own_ref, late_ref, target_ref, own_partial, own_sums, partial_ref, sums_ref = refs[known:]
    spread_sources(sent_ref[0:8, :], source_ref, 0)

    def own(start, count):
        group = (own_target, None, own_before, (source_ref,), None)
        own_ref[...] = run_pairs(
            [group], slots, start, count, count // 8, True, own_partial, own_sums
        )[0]

    member = lax.rem(lax.axis_index("act"), 2)

    @pl.when(member == 0)
    def _():
        late_ref[...] = jnp.zeros_like(late_ref)
        spread_targets(sent_ref[0:8, 0:slots], target_ref, early, slots - early)
        own(0, shares[0])

    @pl.when(member == 1)
    def _():
        spread_targets(sent_ref[0:8, 0:slots], target_ref, 0, slots)
        own(shares[0], shares[1])
        group = (target_ref, None, None, sources + (source_ref,), None)
        late_ref[...] = run_pairs([group], slots, 0, early, 4, True, partial_ref, sums_ref)[0]


def meet_rest(slots, shares, early, source_ref, late_ref, late_target, *refs):
    known = (len(refs) - 4) // 3
    sources, targets, before = refs[: known + 1], refs[known + 1 : 2 * known + 1], refs[2 * known + 1 : 3 * known + 1]
    forces_ref, partial_ref, sums_ref = refs[3 * known + 1 :]
    half = (slots - early) // 2
    used = half * 6

    def run(start, count):
        group = (late_target, None, None, sources + (source_ref,), None)
        first = early if start == 0 else early + half
        late = run_pairs(
            [group],
            slots,
            first,
            half,
            half // 8,
            True,
            partial_ref.at[0:used],
            sums_ref.at[0 : slots + half],
        )[0]
        forces_ref[:, known * slots : (known + 1) * slots] = late_ref[...] + late
        groups = [(t, None, b, (source_ref,), None) for t, b in zip(targets, before)]
        forces = run_pairs(
            groups,
            slots,
            start,
            count,
            count // 8,
            True,
            partial_ref.at[used : used + count * known * 6],
            sums_ref.at[slots + half : slots + half + known * (slots + count)],
        )
        for d in range(known):
            forces_ref[:, d * slots : (d + 1) * slots] = forces[d]

    on_member(shares, run)


def first_step(slots, sent, forces):
    size = sent.shape[1]
    across = size // slots
    old = [
        sent[14 + k // across : 15 + k // across, slots * (k % across) : slots * (k % across + 1)]
        for k in range(6)
    ]
    old = jnp.concatenate(old, axis=0)
    position, velocity = corrected(
        old[0:3], old[3:6], sent[0:3, 0:slots], sent[3:6, 0:slots], forces[0:3], forces[3:6]
    )
    ahead, speed = advance(position, velocity, forces[0:3], forces[3:6], fine_step)
    active = sent[7:8, 0:slots] > 0.5
    return jnp.where(active, jnp.concatenate([ahead, speed], axis=0), sent[8:14, 0:slots])


def meet_still(slots, shards, parts, *refs):
    sent, refs = refs[:shards], refs[shards:]
    shares, refs = refs[:parts], refs[parts:]
    own_ref, again_ref, target_ref, after_ref, still_ref = refs
    own_ref[...] = shares[0][...] + shares[1][...] if parts == 2 else shares[0][...]
    size = sent[0].shape[1]
    chunks = size // 128
    first = slots // 128
    again = first_step(slots, sent[0], own_ref[...])
    again = jnp.concatenate([again, jnp.zeros((2, slots), jnp.float32)], axis=0)
    again_ref[...] = again
    for d in range(shards):
        rows = jnp.concatenate([sent[d][8:14, slots:size], sent[d][6:8, slots:size]], axis=0)
        spread_sources(rows, still_ref, d * (chunks - first))
    spread_targets(again, target_ref, 0, slots)
    run_pairs(
        [(target_ref, None, None, (still_ref,), after_ref)], slots, 0, slots, 4, False, None, None
    )


def finish(slots, shards, parts, *refs):
    sent, refs = refs[:shards], refs[shards:]
    shares, refs = refs[:parts], refs[parts:]
    own_ref, again_ref, target_ref, before_ref, state_ref, place_ref, out_ref = refs[:7]
    later_ref, partial_ref, sums_ref = refs[7:]
    size = state_ref.shape[1]
    first = slots // 128
    own = again_ref[...]
    for d in range(shards):
        if d == 0:
            again = own[0:6]
        else:
            share = [s[:, (d - 1) * slots : d * slots] for s in shares]
            again = first_step(
                slots, sent[d], share[0] + share[1] if parts == 2 else share[0]
            )
        rows = jnp.concatenate([again, sent[d][6:8, 0:slots]], axis=0)
        spread_sources(rows, later_ref, d * first)
    second = run_pairs(
        [(target_ref, None, before_ref, (later_ref,), None)],
        slots,
        0,
        slots,
        8,
        True,
        partial_ref,
        sums_ref,
    )[0]
    before = own_ref[...]
    position, velocity = corrected(
        before[0:3], before[3:6], own[0:3], own[3:6], second[0:3], second[3:6]
    )
    new_rows = jnp.concatenate(
        [position, velocity, second[0:6], jnp.zeros((4, slots), jnp.float32)], axis=0
    )
    slot = lax.broadcasted_iota(jnp.int32, (slots, size), 0).astype(jnp.float32)
    chosen = jnp.where(slot == place_ref[0:1, :], 1.0, 0.0).astype(jnp.bfloat16)
    back = add_terms(jnp.dot(three_terms(new_rows), chosen, preferred_element_type=jnp.float32))
    out_ref[...] = jnp.where(place_ref[1:2, :] > 0.5, back[0:12], state_ref[...])


def direct_per_device(star_state, masses, phases, levels, active_list, active_count):
    del active_count
    size = star_state.shape[1]
    shards = lax.axis_size("src")
    slots = 2 * active_list.shape[0]
    whole = pl.BlockSpec(memory_space=pltpu.VMEM)
    message, place = pl.pallas_call(
        lambda *refs: prepare(slots, size * shards, *refs),
        out_shape=(
            jax.ShapeDtypeStruct((16, size), jnp.float32),
            jax.ShapeDtypeStruct((8, size), jnp.float32),
        ),
        in_specs=[pl.BlockSpec(memory_space=pltpu.HBM)] * 4,
        out_specs=(whole, whole),
        scratch_shapes=[
            pltpu.VMEM((12, size), jnp.float32),
            pltpu.VMEM((1, size), jnp.float32),
            pltpu.VMEM((1, size), jnp.float32),
            pltpu.VMEM((1, size), jnp.int32),
            pltpu.SemaphoreType.DMA((4,)),
        ],
        compiler_params=pltpu.CompilerParams(vmem_limit_bytes=16 * 2**20),
        name="prepare",
    )(
        *(
            pltpu.with_memory_space_constraint(x, pltpu.HBM)
            for x in (star_state, masses.reshape(1, size), phases.reshape(1, size), levels.reshape(1, size))
        )
    )
    sent = [message]
    for shift in range(1, shards):
        pairs = [(d, (d + shift) % shards) for d in range(shards)]
        sent.append(lax.ppermute(message, "src", pairs))

    limit = pltpu.CompilerParams(vmem_limit_bytes=16 * 2**20)
    owners = lax.axis_size("act")
    shares = (slots // 2, slots - slots // 2)
    parts = len(shares)

    def with_other(part):
        return [part, lax.ppermute(part, "act", [(i, i ^ 1) for i in range(owners)])]

    def call(body, operands, out_shape, scratch=(), pairs=0):
        cost = pl.CostEstimate(flops=41 * pairs, bytes_accessed=0, transcendentals=pairs)
        return pl.pallas_call(
            body,
            out_shape=out_shape,
            in_specs=[whole] * len(operands),
            out_specs=jax.tree.map(lambda _: whole, out_shape),
            scratch_shapes=list(scratch),
            compiler_params=limit,
            cost_estimate=cost if pairs else None,
        )(*operands)

    def rows(shape):
        return pltpu.VMEM(shape, jnp.float32)

    source_shape = jax.ShapeDtypeStruct((7, size // 16, 128), jnp.float32)
    target_shape = jax.ShapeDtypeStruct((6, slots, 128), jnp.float32)
    own_shape = jax.ShapeDtypeStruct((8, slots), jnp.float32)
    sources, targets, sums = [], [], []
    known = 0
    for fresh in [2] + [1] * (shards - 3):
        every = known + fresh
        outs = call(
            functools.partial(meet, slots, shares, known, fresh),
            [*sent[known:every], *sources, *targets, *sums],
            [source_shape] * fresh + [target_shape] * (fresh + every),
            [rows((slots, 8))],
        )
        sources += outs[:fresh]
        targets += outs[fresh : 2 * fresh]
        sums = list(outs[2 * fresh :])
        known = every
    early = slots * 3 // 4
    source, own, late, late_target = call(
        functools.partial(meet_own, slots, shares, early),
        [sent[known], targets[0], sums[0], *sources],
        (source_shape, own_shape, own_shape, target_shape),
        [
            rows((max(shares) * 6, 128)),
            rows((slots + max(shares), 8)),
            rows((4 * 48, 128)),
            rows((slots + 32, 8)),
        ],
    )
    others = known - 1
    half = (slots - early) // 2
    own = with_other(own)
    forces = call(
        functools.partial(meet_rest, slots, shares, early),
        [source, late, late_target, *sources, *targets[1:], *sums[1:]],
        jax.ShapeDtypeStruct((8, known * slots), jnp.float32),
        [
            rows((half * 6 + max(shares) * others * 6, 128)),
            rows((slots + half + others * (slots + max(shares)), 8)),
        ],
        others * max(shares) * size,
    )
    forces = with_other(forces)
    first = slots // 128
    own, again, target, still = call(
        functools.partial(meet_still, slots, shards, parts),
        [*sent, *own],
        (own_shape, own_shape, target_shape, target_shape),
        [rows((7, shards * (size // 128 - first) * 8, 128))],
        slots * shards * (size - slots),
    )
    return call(
        functools.partial(finish, slots, shards, parts),
        [*sent, *forces, own, again, target, still, star_state, place],
        jax.ShapeDtypeStruct((12, size), jnp.float32),
        [rows((7, shards * first * 8, 128)), rows((8 * 48, 128)), rows((slots + 64, 8))],
    )


def solution(mesh):
    in_specs = (
        P(None, ("groups", "src")),
        P(("groups", "src")),
        P(("groups", "src")),
        P(("groups", "src")),
        P(("groups", "src", "act")),
        P(("groups", "src", "act")),
    )
    out_specs = P(None, ("groups", "src"))
    few = 3 <= mesh.shape["src"] <= MAX_DIRECT and mesh.shape["act"] % 2 == 0
    return jax.shard_map(
        direct_per_device if few else gather_per_device,
        mesh=mesh,
        in_specs=in_specs,
        out_specs=out_specs,
        check_vma=False,
    )
```

```python
import functools

import jax
import jax.numpy as jnp
from jax import lax
from jax.experimental import pallas as pl
from jax.experimental.pallas import tpu as pltpu
from jax.sharding import PartitionSpec as P

LEVELS = 5
STEPS = 2
MAX_DIRECT = 8


soften_sq = 0.0004
fine_step = 0.03125


def predict(star_state, elapsed):
    interval = elapsed[None, :]
    position = star_state[0:3] + interval * (
        star_state[3:6] + interval * (0.5 * star_state[6:9] + interval * star_state[9:12] / 6.0)
    )
    velocity = star_state[3:6] + interval * (star_state[6:9] + 0.5 * interval * star_state[9:12])
    return jnp.concatenate([position, velocity], axis=0)


def pair_block(targets, sources):
    delta_pos = sources[0:3, None, :] - targets[0:3, :, None]
    delta_vel = sources[3:6, None, :] - targets[3:6, :, None]
    dist_sq = (
        delta_pos[0] * delta_pos[0]
        + delta_pos[1] * delta_pos[1]
        + delta_pos[2] * delta_pos[2]
        + soften_sq
    )
    inverse = lax.rsqrt(dist_sq)
    inv_sq = inverse * inverse
    weight = sources[6][None, :] * inverse * inv_sq
    radial = (
        (delta_pos[0] * delta_vel[0] + delta_pos[1] * delta_vel[1] + delta_pos[2] * delta_vel[2])
        * inv_sq
        * 3.0
    )
    acceleration = jnp.sum(weight[None] * delta_pos, axis=2)
    jerk_sum = jnp.sum(weight[None] * (delta_vel - radial[None] * delta_pos), axis=2)
    return jnp.concatenate([acceleration, jerk_sum], axis=0)


def over_sources(targets, sources):
    count_src = sources.shape[1]
    width = 512
    blocks = sources.reshape(7, count_src // width, width).transpose(1, 0, 2)

    def accumulate(running, portion):
        return (running + pair_block(targets, portion), None)

    init = jnp.zeros((6, targets.shape[1]), jnp.float32)
    running, unused = lax.scan(accumulate, init, blocks)
    return running


def corrected(acc_old, jerk_old, position, velocity, acc_new, jerk_new):
    snap_term = (-6.0 * (acc_old - acc_new) - fine_step * (4.0 * jerk_old + 2.0 * jerk_new)) / (
        fine_step * fine_step
    )
    crackle = (12.0 * (acc_old - acc_new) + 6.0 * fine_step * (jerk_old + jerk_new)) / (
        fine_step * fine_step * fine_step
    )
    new_position = position + fine_step**4 / 24.0 * snap_term + fine_step**5 / 120.0 * crackle
    new_velocity = velocity + fine_step**3 / 6.0 * snap_term + fine_step**4 / 24.0 * crackle
    return new_position, new_velocity


def correct(old_state, predicted_rows, forces):
    new_position, new_velocity = corrected(
        old_state[6:9],
        old_state[9:12],
        predicted_rows[0:3],
        predicted_rows[3:6],
        forces[0:3],
        forces[3:6],
    )
    return jnp.concatenate([new_position, new_velocity, forces], axis=0)


def gather_per_device(star_state, masses, phases, levels, active_list, active_count):
    shard_size = star_state.shape[1]
    total_stars = shard_size * lax.axis_size("src")
    weights = masses / total_stars
    slot_count = active_list.shape[0]
    live = jnp.arange(slot_count, dtype=jnp.int32) < active_count[0]
    write_index = jnp.where(live, active_list, shard_size)
    tick_count = jnp.left_shift(jnp.int32(1), LEVELS - 1 - levels).astype(jnp.float32)
    state_now = star_state
    for substep in range(STEPS):
        elapsed = (
            jnp.where(levels == LEVELS - 1, 1.0, phases * (tick_count - STEPS) + (substep + 1))
            * fine_step
        )
        predicted = predict(state_now, elapsed)
        sources = jnp.concatenate([predicted, weights[None, :]], axis=0)
        targets = predicted[:, active_list]
        forces = over_sources(targets, lax.all_gather(sources, "src", axis=1, tiled=True))
        new_state = correct(state_now[:, active_list], targets, forces)
        all_new, all_index = (
            lax.all_gather(new_state, "act", axis=1, tiled=True),
            lax.all_gather(write_index, "act", axis=0, tiled=True),
        )
        state_now = state_now.at[:, all_index].set(all_new, mode="drop")
    return state_now


def three_terms(x):
    high = x.astype(jnp.bfloat16)
    rest = x - high.astype(jnp.float32)
    middle = rest.astype(jnp.bfloat16)
    low = (rest - middle.astype(jnp.float32)).astype(jnp.bfloat16)
    return jnp.concatenate([high, middle, low], axis=0)


def add_terms(y):
    rows = y.shape[0] // 3
    return (y[0:rows] + y[rows : 2 * rows]) + y[2 * rows : 3 * rows]


def advance(position, velocity, acceleration, jerk, step):
    ahead = position + step * (velocity + step * (0.5 * acceleration + step * jerk / 6.0))
    speed = velocity + step * (acceleration + 0.5 * step * jerk)
    return ahead, speed


def prepare(slots, total_stars, *refs):
    out_ref, place_ref = refs[4:6]
    copies = [
        pltpu.make_async_copy(far, near, refs[10].at[k])
        for k, (far, near) in enumerate(zip(refs[0:4], refs[6:10]))
    ]
    for copy in copies:
        copy.start()
    for copy in copies:
        copy.wait()
    state_ref, mass_ref, phase_ref, level_ref = refs[6:10]
    size = state_ref.shape[1]
    level = level_ref[...]
    active = level == LEVELS - 1
    mask = jnp.where(active, 1.0, 0.0)
    blocks = size // 128
    grouped = jnp.concatenate(
        [mask[:, 128 * b : 128 * (b + 1)] for b in range(blocks)]
        + [jnp.zeros((16 - blocks, 128), jnp.float32)],
        axis=0,
    ).astype(jnp.bfloat16)
    lane_in = lax.broadcasted_iota(jnp.int32, (128, 256), 0)
    lane_out = lax.broadcasted_iota(jnp.int32, (128, 256), 1)
    counting = jnp.where((lane_in <= lane_out) | (lane_out >= 128), 1.0, 0.0).astype(jnp.bfloat16)
    counts = jnp.dot(grouped, counting, preferred_element_type=jnp.float32)
    so_far = []
    before = jnp.zeros((1, 128), jnp.float32)
    for b in range(blocks):
        so_far.append(counts[b : b + 1, 0:128] + before)
        before = before + counts[b : b + 1, 128:256]
    rank = jnp.concatenate(so_far, axis=1)
    total = jnp.concatenate([before] * blocks, axis=1)
    star = lax.broadcasted_iota(jnp.int32, (1, size), 1).astype(jnp.float32)
    place = jnp.where(active, rank - 1.0, total + star - rank)
    place_ref[0:1, :] = place
    place_ref[1:2, :] = mask
    place_ref[2:8, :] = jnp.zeros((6, size), jnp.float32)

    tick_count = jnp.left_shift(jnp.int32(1), LEVELS - 1 - level).astype(jnp.float32)
    offset = phase_ref[...] * (tick_count - STEPS)
    position, velocity = state_ref[0:3, :], state_ref[3:6, :]
    acceleration, jerk = state_ref[6:9, :], state_ref[9:12, :]
    rows = []
    for substep in range(STEPS):
        elapsed = jnp.where(active, 1.0, offset + (substep + 1)) * fine_step
        rows.extend(advance(position, velocity, acceleration, jerk, elapsed))
        if substep == 0:
            rows.append(mass_ref[...] / total_stars)
            rows.append(mask)
    rows.append(jnp.zeros((2, size), jnp.float32))
    rows.extend([acceleration, jerk, jnp.zeros((10, size), jnp.float32)])
    terms = three_terms(jnp.concatenate(rows, axis=0))
    slot = lax.broadcasted_iota(jnp.int32, (size, size), 0).astype(jnp.float32)
    chosen = jnp.where(slot == place, 1.0, 0.0).astype(jnp.bfloat16)
    moved = add_terms(
        lax.dot_general(
            terms, chosen, (((1,), (1,)), ((), ())), preferred_element_type=jnp.float32
        )
    )
    out_ref[...] = moved[0:16]
    across = size // slots
    for k in range(6):
        out_ref[14 + k // across : 15 + k // across, slots * (k % across) : slots * (k % across + 1)] = (
            moved[16 + k : 17 + k, 0:slots]
        )


def pair_terms(source, target, sums):
    sx, sy, sz, su, sv, sw, weight = source
    tx, ty, tz, tu, tv, tw = target
    dx, dy, dz = sx - tx, sy - ty, sz - tz
    du, dv, dw = su - tu, sv - tv, sw - tw
    inverse = lax.rsqrt(dx * dx + dy * dy + (dz * dz + soften_sq))
    inv_sq = inverse * inverse
    pull = weight * inverse * inv_sq
    radial = (dx * du + dy * dv + dz * dw) * (inv_sq * 3.0)
    ax, ay, az, jx, jy, jz = sums
    return (
        ax + pull * dx,
        ay + pull * dy,
        az + pull * dz,
        jx + pull * (du - radial * dx),
        jy + pull * (dv - radial * dy),
        jz + pull * (dw - radial * dz),
    )


def spread_sources(rows, spread_ref, first):
    for c in range(rows.shape[1] // 128):
        for r in range(7):
            spread_ref[r, 8 * (first + c) : 8 * (first + c + 1), :] = jnp.broadcast_to(
                rows[r : r + 1, 128 * c : 128 * (c + 1)], (8, 128)
            )


def spread_targets(rows, spread_ref, start, count):
    columns = jnp.transpose(rows)
    for r in range(6):
        spread_ref[r, start : start + count, :] = jnp.broadcast_to(
            columns[start : start + count, r : r + 1], (count, 128)
        )


def run_pairs(groups, slots, start, count, together, finish, partial_ref, sums_ref):
    lead = 8 * together
    stride = slots + lead

    def reduce(place, many):
        for g in range(many):
            for j in range(len(groups)):
                for q in range(6):
                    row = ((g * len(groups) + j) * 6 + q) * 8
                    sums_ref[pl.ds(j * stride + place + 8 * g, 8), q : q + 1] = jnp.sum(
                        partial_ref[row : row + 8, :], axis=1, keepdims=True
                    )

    def block(base, many):
        for g in range(many):
            here = pl.ds(base + 8 * g, 8)
            for j, (target_ref, columns_ref, before_ref, sources, after_ref) in enumerate(groups):
                if columns_ref is None:
                    target = [target_ref[r, here, :] for r in range(6)]
                else:
                    columns = columns_ref[here, :]
                    target = [jnp.broadcast_to(columns[:, r : r + 1], (8, 128)) for r in range(6)]
                    if target_ref is not None:
                        for r in range(6):
                            target_ref[r, here, :] = target[r]
                if before_ref is None:
                    sums = (jnp.zeros((8, 128), jnp.float32),) * 6
                else:
                    sums = tuple(before_ref[q, here, :] for q in range(6))
                for source_ref in sources:
                    for c in range(source_ref.shape[1] // 8):
                        source = [source_ref[r, 8 * c : 8 * (c + 1), :] for r in range(7)]
                        sums = pair_terms(source, target, sums)
                for q in range(6):
                    if finish:
                        row = ((g * len(groups) + j) * 6 + q) * 8
                        partial_ref[row : row + 8, :] = sums[q]
                    else:
                        after_ref[q, here, :] = sums[q]

    def body(step, unused):
        base = pl.multiple_of(start + step * lead, 8)
        if finish:
            reduce(base, together)
        block(base, together)
        return unused

    if finish:
        used = together * len(groups) * 48
        partial_ref[0:used, :] = jnp.zeros((used, 128), jnp.float32)
        if count < slots:
            sums_ref[...] = jnp.zeros_like(sums_ref)
    steps = count // lead
    lax.fori_loop(0, steps, body, 0)
    rest = (count - steps * lead) // 8
    end = start + steps * lead
    if finish:
        reduce(end, together)
    if rest:
        block(end, rest)
        if finish:
            reduce(end + lead, rest)
    if not finish:
        return None
    return [
        jnp.transpose(sums_ref[j * stride + lead : (j + 1) * stride, :])
        for j in range(len(groups))
    ]


def meet(slots, shares, late_shares, known, fresh, last, *refs):
    every = known + fresh
    sent, refs = refs[:fresh], refs[fresh:]
    old_sources, old_targets, before = refs[:known], refs[known : 2 * known], refs[2 * known : 3 * known]
    refs = refs[3 * known :]
    own_ref = forces_ref = own_partial = own_sums = partial_ref = sums_ref = None
    if last:
        own_ref, forces_ref, refs = refs[0], refs[1], refs[2:]
        new_sources, new_targets, refs = refs[:fresh], refs[fresh : 2 * fresh], refs[2 * fresh :]
        after = (None,) * every
        columns_ref, own_partial, own_sums, partial_ref, sums_ref, late_partial, late_sums = refs
    else:
        new_sources, new_targets, after = refs[:fresh], refs[fresh : 2 * fresh], refs[2 * fresh : 2 * fresh + every]
        columns_ref = refs[2 * fresh + every]
    sources = old_sources + new_sources

    for d in range(fresh):
        spread_sources(sent[d][0:8, :], new_sources[d], 0)
        if known + d > 0 and not last:
            columns_ref[...] = jnp.transpose(sent[d][0:8, 0:slots])
    if known == 0:
        spread_targets(sent[0][0:8, 0:slots], new_targets[0], 0, slots)
        own = (new_targets[0], None, None, sources, after[0])
    else:
        own = (old_targets[0], None, before[0], new_sources, after[0])
    own = run_pairs([own], slots, 0, slots, 4 if known == 0 else 8, last, own_partial, own_sums)
    if last:
        own_ref[...] = own[0]

    def run(member):
        start, count = sum(shares[:member]), shares[member]
        groups = []
        for d in range(1, known):
            groups.append((old_targets[d], None, before[d], new_sources, after[d]))
        if not last:
            for d in range(max(known, 1), every):
                groups.append((new_targets[d - known], columns_ref, None, sources, after[d]))
            together = 4 if known == 0 else 2
            run_pairs(groups, slots, start, count, together, False, None, None)
            return
        late_start, late_count = sum(late_shares[:member]), late_shares[member]
        spread_targets(sent[0][0:8, 0:slots], new_targets[0], late_start, late_count)
        forces = run_pairs(groups, slots, start, count, 4, True, partial_ref, sums_ref)
        late = (new_targets[0], None, None, sources, None)
        together = min(4, late_count // 8)
        forces += run_pairs(
            [late], slots, late_start, late_count, together, True, late_partial, late_sums
        )
        for d in range(1, every):
            forces_ref[:, (d - 1) * slots : d * slots] = forces[d - 1]

    member = lax.rem(lax.axis_index("act"), 2)
    for m in range(2):

        @pl.when(member == m)
        def _():
            run(m)


def first_step(slots, sent, forces):
    size = sent.shape[1]
    across = size // slots
    old = [
        sent[14 + k // across : 15 + k // across, slots * (k % across) : slots * (k % across + 1)]
        for k in range(6)
    ]
    old = jnp.concatenate(old, axis=0)
    position, velocity = corrected(
        old[0:3], old[3:6], sent[0:3, 0:slots], sent[3:6, 0:slots], forces[0:3], forces[3:6]
    )
    ahead, speed = advance(position, velocity, forces[0:3], forces[3:6], fine_step)
    active = sent[7:8, 0:slots] > 0.5
    return jnp.where(active, jnp.concatenate([ahead, speed], axis=0), sent[8:14, 0:slots])


def meet_still(slots, shards, *refs):
    sent, refs = refs[:shards], refs[shards:]
    own_ref, again_ref, target_ref, after_ref, still_ref = refs
    size = sent[0].shape[1]
    chunks = size // 128
    first = slots // 128
    again = first_step(slots, sent[0], own_ref[...])
    again = jnp.concatenate([again, jnp.zeros((2, slots), jnp.float32)], axis=0)
    again_ref[...] = again
    for d in range(shards):
        rows = jnp.concatenate([sent[d][8:14, slots:size], sent[d][6:8, slots:size]], axis=0)
        spread_sources(rows, still_ref, d * (chunks - first))
    spread_targets(again, target_ref, 0, slots)
    run_pairs(
        [(target_ref, None, None, (still_ref,), after_ref)], slots, 0, slots, 4, False, None, None
    )


def finish(slots, shards, parts, *refs):
    sent, refs = refs[:shards], refs[shards:]
    shares, refs = refs[:parts], refs[parts:]
    own_ref, again_ref, target_ref, before_ref, state_ref, place_ref, out_ref = refs[:7]
    later_ref, partial_ref, sums_ref = refs[7:]
    size = state_ref.shape[1]
    first = slots // 128
    own = again_ref[...]
    for d in range(shards):
        if d == 0:
            again = own[0:6]
        else:
            share = [s[:, (d - 1) * slots : d * slots] for s in shares]
            again = first_step(
                slots, sent[d], share[0] + share[1] if parts == 2 else share[0]
            )
        rows = jnp.concatenate([again, sent[d][6:8, 0:slots]], axis=0)
        spread_sources(rows, later_ref, d * first)
    second = run_pairs(
        [(target_ref, None, before_ref, (later_ref,), None)],
        slots,
        0,
        slots,
        8,
        True,
        partial_ref,
        sums_ref,
    )[0]
    before = own_ref[...]
    position, velocity = corrected(
        before[0:3], before[3:6], own[0:3], own[3:6], second[0:3], second[3:6]
    )
    new_rows = jnp.concatenate(
        [position, velocity, second[0:6], jnp.zeros((4, slots), jnp.float32)], axis=0
    )
    slot = lax.broadcasted_iota(jnp.int32, (slots, size), 0).astype(jnp.float32)
    chosen = jnp.where(slot == place_ref[0:1, :], 1.0, 0.0).astype(jnp.bfloat16)
    back = add_terms(jnp.dot(three_terms(new_rows), chosen, preferred_element_type=jnp.float32))
    out_ref[...] = jnp.where(place_ref[1:2, :] > 0.5, back[0:12], state_ref[...])


def direct_per_device(star_state, masses, phases, levels, active_list, active_count):
    del active_count
    size = star_state.shape[1]
    shards = lax.axis_size("src")
    slots = 2 * active_list.shape[0]
    whole = pl.BlockSpec(memory_space=pltpu.VMEM)
    message, place = pl.pallas_call(
        lambda *refs: prepare(slots, size * shards, *refs),
        out_shape=(
            jax.ShapeDtypeStruct((16, size), jnp.float32),
            jax.ShapeDtypeStruct((8, size), jnp.float32),
        ),
        in_specs=[pl.BlockSpec(memory_space=pltpu.HBM)] * 4,
        out_specs=(whole, whole),
        scratch_shapes=[
            pltpu.VMEM((12, size), jnp.float32),
            pltpu.VMEM((1, size), jnp.float32),
            pltpu.VMEM((1, size), jnp.float32),
            pltpu.VMEM((1, size), jnp.int32),
            pltpu.SemaphoreType.DMA((4,)),
        ],
        compiler_params=pltpu.CompilerParams(vmem_limit_bytes=16 * 2**20),
        name="prepare",
    )(
        *(
            pltpu.with_memory_space_constraint(x, pltpu.HBM)
            for x in (star_state, masses.reshape(1, size), phases.reshape(1, size), levels.reshape(1, size))
        )
    )
    sent = [message]
    for shift in range(1, shards):
        pairs = [(d, (d + shift) % shards) for d in range(shards)]
        sent.append(lax.ppermute(message, "src", pairs))

    limit = pltpu.CompilerParams(vmem_limit_bytes=16 * 2**20)
    owners = lax.axis_size("act")
    shares = (slots // 2, slots - slots // 2)
    late_shares = (slots // 8, slots - slots // 8)
    source_shape = jax.ShapeDtypeStruct((7, size // 16, 128), jnp.float32)
    target_shape = jax.ShapeDtypeStruct((6, slots, 128), jnp.float32)
    own_shape = jax.ShapeDtypeStruct((8, slots), jnp.float32)
    columns = pltpu.VMEM((slots, 8), jnp.float32)
    sources, targets, sums = [], [], []
    known = 0
    for fresh in [2] + [1] * (shards - 2):
        every = known + fresh
        last = every == shards
        if last:
            out_shape = (own_shape, jax.ShapeDtypeStruct((8, (shards - 1) * slots), jnp.float32))
            scratch = [
                pltpu.VMEM(source_shape.shape, jnp.float32),
                pltpu.VMEM(target_shape.shape, jnp.float32),
                columns,
                pltpu.VMEM((8 * 48, 128), jnp.float32),
                pltpu.VMEM((slots + 64, 8), jnp.float32),
                pltpu.VMEM((4 * (known - 1) * 48, 128), jnp.float32),
                pltpu.VMEM(((known - 1) * (slots + 32), 8), jnp.float32),
                pltpu.VMEM((4 * 48, 128), jnp.float32),
                pltpu.VMEM((slots + 32, 8), jnp.float32),
            ]
        else:
            out_shape = [source_shape] * fresh + [target_shape] * (fresh + every)
            scratch = [columns]
        outs = pl.pallas_call(
            functools.partial(meet, slots, shares, late_shares, known, fresh, last),
            out_shape=out_shape,
            in_specs=[whole] * (fresh + 3 * known),
            out_specs=(whole, whole) if last else [whole] * (2 * fresh + every),
            scratch_shapes=scratch,
            compiler_params=limit,
            name=f"meet_{every}",
        )(*sent[known:every], *sources, *targets, *sums)
        if last:
            break
        sources += outs[:fresh]
        targets += outs[fresh : 2 * fresh]
        sums = list(outs[2 * fresh :])
        known = every
    own, part = outs
    parts = [part]
    if len(shares) == 2:
        parts.append(lax.ppermute(part, "act", [(i, i ^ 1) for i in range(owners)]))
    first = slots // 128
    again, target, still = pl.pallas_call(
        functools.partial(meet_still, slots, shards),
        out_shape=(own_shape, target_shape, target_shape),
        in_specs=[whole] * (shards + 1),
        out_specs=(whole,) * 3,
        scratch_shapes=[pltpu.VMEM((7, shards * (size // 128 - first) * 8, 128), jnp.float32)],
        compiler_params=limit,
        name="meet_still",
    )(*sent, own)
    return pl.pallas_call(
        functools.partial(finish, slots, shards, len(parts)),
        out_shape=jax.ShapeDtypeStruct((12, size), jnp.float32),
        in_specs=[whole] * (shards + len(parts) + 6),
        out_specs=whole,
        scratch_shapes=[
            pltpu.VMEM((7, shards * first * 8, 128), jnp.float32),
            pltpu.VMEM((8 * 48, 128), jnp.float32),
            pltpu.VMEM((slots + 64, 8), jnp.float32),
        ],
        compiler_params=limit,
        name="finish",
    )(*sent, *parts, own, again, target, still, star_state, place)


def solution(mesh):
    in_specs = (
        P(None, ("groups", "src")),
        P(("groups", "src")),
        P(("groups", "src")),
        P(("groups", "src")),
        P(("groups", "src", "act")),
        P(("groups", "src", "act")),
    )
    out_specs = P(None, ("groups", "src"))
    few = 3 <= mesh.shape["src"] <= MAX_DIRECT and mesh.shape["act"] % 2 == 0
    return jax.shard_map(
        direct_per_device if few else gather_per_device,
        mesh=mesh,
        in_specs=in_specs,
        out_specs=out_specs,
        check_vma=False,
    )
```

```python
import functools

import jax
import jax.numpy as jnp
from jax import lax
from jax.experimental import pallas as pl
from jax.experimental.pallas import tpu as pltpu
from jax.sharding import PartitionSpec as P


LEVELS = 5
STEPS = 2
MAX_DIRECT = 8


soften_sq = 0.0004
fine_step = 0.03125


def predict(star_state, elapsed):
    interval = elapsed[None, :]
    position = star_state[0:3] + interval * (
        star_state[3:6] + interval * (0.5 * star_state[6:9] + interval * star_state[9:12] / 6.0)
    )
    velocity = star_state[3:6] + interval * (star_state[6:9] + 0.5 * interval * star_state[9:12])
    return jnp.concatenate([position, velocity], axis=0)


def pair_block(targets, sources):
    delta_pos = sources[0:3, None, :] - targets[0:3, :, None]
    delta_vel = sources[3:6, None, :] - targets[3:6, :, None]
    dist_sq = (
        delta_pos[0] * delta_pos[0]
        + delta_pos[1] * delta_pos[1]
        + delta_pos[2] * delta_pos[2]
        + soften_sq
    )
    inverse = lax.rsqrt(dist_sq)
    inv_sq = inverse * inverse
    weight = sources[6][None, :] * inverse * inv_sq
    radial = (
        (delta_pos[0] * delta_vel[0] + delta_pos[1] * delta_vel[1] + delta_pos[2] * delta_vel[2])
        * inv_sq
        * 3.0
    )
    acceleration = jnp.sum(weight[None] * delta_pos, axis=2)
    jerk_sum = jnp.sum(weight[None] * (delta_vel - radial[None] * delta_pos), axis=2)
    return jnp.concatenate([acceleration, jerk_sum], axis=0)


def over_sources(targets, sources):
    count_src = sources.shape[1]
    width = 512
    blocks = sources.reshape(7, count_src // width, width).transpose(1, 0, 2)

    def accumulate(running, portion):
        return (running + pair_block(targets, portion), None)

    init = jnp.zeros((6, targets.shape[1]), jnp.float32)
    running, _ = lax.scan(accumulate, init, blocks)
    return running


def corrected(acc_old, jerk_old, position, velocity, acc_new, jerk_new):
    snap_term = (-6.0 * (acc_old - acc_new) - fine_step * (4.0 * jerk_old + 2.0 * jerk_new)) / (
        fine_step * fine_step
    )
    crackle = (12.0 * (acc_old - acc_new) + 6.0 * fine_step * (jerk_old + jerk_new)) / (
        fine_step * fine_step * fine_step
    )
    new_position = position + fine_step**4 / 24.0 * snap_term + fine_step**5 / 120.0 * crackle
    new_velocity = velocity + fine_step**3 / 6.0 * snap_term + fine_step**4 / 24.0 * crackle
    return new_position, new_velocity


def correct(old_state, predicted_rows, forces):
    new_position, new_velocity = corrected(
        old_state[6:9],
        old_state[9:12],
        predicted_rows[0:3],
        predicted_rows[3:6],
        forces[0:3],
        forces[3:6],
    )
    return jnp.concatenate([new_position, new_velocity, forces], axis=0)


def gather_per_device(star_state, masses, phases, levels, active_list, active_count):
    shard_size = star_state.shape[1]
    total_stars = shard_size * lax.axis_size("src")
    weights = masses / total_stars
    slot_count = active_list.shape[0]
    live = jnp.arange(slot_count, dtype=jnp.int32) < active_count[0]
    write_index = jnp.where(live, active_list, shard_size)
    tick_count = jnp.left_shift(jnp.int32(1), LEVELS - 1 - levels).astype(jnp.float32)
    state_now = star_state
    for substep in range(STEPS):
        elapsed = (
            jnp.where(levels == LEVELS - 1, 1.0, phases * (tick_count - STEPS) + (substep + 1))
            * fine_step
        )
        predicted = predict(state_now, elapsed)
        sources = jnp.concatenate([predicted, weights[None, :]], axis=0)
        targets = predicted[:, active_list]
        forces = over_sources(targets, lax.all_gather(sources, "src", axis=1, tiled=True))
        new_state = correct(state_now[:, active_list], targets, forces)
        all_new, all_index = (
            lax.all_gather(new_state, "act", axis=1, tiled=True),
            lax.all_gather(write_index, "act", axis=0, tiled=True),
        )
        state_now = state_now.at[:, all_index].set(all_new, mode="drop")
    return state_now


def three_terms(x):
    high = x.astype(jnp.bfloat16)
    rest = x - high.astype(jnp.float32)
    middle = rest.astype(jnp.bfloat16)
    low = (rest - middle.astype(jnp.float32)).astype(jnp.bfloat16)
    return jnp.concatenate([high, middle, low], axis=0)


def add_terms(y):
    rows = y.shape[0] // 3
    return (y[0:rows] + y[rows : 2 * rows]) + y[2 * rows : 3 * rows]


def advance(position, velocity, acceleration, jerk, step):
    ahead = position + step * (velocity + step * (0.5 * acceleration + step * jerk / 6.0))
    speed = velocity + step * (acceleration + 0.5 * step * jerk)
    return ahead, speed


def prepare(slots, total_stars, *refs):
    out_ref, place_ref = refs[4:6]
    copies = [
        pltpu.make_async_copy(far, near, refs[10].at[k])
        for k, (far, near) in enumerate(zip(refs[0:4], refs[6:10]))
    ]
    for copy in copies:
        copy.start()
    for copy in copies:
        copy.wait()
    state_ref, mass_ref, phase_ref, level_ref = refs[6:10]
    size = state_ref.shape[1]
    level = level_ref[...]
    active = level == LEVELS - 1
    mask = jnp.where(active, 1.0, 0.0)
    blocks = size // 128
    grouped = jnp.concatenate(
        [mask[:, 128 * b : 128 * (b + 1)] for b in range(blocks)]
        + [jnp.zeros((16 - blocks, 128), jnp.float32)],
        axis=0,
    ).astype(jnp.bfloat16)
    lane_in = lax.broadcasted_iota(jnp.int32, (128, 256), 0)
    lane_out = lax.broadcasted_iota(jnp.int32, (128, 256), 1)
    counting = jnp.where((lane_in <= lane_out) | (lane_out >= 128), 1.0, 0.0).astype(jnp.bfloat16)
    counts = jnp.dot(grouped, counting, preferred_element_type=jnp.float32)
    so_far = []
    before = jnp.zeros((1, 128), jnp.float32)
    for b in range(blocks):
        so_far.append(counts[b : b + 1, 0:128] + before)
        before = before + counts[b : b + 1, 128:256]
    rank = jnp.concatenate(so_far, axis=1)
    total = jnp.concatenate([before] * blocks, axis=1)
    star = lax.broadcasted_iota(jnp.int32, (1, size), 1).astype(jnp.float32)
    place = jnp.where(active, rank - 1.0, total + star - rank)
    place_ref[0:1, :] = place
    place_ref[1:2, :] = mask
    place_ref[2:8, :] = jnp.zeros((6, size), jnp.float32)

    tick_count = jnp.left_shift(jnp.int32(1), LEVELS - 1 - level).astype(jnp.float32)
    offset = phase_ref[...] * (tick_count - STEPS)
    position, velocity = state_ref[0:3, :], state_ref[3:6, :]
    acceleration, jerk = state_ref[6:9, :], state_ref[9:12, :]
    rows = []
    for substep in range(STEPS):
        elapsed = jnp.where(active, 1.0, offset + (substep + 1)) * fine_step
        rows.extend(advance(position, velocity, acceleration, jerk, elapsed))
        if substep == 0:
            rows.append(mass_ref[...] / total_stars)
            rows.append(mask)
    rows.append(jnp.zeros((2, size), jnp.float32))
    rows.extend([acceleration, jerk, jnp.zeros((10, size), jnp.float32)])
    terms = three_terms(jnp.concatenate(rows, axis=0))
    slot = lax.broadcasted_iota(jnp.int32, (size, size), 0).astype(jnp.float32)
    chosen = jnp.where(slot == place, 1.0, 0.0).astype(jnp.bfloat16)
    moved = add_terms(
        lax.dot_general(
            terms, chosen, (((1,), (1,)), ((), ())), preferred_element_type=jnp.float32
        )
    )
    out_ref[...] = moved[0:16]
    across = size // slots
    for k in range(6):
        out_ref[14 + k // across : 15 + k // across, slots * (k % across) : slots * (k % across + 1)] = (
            moved[16 + k : 17 + k, 0:slots]
        )


def pair_terms(source, target, sums):
    sx, sy, sz, su, sv, sw, weight = source
    tx, ty, tz, tu, tv, tw = target
    dx, dy, dz = sx - tx, sy - ty, sz - tz
    du, dv, dw = su - tu, sv - tv, sw - tw
    inverse = lax.rsqrt(dx * dx + dy * dy + (dz * dz + soften_sq))
    inv_sq = inverse * inverse
    pull = weight * inverse * inv_sq
    radial = (dx * du + dy * dv + dz * dw) * (inv_sq * 3.0)
    ax, ay, az, jx, jy, jz = sums
    return (
        ax + pull * dx,
        ay + pull * dy,
        az + pull * dz,
        jx + pull * (du - radial * dx),
        jy + pull * (dv - radial * dy),
        jz + pull * (dw - radial * dz),
    )


def spread_sources(rows, spread_ref, first):
    for c in range(rows.shape[1] // 128):
        for r in range(7):
            spread_ref[r, 8 * (first + c) : 8 * (first + c + 1), :] = jnp.broadcast_to(
                rows[r : r + 1, 128 * c : 128 * (c + 1)], (8, 128)
            )


def spread_targets(rows, spread_ref, start, count):
    columns = jnp.transpose(rows)
    for r in range(6):
        spread_ref[r, start : start + count, :] = jnp.broadcast_to(
            columns[start : start + count, r : r + 1], (count, 128)
        )


def run_pairs(groups, slots, start, count, together, finish, partial_ref, sums_ref):
    lead = 8 * together
    stride = slots + lead

    def reduce(place, many):
        for g in range(many):
            for j in range(len(groups)):
                for q in range(6):
                    row = ((g * len(groups) + j) * 6 + q) * 8
                    sums_ref[pl.ds(j * stride + place + 8 * g, 8), q : q + 1] = jnp.sum(
                        partial_ref[row : row + 8, :], axis=1, keepdims=True
                    )

    def block(base, many):
        for g in range(many):
            here = pl.ds(base + 8 * g, 8)
            for j, (target_ref, columns_ref, before_ref, sources, after_ref) in enumerate(groups):
                if not sources:
                    target = None
                elif columns_ref is None:
                    target = [target_ref[r, here, :] for r in range(6)]
                else:
                    columns = columns_ref[here, :]
                    target = [jnp.broadcast_to(columns[:, r : r + 1], (8, 128)) for r in range(6)]
                    if target_ref is not None:
                        for r in range(6):
                            target_ref[r, here, :] = target[r]
                if before_ref is None:
                    sums = (jnp.zeros((8, 128), jnp.float32),) * 6
                else:
                    sums = tuple(before_ref[q, here, :] for q in range(6))
                for source_ref in sources:
                    for c in range(source_ref.shape[1] // 8):
                        source = [source_ref[r, 8 * c : 8 * (c + 1), :] for r in range(7)]
                        sums = pair_terms(source, target, sums)
                for q in range(6):
                    if finish:
                        row = ((g * len(groups) + j) * 6 + q) * 8
                        partial_ref[row : row + 8, :] = sums[q]
                    else:
                        after_ref[q, here, :] = sums[q]

    def body(step, unused):
        base = pl.multiple_of(start + step * lead, 8)
        if finish:
            reduce(base, together)
        block(base, together)
        return unused

    if finish:
        used = together * len(groups) * 48
        partial_ref[0:used, :] = jnp.zeros((used, 128), jnp.float32)
        if count < slots:
            sums_ref[...] = jnp.zeros_like(sums_ref)
    steps = count // lead
    lax.fori_loop(0, steps, body, 0)
    rest = (count - steps * lead) // 8
    end = start + steps * lead
    if finish:
        reduce(end, together)
    if rest:
        block(end, rest)
        if finish:
            reduce(end + lead, rest)
    if not finish:
        return None
    return [
        jnp.transpose(sums_ref[j * stride + lead : (j + 1) * stride, :])
        for j in range(len(groups))
    ]


def on_member(shares, run):
    member = lax.rem(lax.axis_index("act"), len(shares))
    for m in range(len(shares)):

        @pl.when(member == m)
        def _():
            run(sum(shares[:m]), shares[m])


def meet(slots, shares, known, fresh, tail, *refs):
    every = known + fresh
    sent, refs = refs[:fresh], refs[fresh:]
    old_sources, old_targets, before = refs[:known], refs[known : 2 * known], refs[2 * known : 3 * known]
    refs = refs[3 * known :]
    new_sources, new_targets, after = refs[:fresh], refs[fresh : 2 * fresh], refs[2 * fresh : 2 * fresh + every]
    refs = refs[2 * fresh + every :]
    sources = old_sources + new_sources

    def run(start, count):
        groups = []
        for d in range(known):
            groups.append((old_targets[d], None, before[d], new_sources, after[d]))
        for d in range(fresh):
            spread_sources(sent[d][0:8, :], new_sources[d], 0)
            in_loop = None
            if known:
                in_loop = refs[-1]
                in_loop[...] = jnp.transpose(sent[d][0:8, 0:slots])
            elif d == 0 and start > 0:
                spread_targets(sent[d][0:8, 0:slots], new_targets[d], 0, slots)
            else:
                spread_targets(sent[d][0:8, 0:slots], new_targets[d], start, count)
            groups.append((new_targets[d], in_loop, None, sources, after[known + d]))
        run_pairs(groups, slots, start, count, 2, False, None, None)
        if tail:
            part_ref, partial_ref, sums_ref = refs[0:3]
            if start == 0:
                group = (None, None, after[0], (), None)
                part_ref[...] = run_pairs(
                    [group], slots, start, count, count // 8, True, partial_ref, sums_ref
                )[0]
            else:
                part_ref[...] = jnp.zeros_like(part_ref)

    on_member(shares, run)


def meet_own(slots, shares, early, sent_ref, part_ref, own_target, own_before, *refs):
    known = len(refs) - 8
    sources = refs[:known]
    source_ref, own_ref, late_ref, target_ref, own_partial, own_sums, partial_ref, sums_ref = refs[known:]
    spread_sources(sent_ref[0:8, :], source_ref, 0)
    member = lax.rem(lax.axis_index("act"), 2)

    @pl.when(member == 0)
    def _():
        late_ref[...] = jnp.zeros_like(late_ref)
        own_ref[...] = part_ref[...]

    @pl.when(member == 1)
    def _():
        spread_targets(sent_ref[0:8, 0:slots], target_ref, 0, slots)
        rows, width = max(shares) * 6, slots + max(shares)
        own = []
        for m, before in enumerate((None, own_before)):
            group = (own_target, None, before, (source_ref,), None)
            own += run_pairs(
                [group],
                slots,
                sum(shares[:m]),
                shares[m],
                shares[m] // 8,
                True,
                own_partial.at[m * rows : (m + 1) * rows],
                own_sums.at[m * width : (m + 1) * width],
            )
        own_ref[...] = own[0] + own[1]
        group = (target_ref, None, None, sources + (source_ref,), None)
        late_ref[...] = run_pairs([group], slots, 0, early, 4, True, partial_ref, sums_ref)[0]


def meet_rest(slots, shares, late_shares, sent_ref, source_ref, late_ref, late_target, *refs):
    known = (len(refs) - 7) // 3
    sources, targets, before = refs[: known + 1], refs[known + 1 : 2 * known + 1], refs[2 * known + 1 : 3 * known + 1]
    forces_ref, partial_ref, sums_ref, late_partial, late_sums, target_ref = refs[3 * known + 1 :]

    def run(start, count):
        member = 0 if start == 0 else 1
        first, many = slots - sum(late_shares[member:]), late_shares[member]
        goal = late_target
        if member == 0:
            goal = target_ref
            spread_targets(sent_ref[0:8, 0:slots], target_ref, first, many)
        groups = [(t, None, b, (source_ref,), None) for t, b in zip(targets, before)]
        forces = run_pairs(groups, slots, start, count, 4, True, partial_ref, sums_ref)
        for d in range(known):
            forces_ref[:, d * slots : (d + 1) * slots] = forces[d]
        group = (goal, None, None, sources + (source_ref,), None)
        together = max(many // 16, 1)
        late = run_pairs(
            [group],
            slots,
            first,
            many,
            together,
            True,
            late_partial,
            late_sums.at[0 : slots + 8 * together],
        )[0]
        forces_ref[:, known * slots : (known + 1) * slots] = late_ref[...] + late

    on_member(shares, run)


def first_step(slots, sent, forces):
    size = sent.shape[1]
    across = size // slots
    old = [
        sent[14 + k // across : 15 + k // across, slots * (k % across) : slots * (k % across + 1)]
        for k in range(6)
    ]
    old = jnp.concatenate(old, axis=0)
    position, velocity = corrected(
        old[0:3], old[3:6], sent[0:3, 0:slots], sent[3:6, 0:slots], forces[0:3], forces[3:6]
    )
    ahead, speed = advance(position, velocity, forces[0:3], forces[3:6], fine_step)
    active = sent[7:8, 0:slots] > 0.5
    return jnp.where(active, jnp.concatenate([ahead, speed], axis=0), sent[8:14, 0:slots])


def meet_still(slots, shards, parts, *refs):
    sent, refs = refs[:shards], refs[shards:]
    shares, refs = refs[:parts], refs[parts:]
    own_ref, again_ref, target_ref, after_ref, still_ref = refs
    own_ref[...] = shares[0][...] + shares[1][...] if parts == 2 else shares[0][...]
    size = sent[0].shape[1]
    chunks = size // 128
    first = slots // 128
    again = first_step(slots, sent[0], own_ref[...])
    again = jnp.concatenate([again, jnp.zeros((2, slots), jnp.float32)], axis=0)
    again_ref[...] = again
    for d in range(shards):
        rows = jnp.concatenate([sent[d][8:14, slots:size], sent[d][6:8, slots:size]], axis=0)
        spread_sources(rows, still_ref, d * (chunks - first))
    spread_targets(again, target_ref, 0, slots)
    run_pairs(
        [(target_ref, None, None, (still_ref,), after_ref)], slots, 0, slots, 4, False, None, None
    )


def finish(slots, shards, parts, *refs):
    sent, refs = refs[:shards], refs[shards:]
    shares, refs = refs[:parts], refs[parts:]
    own_ref, again_ref, target_ref, before_ref, state_ref, place_ref, out_ref = refs[:7]
    later_ref, partial_ref, sums_ref = refs[7:]
    size = state_ref.shape[1]
    first = slots // 128
    own = again_ref[...]
    for d in range(shards):
        if d == 0:
            again = own[0:6]
        else:
            share = [s[:, (d - 1) * slots : d * slots] for s in shares]
            again = first_step(
                slots, sent[d], share[0] + share[1] if parts == 2 else share[0]
            )
        rows = jnp.concatenate([again, sent[d][6:8, 0:slots]], axis=0)
        spread_sources(rows, later_ref, d * first)
    second = run_pairs(
        [(target_ref, None, before_ref, (later_ref,), None)],
        slots,
        0,
        slots,
        8,
        True,
        partial_ref,
        sums_ref,
    )[0]
    before = own_ref[...]
    position, velocity = corrected(
        before[0:3], before[3:6], own[0:3], own[3:6], second[0:3], second[3:6]
    )
    new_rows = jnp.concatenate(
        [position, velocity, second[0:6], jnp.zeros((4, slots), jnp.float32)], axis=0
    )
    slot = lax.broadcasted_iota(jnp.int32, (slots, size), 0).astype(jnp.float32)
    chosen = jnp.where(slot == place_ref[0:1, :], 1.0, 0.0).astype(jnp.bfloat16)
    back = add_terms(jnp.dot(three_terms(new_rows), chosen, preferred_element_type=jnp.float32))
    out_ref[...] = jnp.where(place_ref[1:2, :] > 0.5, back[0:12], state_ref[...])


def direct_per_device(star_state, masses, phases, levels, active_list, active_count):
    del active_count
    size = star_state.shape[1]
    shards = lax.axis_size("src")
    slots = 2 * active_list.shape[0]
    whole = pl.BlockSpec(memory_space=pltpu.VMEM)
    message, place = pl.pallas_call(
        lambda *refs: prepare(slots, size * shards, *refs),
        out_shape=(
            jax.ShapeDtypeStruct((16, size), jnp.float32),
            jax.ShapeDtypeStruct((8, size), jnp.float32),
        ),
        in_specs=[pl.BlockSpec(memory_space=pltpu.HBM)] * 4,
        out_specs=(whole, whole),
        scratch_shapes=[
            pltpu.VMEM((12, size), jnp.float32),
            pltpu.VMEM((1, size), jnp.float32),
            pltpu.VMEM((1, size), jnp.float32),
            pltpu.VMEM((1, size), jnp.int32),
            pltpu.SemaphoreType.DMA((4,)),
        ],
        compiler_params=pltpu.CompilerParams(vmem_limit_bytes=16 * 2**20),
        name="prepare",
    )(
        *(
            pltpu.with_memory_space_constraint(x, pltpu.HBM)
            for x in (star_state, masses.reshape(1, size), phases.reshape(1, size), levels.reshape(1, size))
        )
    )
    sent = [message]
    for shift in range(1, shards):
        pairs = [(d, (d + shift) % shards) for d in range(shards)]
        sent.append(lax.ppermute(message, "src", pairs))

    limit = pltpu.CompilerParams(vmem_limit_bytes=16 * 2**20)
    owners = lax.axis_size("act")
    shares = (slots // 2, slots - slots // 2)
    parts = len(shares)

    def with_other(part):
        return [part, lax.ppermute(part, "act", [(i, i ^ 1) for i in range(owners)])]

    def call(body, operands, out_shape, scratch=(), pairs=0):
        cost = pl.CostEstimate(flops=41 * pairs, bytes_accessed=0, transcendentals=pairs)
        return pl.pallas_call(
            body,
            out_shape=out_shape,
            in_specs=[whole] * len(operands),
            out_specs=jax.tree.map(lambda _: whole, out_shape),
            scratch_shapes=list(scratch),
            compiler_params=limit,
            cost_estimate=cost if pairs else None,
        )(*operands)

    def rows(shape):
        return pltpu.VMEM(shape, jnp.float32)

    source_shape = jax.ShapeDtypeStruct((7, size // 16, 128), jnp.float32)
    target_shape = jax.ShapeDtypeStruct((6, slots, 128), jnp.float32)
    own_shape = jax.ShapeDtypeStruct((8, slots), jnp.float32)
    sources, targets, sums = [], [], []
    known = 0
    for fresh in [2] + [1] * (shards - 3):
        every = known + fresh
        tail = every == shards - 1
        outs = call(
            functools.partial(meet, slots, shares, known, fresh, tail),
            [*sent[known:every], *sources, *targets, *sums],
            [source_shape] * fresh + [target_shape] * (fresh + every) + [own_shape] * tail,
            [rows((max(shares) * 6, 128)), rows((slots + max(shares), 8))] * tail
            + [rows((slots, 8))],
        )
        sources += outs[:fresh]
        targets += outs[fresh : 2 * fresh]
        sums = list(outs[2 * fresh : 2 * fresh + every])
        known = every
    early = slots // 2
    late_shares = (slots * 3 // 8, slots // 8)
    source, own, late, late_target = call(
        functools.partial(meet_own, slots, shares, early),
        [sent[known], outs[-1], targets[0], sums[0], *sources],
        (source_shape, own_shape, own_shape, target_shape),
        [
            rows((2 * max(shares) * 6, 128)),
            rows((2 * (slots + max(shares)), 8)),
            rows((4 * 48, 128)),
            rows((slots + 32, 8)),
        ],
    )
    others = known - 1
    together = max(late_shares) // 16
    own = with_other(own)
    forces = call(
        functools.partial(meet_rest, slots, shares, late_shares),
        [sent[known], source, late, late_target, *sources, *targets[1:], *sums[1:]],
        jax.ShapeDtypeStruct((8, known * slots), jnp.float32),
        [
            rows((4 * others * 48, 128)),
            rows((others * (slots + 32), 8)),
            rows((together * 48, 128)),
            rows((slots + 8 * together, 8)),
            rows(target_shape.shape),
        ],
        others * max(shares) * size,
    )
    forces = with_other(forces)
    first = slots // 128
    own, again, target, still = call(
        functools.partial(meet_still, slots, shards, parts),
        [*sent, *own],
        (own_shape, own_shape, target_shape, target_shape),
        [rows((7, shards * (size // 128 - first) * 8, 128))],
        slots * shards * (size - slots),
    )
    return call(
        functools.partial(finish, slots, shards, parts),
        [*sent, *forces, own, again, target, still, star_state, place],
        jax.ShapeDtypeStruct((12, size), jnp.float32),
        [rows((7, shards * first * 8, 128)), rows((8 * 48, 128)), rows((slots + 64, 8))],
    )


def solution(mesh):
    in_specs = (
        P(None, ("groups", "src")),
        P(("groups", "src")),
        P(("groups", "src")),
        P(("groups", "src")),
        P(("groups", "src", "act")),
        P(("groups", "src", "act")),
    )
    out_specs = P(None, ("groups", "src"))
    few = 3 <= mesh.shape["src"] <= MAX_DIRECT and mesh.shape["act"] % 2 == 0
    return jax.shard_map(
        direct_per_device if few else gather_per_device,
        mesh=mesh,
        in_specs=in_specs,
        out_specs=out_specs,
        check_vma=False,
    )
```

```python
import functools

import jax
import jax.numpy as jnp
from jax import lax
from jax.experimental import pallas as pl
from jax.experimental.pallas import tpu as pltpu
from jax.sharding import PartitionSpec as P


LEVELS = 5
STEPS = 2
MAX_DIRECT = 8


soften_sq = 0.0004
fine_step = 0.03125


def predict(star_state, elapsed):
    interval = elapsed[None, :]
    position = star_state[0:3] + interval * (
        star_state[3:6] + interval * (0.5 * star_state[6:9] + interval * star_state[9:12] / 6.0)
    )
    velocity = star_state[3:6] + interval * (star_state[6:9] + 0.5 * interval * star_state[9:12])
    return jnp.concatenate([position, velocity], axis=0)


def pair_block(targets, sources):
    delta_pos = sources[0:3, None, :] - targets[0:3, :, None]
    delta_vel = sources[3:6, None, :] - targets[3:6, :, None]
    dist_sq = (
        delta_pos[0] * delta_pos[0]
        + delta_pos[1] * delta_pos[1]
        + delta_pos[2] * delta_pos[2]
        + soften_sq
    )
    inverse = lax.rsqrt(dist_sq)
    inv_sq = inverse * inverse
    weight = sources[6][None, :] * inverse * inv_sq
    radial = (
        (delta_pos[0] * delta_vel[0] + delta_pos[1] * delta_vel[1] + delta_pos[2] * delta_vel[2])
        * inv_sq
        * 3.0
    )
    acceleration = jnp.sum(weight[None] * delta_pos, axis=2)
    jerk_sum = jnp.sum(weight[None] * (delta_vel - radial[None] * delta_pos), axis=2)
    return jnp.concatenate([acceleration, jerk_sum], axis=0)


def over_sources(targets, sources):
    count_src = sources.shape[1]
    width = 512
    blocks = sources.reshape(7, count_src // width, width).transpose(1, 0, 2)

    def accumulate(running, portion):
        return (running + pair_block(targets, portion), None)

    init = jnp.zeros((6, targets.shape[1]), jnp.float32)
    running, _ = lax.scan(accumulate, init, blocks)
    return running


def corrected(acc_old, jerk_old, position, velocity, acc_new, jerk_new):
    snap_term = (-6.0 * (acc_old - acc_new) - fine_step * (4.0 * jerk_old + 2.0 * jerk_new)) / (
        fine_step * fine_step
    )
    crackle = (12.0 * (acc_old - acc_new) + 6.0 * fine_step * (jerk_old + jerk_new)) / (
        fine_step * fine_step * fine_step
    )
    new_position = position + fine_step**4 / 24.0 * snap_term + fine_step**5 / 120.0 * crackle
    new_velocity = velocity + fine_step**3 / 6.0 * snap_term + fine_step**4 / 24.0 * crackle
    return new_position, new_velocity


def correct(old_state, predicted_rows, forces):
    new_position, new_velocity = corrected(
        old_state[6:9],
        old_state[9:12],
        predicted_rows[0:3],
        predicted_rows[3:6],
        forces[0:3],
        forces[3:6],
    )
    return jnp.concatenate([new_position, new_velocity, forces], axis=0)


def gather_per_device(star_state, masses, phases, levels, active_list, active_count):
    shard_size = star_state.shape[1]
    total_stars = shard_size * lax.axis_size("src")
    weights = masses / total_stars
    slot_count = active_list.shape[0]
    live = jnp.arange(slot_count, dtype=jnp.int32) < active_count[0]
    write_index = jnp.where(live, active_list, shard_size)
    tick_count = jnp.left_shift(jnp.int32(1), LEVELS - 1 - levels).astype(jnp.float32)
    state_now = star_state
    for substep in range(STEPS):
        elapsed = (
            jnp.where(levels == LEVELS - 1, 1.0, phases * (tick_count - STEPS) + (substep + 1))
            * fine_step
        )
        predicted = predict(state_now, elapsed)
        sources = jnp.concatenate([predicted, weights[None, :]], axis=0)
        targets = predicted[:, active_list]
        forces = over_sources(targets, lax.all_gather(sources, "src", axis=1, tiled=True))
        new_state = correct(state_now[:, active_list], targets, forces)
        all_new, all_index = (
            lax.all_gather(new_state, "act", axis=1, tiled=True),
            lax.all_gather(write_index, "act", axis=0, tiled=True),
        )
        state_now = state_now.at[:, all_index].set(all_new, mode="drop")
    return state_now


def three_terms(x):
    high = x.astype(jnp.bfloat16)
    rest = x - high.astype(jnp.float32)
    middle = rest.astype(jnp.bfloat16)
    low = (rest - middle.astype(jnp.float32)).astype(jnp.bfloat16)
    return jnp.concatenate([high, middle, low], axis=0)


def add_terms(y):
    rows = y.shape[0] // 3
    return (y[0:rows] + y[rows : 2 * rows]) + y[2 * rows : 3 * rows]


def advance(position, velocity, acceleration, jerk, step):
    ahead = position + step * (velocity + step * (0.5 * acceleration + step * jerk / 6.0))
    speed = velocity + step * (acceleration + 0.5 * step * jerk)
    return ahead, speed


def prepare(slots, total_stars, *refs):
    out_ref, place_ref = refs[4:6]
    copies = [
        pltpu.make_async_copy(far, near, refs[10].at[k])
        for k, (far, near) in enumerate(zip(refs[0:4], refs[6:10]))
    ]
    for copy in copies:
        copy.start()
    for copy in copies:
        copy.wait()
    state_ref, mass_ref, phase_ref, level_ref = refs[6:10]
    size = state_ref.shape[1]
    level = level_ref[...]
    active = level == LEVELS - 1
    mask = jnp.where(active, 1.0, 0.0)
    blocks = size // 128
    grouped = jnp.concatenate(
        [mask[:, 128 * b : 128 * (b + 1)] for b in range(blocks)]
        + [jnp.zeros((16 - blocks, 128), jnp.float32)],
        axis=0,
    ).astype(jnp.bfloat16)
    lane_in = lax.broadcasted_iota(jnp.int32, (128, 256), 0)
    lane_out = lax.broadcasted_iota(jnp.int32, (128, 256), 1)
    counting = jnp.where((lane_in <= lane_out) | (lane_out >= 128), 1.0, 0.0).astype(jnp.bfloat16)
    counts = jnp.dot(grouped, counting, preferred_element_type=jnp.float32)
    so_far = []
    before = jnp.zeros((1, 128), jnp.float32)
    for b in range(blocks):
        so_far.append(counts[b : b + 1, 0:128] + before)
        before = before + counts[b : b + 1, 128:256]
    rank = jnp.concatenate(so_far, axis=1)
    total = jnp.concatenate([before] * blocks, axis=1)
    star = lax.broadcasted_iota(jnp.int32, (1, size), 1).astype(jnp.float32)
    place = jnp.where(active, rank - 1.0, total + star - rank)
    place_ref[0:1, :] = place
    place_ref[1:2, :] = mask
    place_ref[2:8, :] = jnp.zeros((6, size), jnp.float32)

    tick_count = jnp.left_shift(jnp.int32(1), LEVELS - 1 - level).astype(jnp.float32)
    offset = phase_ref[...] * (tick_count - STEPS)
    position, velocity = state_ref[0:3, :], state_ref[3:6, :]
    acceleration, jerk = state_ref[6:9, :], state_ref[9:12, :]
    rows = []
    for substep in range(STEPS):
        elapsed = jnp.where(active, 1.0, offset + (substep + 1)) * fine_step
        rows.extend(advance(position, velocity, acceleration, jerk, elapsed))
        if substep == 0:
            rows.append(mass_ref[...] / total_stars)
            rows.append(mask)
    rows.append(jnp.zeros((2, size), jnp.float32))
    rows.extend([acceleration, jerk, jnp.zeros((10, size), jnp.float32)])
    terms = three_terms(jnp.concatenate(rows, axis=0))
    slot = lax.broadcasted_iota(jnp.int32, (size, size), 0).astype(jnp.float32)
    chosen = jnp.where(slot == place, 1.0, 0.0).astype(jnp.bfloat16)
    moved = add_terms(
        lax.dot_general(
            terms, chosen, (((1,), (1,)), ((), ())), preferred_element_type=jnp.float32
        )
    )
    out_ref[...] = moved[0:16]
    across = size // slots
    for k in range(6):
        out_ref[14 + k // across : 15 + k // across, slots * (k % across) : slots * (k % across + 1)] = (
            moved[16 + k : 17 + k, 0:slots]
        )


def pair_terms(source, target, sums):
    sx, sy, sz, su, sv, sw, weight = source
    tx, ty, tz, tu, tv, tw = target
    dx, dy, dz = sx - tx, sy - ty, sz - tz
    du, dv, dw = su - tu, sv - tv, sw - tw
    inverse = lax.rsqrt(dx * dx + dy * dy + (dz * dz + soften_sq))
    inv_sq = inverse * inverse
    pull = weight * inverse * inv_sq
    radial = (dx * du + dy * dv + dz * dw) * (inv_sq * 3.0)
    ax, ay, az, jx, jy, jz = sums
    return (
        ax + pull * dx,
        ay + pull * dy,
        az + pull * dz,
        jx + pull * (du - radial * dx),
        jy + pull * (dv - radial * dy),
        jz + pull * (dw - radial * dz),
    )


def spread_sources(rows, spread_ref, first):
    for c in range(rows.shape[1] // 128):
        for r in range(7):
            spread_ref[r, 8 * (first + c) : 8 * (first + c + 1), :] = jnp.broadcast_to(
                rows[r : r + 1, 128 * c : 128 * (c + 1)], (8, 128)
            )


def spread_targets(rows, spread_ref, start, count):
    columns = jnp.transpose(rows)
    for r in range(6):
        spread_ref[r, start : start + count, :] = jnp.broadcast_to(
            columns[start : start + count, r : r + 1], (count, 128)
        )


def run_pairs(groups, slots, start, count, together, finish, partial_ref, sums_ref):
    lead = 8 * together
    stride = slots + lead

    def reduce(place, many):
        for g in range(many):
            for j in range(len(groups)):
                for q in range(6):
                    row = ((g * len(groups) + j) * 6 + q) * 8
                    sums_ref[pl.ds(j * stride + place + 8 * g, 8), q : q + 1] = jnp.sum(
                        partial_ref[row : row + 8, :], axis=1, keepdims=True
                    )

    def block(base, many):
        for g in range(many):
            here = pl.ds(base + 8 * g, 8)
            for j, (target_ref, columns_ref, before_ref, sources, after_ref) in enumerate(groups):
                if columns_ref is None:
                    target = [target_ref[r, here, :] for r in range(6)]
                else:
                    columns = columns_ref[here, :]
                    target = [jnp.broadcast_to(columns[:, r : r + 1], (8, 128)) for r in range(6)]
                    if target_ref is not None:
                        for r in range(6):
                            target_ref[r, here, :] = target[r]
                if before_ref is None:
                    sums = (jnp.zeros((8, 128), jnp.float32),) * 6
                else:
                    sums = tuple(before_ref[q, here, :] for q in range(6))
                for source_ref in sources:
                    for c in range(source_ref.shape[1] // 8):
                        source = [source_ref[r, 8 * c : 8 * (c + 1), :] for r in range(7)]
                        sums = pair_terms(source, target, sums)
                for q in range(6):
                    if finish:
                        row = ((g * len(groups) + j) * 6 + q) * 8
                        partial_ref[row : row + 8, :] = sums[q]
                    else:
                        after_ref[q, here, :] = sums[q]

    def body(step, unused):
        base = pl.multiple_of(start + step * lead, 8)
        if finish:
            reduce(base, together)
        block(base, together)
        return unused

    if finish:
        used = together * len(groups) * 48
        partial_ref[0:used, :] = jnp.zeros((used, 128), jnp.float32)
        if count < slots:
            sums_ref[...] = jnp.zeros_like(sums_ref)
    steps = count // lead
    lax.fori_loop(0, steps, body, 0)
    rest = (count - steps * lead) // 8
    end = start + steps * lead
    if finish:
        reduce(end, together)
    if rest:
        block(end, rest)
        if finish:
            reduce(end + lead, rest)
    if not finish:
        return None
    return [
        jnp.transpose(sums_ref[j * stride + lead : (j + 1) * stride, :])
        for j in range(len(groups))
    ]


def on_member(shares, run):
    member = lax.rem(lax.axis_index("act"), len(shares))
    for m in range(len(shares)):

        @pl.when(member == m)
        def _():
            run(sum(shares[:m]), shares[m])


def meet(slots, shares, known, fresh, *refs):
    every = known + fresh
    sent, refs = refs[:fresh], refs[fresh:]
    old_sources, old_targets, before = refs[:known], refs[known : 2 * known], refs[2 * known : 3 * known]
    refs = refs[3 * known :]
    new_sources, new_targets, after = refs[:fresh], refs[fresh : 2 * fresh], refs[2 * fresh : 2 * fresh + every]
    columns_ref = refs[2 * fresh + every]
    sources = old_sources + new_sources

    def run(start, count):
        groups = []
        for d in range(known):
            groups.append((old_targets[d], None, before[d], new_sources, after[d]))
        for d in range(fresh):
            spread_sources(sent[d][0:8, :], new_sources[d], 0)
            in_loop = None
            if known:
                in_loop = columns_ref
                columns_ref[...] = jnp.transpose(sent[d][0:8, 0:slots])
            else:
                spread_targets(sent[d][0:8, 0:slots], new_targets[d], start, count)
            groups.append((new_targets[d], in_loop, None, sources, after[known + d]))
        run_pairs(groups, slots, start, count, 2, False, None, None)

    on_member(shares, run)


def meet_own(slots, shares, early, sent_ref, own_target, own_before, *refs):
    known = len(refs) - 8
    sources = refs[:known]
    source_ref, own_ref, late_ref, target_ref, own_partial, own_sums, partial_ref, sums_ref = refs[known:]
    spread_sources(sent_ref[0:8, :], source_ref, 0)

    def own(start, count):
        group = (own_target, None, own_before, (source_ref,), None)
        own_ref[...] = run_pairs(
            [group], slots, start, count, 4, True, own_partial, own_sums
        )[0]

    member = lax.rem(lax.axis_index("act"), 2)

    @pl.when(member == 0)
    def _():
        late_ref[...] = jnp.zeros_like(late_ref)
        spread_targets(sent_ref[0:8, 0:slots], target_ref, early, slots - early)
        own(0, shares[0])

    @pl.when(member == 1)
    def _():
        spread_targets(sent_ref[0:8, 0:slots], target_ref, 0, slots)
        own(shares[0], shares[1])
        group = (target_ref, None, None, sources + (source_ref,), None)
        late_ref[...] = run_pairs([group], slots, 0, early, 2, True, partial_ref, sums_ref)[0]


def meet_rest(slots, shares, early, source_ref, late_ref, late_target, *refs):
    known = (len(refs) - 4) // 3
    sources, targets, before = refs[: known + 1], refs[known + 1 : 2 * known + 1], refs[2 * known + 1 : 3 * known + 1]
    forces_ref, partial_ref, sums_ref = refs[3 * known + 1 :]

    def run(start, count):
        groups = [(t, None, b, (source_ref,), None) for t, b in zip(targets, before)]
        forces = run_pairs(groups, slots, start, count, 4, True, partial_ref, sums_ref)
        for d in range(known):
            forces_ref[:, d * slots : (d + 1) * slots] = forces[d]
        late = late_ref[...]
        if start == 0:
            group = (late_target, None, None, sources + (source_ref,), None)
            late += run_pairs(
                [group],
                slots,
                early,
                slots - early,
                1,
                True,
                partial_ref.at[0:48],
                sums_ref.at[0 : slots + 8],
            )[0]
        forces_ref[:, known * slots : (known + 1) * slots] = late

    on_member(shares, run)


def first_step(slots, sent, forces):
    size = sent.shape[1]
    across = size // slots
    old = [
        sent[14 + k // across : 15 + k // across, slots * (k % across) : slots * (k % across + 1)]
        for k in range(6)
    ]
    old = jnp.concatenate(old, axis=0)
    position, velocity = corrected(
        old[0:3], old[3:6], sent[0:3, 0:slots], sent[3:6, 0:slots], forces[0:3], forces[3:6]
    )
    ahead, speed = advance(position, velocity, forces[0:3], forces[3:6], fine_step)
    active = sent[7:8, 0:slots] > 0.5
    return jnp.where(active, jnp.concatenate([ahead, speed], axis=0), sent[8:14, 0:slots])


def meet_still(slots, shards, parts, *refs):
    sent, refs = refs[:shards], refs[shards:]
    shares, refs = refs[:parts], refs[parts:]
    own_ref, again_ref, target_ref, after_ref, still_ref = refs
    own_ref[...] = shares[0][...] + shares[1][...] if parts == 2 else shares[0][...]
    size = sent[0].shape[1]
    chunks = size // 128
    first = slots // 128
    again = first_step(slots, sent[0], own_ref[...])
    again = jnp.concatenate([again, jnp.zeros((2, slots), jnp.float32)], axis=0)
    again_ref[...] = again
    for d in range(shards):
        rows = jnp.concatenate([sent[d][8:14, slots:size], sent[d][6:8, slots:size]], axis=0)
        spread_sources(rows, still_ref, d * (chunks - first))
    spread_targets(again, target_ref, 0, slots)
    run_pairs(
        [(target_ref, None, None, (still_ref,), after_ref)], slots, 0, slots, 4, False, None, None
    )


def finish(slots, shards, parts, *refs):
    sent, refs = refs[:shards], refs[shards:]
    shares, refs = refs[:parts], refs[parts:]
    own_ref, again_ref, target_ref, before_ref, state_ref, place_ref, out_ref = refs[:7]
    later_ref, partial_ref, sums_ref = refs[7:]
    size = state_ref.shape[1]
    first = slots // 128
    own = again_ref[...]
    for d in range(shards):
        if d == 0:
            again = own[0:6]
        else:
            share = [s[:, (d - 1) * slots : d * slots] for s in shares]
            again = first_step(
                slots, sent[d], share[0] + share[1] if parts == 2 else share[0]
            )
        rows = jnp.concatenate([again, sent[d][6:8, 0:slots]], axis=0)
        spread_sources(rows, later_ref, d * first)
    second = run_pairs(
        [(target_ref, None, before_ref, (later_ref,), None)],
        slots,
        0,
        slots,
        8,
        True,
        partial_ref,
        sums_ref,
    )[0]
    before = own_ref[...]
    position, velocity = corrected(
        before[0:3], before[3:6], own[0:3], own[3:6], second[0:3], second[3:6]
    )
    new_rows = jnp.concatenate(
        [position, velocity, second[0:6], jnp.zeros((4, slots), jnp.float32)], axis=0
    )
    slot = lax.broadcasted_iota(jnp.int32, (slots, size), 0).astype(jnp.float32)
    chosen = jnp.where(slot == place_ref[0:1, :], 1.0, 0.0).astype(jnp.bfloat16)
    back = add_terms(jnp.dot(three_terms(new_rows), chosen, preferred_element_type=jnp.float32))
    out_ref[...] = jnp.where(place_ref[1:2, :] > 0.5, back[0:12], state_ref[...])


def direct_per_device(star_state, masses, phases, levels, active_list, active_count):
    del active_count
    size = star_state.shape[1]
    shards = lax.axis_size("src")
    slots = 2 * active_list.shape[0]
    whole = pl.BlockSpec(memory_space=pltpu.VMEM)
    message, place = pl.pallas_call(
        lambda *refs: prepare(slots, size * shards, *refs),
        out_shape=(
            jax.ShapeDtypeStruct((16, size), jnp.float32),
            jax.ShapeDtypeStruct((8, size), jnp.float32),
        ),
        in_specs=[pl.BlockSpec(memory_space=pltpu.HBM)] * 4,
        out_specs=(whole, whole),
        scratch_shapes=[
            pltpu.VMEM((12, size), jnp.float32),
            pltpu.VMEM((1, size), jnp.float32),
            pltpu.VMEM((1, size), jnp.float32),
            pltpu.VMEM((1, size), jnp.int32),
            pltpu.SemaphoreType.DMA((4,)),
        ],
        compiler_params=pltpu.CompilerParams(vmem_limit_bytes=16 * 2**20),
        name="prepare",
    )(
        *(
            pltpu.with_memory_space_constraint(x, pltpu.HBM)
            for x in (star_state, masses.reshape(1, size), phases.reshape(1, size), levels.reshape(1, size))
        )
    )
    sent = [message]
    for shift in range(1, shards):
        pairs = [(d, (d + shift) % shards) for d in range(shards)]
        sent.append(lax.ppermute(message, "src", pairs))

    limit = pltpu.CompilerParams(vmem_limit_bytes=16 * 2**20)
    owners = lax.axis_size("act")
    shares = (slots // 2, slots - slots // 2)
    parts = len(shares)

    def with_other(part):
        return [part, lax.ppermute(part, "act", [(i, i ^ 1) for i in range(owners)])]

    def call(body, operands, out_shape, scratch=(), pairs=0):
        cost = pl.CostEstimate(flops=41 * pairs, bytes_accessed=0, transcendentals=pairs)
        return pl.pallas_call(
            body,
            out_shape=out_shape,
            in_specs=[whole] * len(operands),
            out_specs=jax.tree.map(lambda _: whole, out_shape),
            scratch_shapes=list(scratch),
            compiler_params=limit,
            cost_estimate=cost if pairs else None,
        )(*operands)

    def rows(shape):
        return pltpu.VMEM(shape, jnp.float32)

    source_shape = jax.ShapeDtypeStruct((7, size // 16, 128), jnp.float32)
    target_shape = jax.ShapeDtypeStruct((6, slots, 128), jnp.float32)
    own_shape = jax.ShapeDtypeStruct((8, slots), jnp.float32)
    sources, targets, sums = [], [], []
    known = 0
    for fresh in [2] + [1] * (shards - 3):
        every = known + fresh
        outs = call(
            functools.partial(meet, slots, shares, known, fresh),
            [*sent[known:every], *sources, *targets, *sums],
            [source_shape] * fresh + [target_shape] * (fresh + every),
            [rows((slots, 8))],
        )
        sources += outs[:fresh]
        targets += outs[fresh : 2 * fresh]
        sums = list(outs[2 * fresh :])
        known = every
    early = slots * 7 // 8
    source, own, late, late_target = call(
        functools.partial(meet_own, slots, shares, early),
        [sent[known], targets[0], sums[0], *sources],
        (source_shape, own_shape, own_shape, target_shape),
        [
            rows((max(shares) * 6, 128)),
            rows((slots + max(shares), 8)),
            rows((4 * 48, 128)),
            rows((slots + 32, 8)),
        ],
    )
    others = known - 1
    own = with_other(own)
    forces = call(
        functools.partial(meet_rest, slots, shares, early),
        [source, late, late_target, *sources, *targets[1:], *sums[1:]],
        jax.ShapeDtypeStruct((8, known * slots), jnp.float32),
        [
            rows((4 * others * 48, 128)),
            rows((others * (slots + 32), 8)),
        ],
        others * max(shares) * size,
    )
    forces = with_other(forces)
    first = slots // 128
    own, again, target, still = call(
        functools.partial(meet_still, slots, shards, parts),
        [*sent, *own],
        (own_shape, own_shape, target_shape, target_shape),
        [rows((7, shards * (size // 128 - first) * 8, 128))],
        slots * shards * (size - slots),
    )
    return call(
        functools.partial(finish, slots, shards, parts),
        [*sent, *forces, own, again, target, still, star_state, place],
        jax.ShapeDtypeStruct((12, size), jnp.float32),
        [rows((7, shards * first * 8, 128)), rows((8 * 48, 128)), rows((slots + 64, 8))],
    )


def solution(mesh):
    in_specs = (
        P(None, ("groups", "src")),
        P(("groups", "src")),
        P(("groups", "src")),
        P(("groups", "src")),
        P(("groups", "src", "act")),
        P(("groups", "src", "act")),
    )
    out_specs = P(None, ("groups", "src"))
    few = 3 <= mesh.shape["src"] <= MAX_DIRECT and mesh.shape["act"] % 2 == 0
    return jax.shard_map(
        direct_per_device if few else gather_per_device,
        mesh=mesh,
        in_specs=in_specs,
        out_specs=out_specs,
        check_vma=False,
    )
```

```python
import functools

import jax
import jax.numpy as jnp
from jax import lax
from jax.experimental import pallas as pl
from jax.experimental.pallas import tpu as pltpu
from jax.sharding import PartitionSpec as P


LEVELS = 5
STEPS = 2
MAX_DIRECT = 8


soften_sq = 0.0004
fine_step = 0.03125


def predict(star_state, elapsed):
    interval = elapsed[None, :]
    position = star_state[0:3] + interval * (
        star_state[3:6] + interval * (0.5 * star_state[6:9] + interval * star_state[9:12] / 6.0)
    )
    velocity = star_state[3:6] + interval * (star_state[6:9] + 0.5 * interval * star_state[9:12])
    return jnp.concatenate([position, velocity], axis=0)


def pair_block(targets, sources):
    delta_pos = sources[0:3, None, :] - targets[0:3, :, None]
    delta_vel = sources[3:6, None, :] - targets[3:6, :, None]
    dist_sq = (
        delta_pos[0] * delta_pos[0]
        + delta_pos[1] * delta_pos[1]
        + delta_pos[2] * delta_pos[2]
        + soften_sq
    )
    inverse = lax.rsqrt(dist_sq)
    inv_sq = inverse * inverse
    weight = sources[6][None, :] * inverse * inv_sq
    radial = (
        (delta_pos[0] * delta_vel[0] + delta_pos[1] * delta_vel[1] + delta_pos[2] * delta_vel[2])
        * inv_sq
        * 3.0
    )
    acceleration = jnp.sum(weight[None] * delta_pos, axis=2)
    jerk_sum = jnp.sum(weight[None] * (delta_vel - radial[None] * delta_pos), axis=2)
    return jnp.concatenate([acceleration, jerk_sum], axis=0)


def over_sources(targets, sources):
    count_src = sources.shape[1]
    width = 512
    blocks = sources.reshape(7, count_src // width, width).transpose(1, 0, 2)

    def accumulate(running, portion):
        return (running + pair_block(targets, portion), None)

    init = jnp.zeros((6, targets.shape[1]), jnp.float32)
    running, _ = lax.scan(accumulate, init, blocks)
    return running


def corrected(acc_old, jerk_old, position, velocity, acc_new, jerk_new):
    snap_term = (-6.0 * (acc_old - acc_new) - fine_step * (4.0 * jerk_old + 2.0 * jerk_new)) / (
        fine_step * fine_step
    )
    crackle = (12.0 * (acc_old - acc_new) + 6.0 * fine_step * (jerk_old + jerk_new)) / (
        fine_step * fine_step * fine_step
    )
    new_position = position + fine_step**4 / 24.0 * snap_term + fine_step**5 / 120.0 * crackle
    new_velocity = velocity + fine_step**3 / 6.0 * snap_term + fine_step**4 / 24.0 * crackle
    return new_position, new_velocity


def correct(old_state, predicted_rows, forces):
    new_position, new_velocity = corrected(
        old_state[6:9],
        old_state[9:12],
        predicted_rows[0:3],
        predicted_rows[3:6],
        forces[0:3],
        forces[3:6],
    )
    return jnp.concatenate([new_position, new_velocity, forces], axis=0)


def gather_per_device(star_state, masses, phases, levels, active_list, active_count):
    shard_size = star_state.shape[1]
    total_stars = shard_size * lax.axis_size("src")
    weights = masses / total_stars
    slot_count = active_list.shape[0]
    live = jnp.arange(slot_count, dtype=jnp.int32) < active_count[0]
    write_index = jnp.where(live, active_list, shard_size)
    tick_count = jnp.left_shift(jnp.int32(1), LEVELS - 1 - levels).astype(jnp.float32)
    state_now = star_state
    for substep in range(STEPS):
        elapsed = (
            jnp.where(levels == LEVELS - 1, 1.0, phases * (tick_count - STEPS) + (substep + 1))
            * fine_step
        )
        predicted = predict(state_now, elapsed)
        sources = jnp.concatenate([predicted, weights[None, :]], axis=0)
        targets = predicted[:, active_list]
        forces = over_sources(targets, lax.all_gather(sources, "src", axis=1, tiled=True))
        new_state = correct(state_now[:, active_list], targets, forces)
        all_new, all_index = (
            lax.all_gather(new_state, "act", axis=1, tiled=True),
            lax.all_gather(write_index, "act", axis=0, tiled=True),
        )
        state_now = state_now.at[:, all_index].set(all_new, mode="drop")
    return state_now


def three_terms(x):
    high = x.astype(jnp.bfloat16)
    rest = x - high.astype(jnp.float32)
    middle = rest.astype(jnp.bfloat16)
    low = (rest - middle.astype(jnp.float32)).astype(jnp.bfloat16)
    return jnp.concatenate([high, middle, low], axis=0)


def add_terms(y):
    rows = y.shape[0] // 3
    return (y[0:rows] + y[rows : 2 * rows]) + y[2 * rows : 3 * rows]


def advance(position, velocity, acceleration, jerk, step):
    ahead = position + step * (velocity + step * (0.5 * acceleration + step * jerk / 6.0))
    speed = velocity + step * (acceleration + 0.5 * step * jerk)
    return ahead, speed


def prepare(slots, total_stars, *refs):
    out_ref, place_ref = refs[4:6]
    copies = [
        pltpu.make_async_copy(far, near, refs[10].at[k])
        for k, (far, near) in enumerate(zip(refs[0:4], refs[6:10]))
    ]
    for copy in copies:
        copy.start()
    for copy in copies:
        copy.wait()
    state_ref, mass_ref, phase_ref, level_ref = refs[6:10]
    size = state_ref.shape[1]
    level = level_ref[...]
    active = level == LEVELS - 1
    mask = jnp.where(active, 1.0, 0.0)
    blocks = size // 128
    grouped = jnp.concatenate(
        [mask[:, 128 * b : 128 * (b + 1)] for b in range(blocks)]
        + [jnp.zeros((16 - blocks, 128), jnp.float32)],
        axis=0,
    ).astype(jnp.bfloat16)
    lane_in = lax.broadcasted_iota(jnp.int32, (128, 256), 0)
    lane_out = lax.broadcasted_iota(jnp.int32, (128, 256), 1)
    counting = jnp.where((lane_in <= lane_out) | (lane_out >= 128), 1.0, 0.0).astype(jnp.bfloat16)
    counts = jnp.dot(grouped, counting, preferred_element_type=jnp.float32)
    so_far = []
    before = jnp.zeros((1, 128), jnp.float32)
    for b in range(blocks):
        so_far.append(counts[b : b + 1, 0:128] + before)
        before = before + counts[b : b + 1, 128:256]
    rank = jnp.concatenate(so_far, axis=1)
    total = jnp.concatenate([before] * blocks, axis=1)
    star = lax.broadcasted_iota(jnp.int32, (1, size), 1).astype(jnp.float32)
    place = jnp.where(active, rank - 1.0, total + star - rank)
    place_ref[0:1, :] = place
    place_ref[1:2, :] = mask
    place_ref[2:8, :] = jnp.zeros((6, size), jnp.float32)

    tick_count = jnp.left_shift(jnp.int32(1), LEVELS - 1 - level).astype(jnp.float32)
    offset = phase_ref[...] * (tick_count - STEPS)
    position, velocity = state_ref[0:3, :], state_ref[3:6, :]
    acceleration, jerk = state_ref[6:9, :], state_ref[9:12, :]
    rows = []
    for substep in range(STEPS):
        elapsed = jnp.where(active, 1.0, offset + (substep + 1)) * fine_step
        rows.extend(advance(position, velocity, acceleration, jerk, elapsed))
        if substep == 0:
            rows.append(mass_ref[...] / total_stars)
            rows.append(mask)
    rows.append(jnp.zeros((2, size), jnp.float32))
    rows.extend([acceleration, jerk, jnp.zeros((10, size), jnp.float32)])
    terms = three_terms(jnp.concatenate(rows, axis=0))
    slot = lax.broadcasted_iota(jnp.int32, (size, size), 0).astype(jnp.float32)
    chosen = jnp.where(slot == place, 1.0, 0.0).astype(jnp.bfloat16)
    moved = add_terms(
        lax.dot_general(
            terms, chosen, (((1,), (1,)), ((), ())), preferred_element_type=jnp.float32
        )
    )
    out_ref[...] = moved[0:16]
    across = size // slots
    for k in range(6):
        out_ref[14 + k // across : 15 + k // across, slots * (k % across) : slots * (k % across + 1)] = (
            moved[16 + k : 17 + k, 0:slots]
        )


def pair_terms(source, target, sums):
    sx, sy, sz, su, sv, sw, weight = source
    tx, ty, tz, tu, tv, tw = target
    dx, dy, dz = sx - tx, sy - ty, sz - tz
    du, dv, dw = su - tu, sv - tv, sw - tw
    inverse = lax.rsqrt(dx * dx + dy * dy + (dz * dz + soften_sq))
    inv_sq = inverse * inverse
    pull = weight * inverse * inv_sq
    radial = (dx * du + dy * dv + dz * dw) * (inv_sq * 3.0)
    ax, ay, az, jx, jy, jz = sums
    return (
        ax + pull * dx,
        ay + pull * dy,
        az + pull * dz,
        jx + pull * (du - radial * dx),
        jy + pull * (dv - radial * dy),
        jz + pull * (dw - radial * dz),
    )


def spread_sources(rows, spread_ref, first):
    for c in range(rows.shape[1] // 128):
        for r in range(7):
            spread_ref[r, 8 * (first + c) : 8 * (first + c + 1), :] = jnp.broadcast_to(
                rows[r : r + 1, 128 * c : 128 * (c + 1)], (8, 128)
            )


def spread_targets(rows, spread_ref, start, count):
    columns = jnp.transpose(rows)
    for r in range(6):
        spread_ref[r, start : start + count, :] = jnp.broadcast_to(
            columns[start : start + count, r : r + 1], (count, 128)
        )


def run_pairs(groups, slots, start, count, together, finish, partial_ref, sums_ref):
    lead = 8 * together
    stride = slots + lead

    def reduce(place, many):
        for g in range(many):
            for j in range(len(groups)):
                for q in range(6):
                    row = ((g * len(groups) + j) * 6 + q) * 8
                    sums_ref[pl.ds(j * stride + place + 8 * g, 8), q : q + 1] = jnp.sum(
                        partial_ref[row : row + 8, :], axis=1, keepdims=True
                    )

    def block(base, many):
        for g in range(many):
            here = pl.ds(base + 8 * g, 8)
            for j, (target_ref, columns_ref, before_ref, sources, after_ref) in enumerate(groups):
                if columns_ref is None:
                    target = [target_ref[r, here, :] for r in range(6)]
                else:
                    columns = columns_ref[here, :]
                    target = [jnp.broadcast_to(columns[:, r : r + 1], (8, 128)) for r in range(6)]
                    if target_ref is not None:
                        for r in range(6):
                            target_ref[r, here, :] = target[r]
                if before_ref is None:
                    sums = (jnp.zeros((8, 128), jnp.float32),) * 6
                else:
                    sums = tuple(before_ref[q, here, :] for q in range(6))
                for source_ref in sources:
                    for c in range(source_ref.shape[1] // 8):
                        source = [source_ref[r, 8 * c : 8 * (c + 1), :] for r in range(7)]
                        sums = pair_terms(source, target, sums)
                for q in range(6):
                    if finish:
                        row = ((g * len(groups) + j) * 6 + q) * 8
                        partial_ref[row : row + 8, :] = sums[q]
                    else:
                        after_ref[q, here, :] = sums[q]

    def body(step, unused):
        base = pl.multiple_of(start + step * lead, 8)
        if finish:
            reduce(base, together)
        block(base, together)
        return unused

    if finish:
        used = together * len(groups) * 48
        partial_ref[0:used, :] = jnp.zeros((used, 128), jnp.float32)
        if count < slots:
            sums_ref[...] = jnp.zeros_like(sums_ref)
    steps = count // lead
    lax.fori_loop(0, steps, body, 0)
    rest = (count - steps * lead) // 8
    end = start + steps * lead
    if finish:
        reduce(end, together)
    if rest:
        block(end, rest)
        if finish:
            reduce(end + lead, rest)
    if not finish:
        return None
    return [
        jnp.transpose(sums_ref[j * stride + lead : (j + 1) * stride, :])
        for j in range(len(groups))
    ]


def on_member(shares, run):
    member = lax.rem(lax.axis_index("act"), len(shares))
    for m in range(len(shares)):

        @pl.when(member == m)
        def _():
            run(sum(shares[:m]), shares[m])


def meet(slots, shares, known, fresh, *refs):
    every = known + fresh
    sent, refs = refs[:fresh], refs[fresh:]
    old_sources, old_targets, before = refs[:known], refs[known : 2 * known], refs[2 * known : 3 * known]
    refs = refs[3 * known :]
    new_sources, new_targets, after = refs[:fresh], refs[fresh : 2 * fresh], refs[2 * fresh : 2 * fresh + every]
    columns_ref = refs[2 * fresh + every]
    sources = old_sources + new_sources

    def run(start, count):
        groups = []
        for d in range(known):
            groups.append((old_targets[d], None, before[d], new_sources, after[d]))
        for d in range(fresh):
            spread_sources(sent[d][0:8, :], new_sources[d], 0)
            in_loop = None
            if known:
                in_loop = columns_ref
                columns_ref[...] = jnp.transpose(sent[d][0:8, 0:slots])
            else:
                spread_targets(sent[d][0:8, 0:slots], new_targets[d], start, count)
            groups.append((new_targets[d], in_loop, None, sources, after[known + d]))
        run_pairs(groups, slots, start, count, 2, False, None, None)

    on_member(shares, run)


def meet_own(slots, shares, early, sent_ref, own_target, own_before, *refs):
    known = len(refs) - 8
    sources = refs[:known]
    source_ref, own_ref, late_ref, target_ref, own_partial, own_sums, partial_ref, sums_ref = refs[known:]
    spread_sources(sent_ref[0:8, :], source_ref, 0)

    def own(start, count):
        group = (own_target, None, own_before, (source_ref,), None)
        own_ref[...] = run_pairs(
            [group], slots, start, count, count // 8, True, own_partial, own_sums
        )[0]

    member = lax.rem(lax.axis_index("act"), 2)

    @pl.when(member == 0)
    def _():
        late_ref[...] = jnp.zeros_like(late_ref)
        spread_targets(sent_ref[0:8, 0:slots], target_ref, early, slots - early)
        own(0, shares[0])

    @pl.when(member == 1)
    def _():
        spread_targets(sent_ref[0:8, 0:slots], target_ref, 0, slots)
        own(shares[0], shares[1])
        group = (target_ref, None, None, sources + (source_ref,), None)
        late_ref[...] = run_pairs([group], slots, 0, early, 4, True, partial_ref, sums_ref)[0]


def meet_rest(slots, shares, early, source_ref, late_ref, late_target, *refs):
    known = (len(refs) - 4) // 3
    sources, targets, before = refs[: known + 1], refs[known + 1 : 2 * known + 1], refs[2 * known + 1 : 3 * known + 1]
    forces_ref, partial_ref, sums_ref = refs[3 * known + 1 :]

    def run(start, count):
        groups = [(t, None, b, (source_ref,), None) for t, b in zip(targets, before)]
        forces = run_pairs(groups, slots, start, count, 4, True, partial_ref, sums_ref)
        for d in range(known):
            forces_ref[:, d * slots : (d + 1) * slots] = forces[d]
        late = late_ref[...]
        if start == 0:
            group = (late_target, None, None, sources + (source_ref,), None)
            late += run_pairs(
                [group],
                slots,
                early,
                slots - early,
                2,
                True,
                partial_ref.at[0:96],
                sums_ref.at[0 : slots + 16],
            )[0]
        forces_ref[:, known * slots : (known + 1) * slots] = late

    on_member(shares, run)


def first_step(slots, sent, forces):
    size = sent.shape[1]
    across = size // slots
    old = [
        sent[14 + k // across : 15 + k // across, slots * (k % across) : slots * (k % across + 1)]
        for k in range(6)
    ]
    old = jnp.concatenate(old, axis=0)
    position, velocity = corrected(
        old[0:3], old[3:6], sent[0:3, 0:slots], sent[3:6, 0:slots], forces[0:3], forces[3:6]
    )
    ahead, speed = advance(position, velocity, forces[0:3], forces[3:6], fine_step)
    active = sent[7:8, 0:slots] > 0.5
    return jnp.where(active, jnp.concatenate([ahead, speed], axis=0), sent[8:14, 0:slots])


def meet_still(slots, shards, parts, *refs):
    sent, refs = refs[:shards], refs[shards:]
    shares, refs = refs[:parts], refs[parts:]
    own_ref, again_ref, target_ref, after_ref, still_ref = refs
    own_ref[...] = shares[0][...] + shares[1][...] if parts == 2 else shares[0][...]
    size = sent[0].shape[1]
    chunks = size // 128
    first = slots // 128
    again = first_step(slots, sent[0], own_ref[...])
    again = jnp.concatenate([again, jnp.zeros((2, slots), jnp.float32)], axis=0)
    again_ref[...] = again
    for d in range(shards):
        rows = jnp.concatenate([sent[d][8:14, slots:size], sent[d][6:8, slots:size]], axis=0)
        spread_sources(rows, still_ref, d * (chunks - first))
    spread_targets(again, target_ref, 0, slots)
    run_pairs(
        [(target_ref, None, None, (still_ref,), after_ref)], slots, 0, slots, 4, False, None, None
    )


def finish(slots, shards, parts, *refs):
    sent, refs = refs[:shards], refs[shards:]
    shares, refs = refs[:parts], refs[parts:]
    own_ref, again_ref, target_ref, before_ref, state_ref, place_ref, out_ref = refs[:7]
    later_ref, partial_ref, sums_ref = refs[7:]
    size = state_ref.shape[1]
    first = slots // 128
    own = again_ref[...]
    for d in range(shards):
        if d == 0:
            again = own[0:6]
        else:
            share = [s[:, (d - 1) * slots : d * slots] for s in shares]
            again = first_step(
                slots, sent[d], share[0] + share[1] if parts == 2 else share[0]
            )
        rows = jnp.concatenate([again, sent[d][6:8, 0:slots]], axis=0)
        spread_sources(rows, later_ref, d * first)
    second = run_pairs(
        [(target_ref, None, before_ref, (later_ref,), None)],
        slots,
        0,
        slots,
        8,
        True,
        partial_ref,
        sums_ref,
    )[0]
    before = own_ref[...]
    position, velocity = corrected(
        before[0:3], before[3:6], own[0:3], own[3:6], second[0:3], second[3:6]
    )
    new_rows = jnp.concatenate(
        [position, velocity, second[0:6], jnp.zeros((4, slots), jnp.float32)], axis=0
    )
    slot = lax.broadcasted_iota(jnp.int32, (slots, size), 0).astype(jnp.float32)
    chosen = jnp.where(slot == place_ref[0:1, :], 1.0, 0.0).astype(jnp.bfloat16)
    back = add_terms(jnp.dot(three_terms(new_rows), chosen, preferred_element_type=jnp.float32))
    out_ref[...] = jnp.where(place_ref[1:2, :] > 0.5, back[0:12], state_ref[...])


def direct_per_device(star_state, masses, phases, levels, active_list, active_count):
    del active_count
    size = star_state.shape[1]
    shards = lax.axis_size("src")
    slots = 2 * active_list.shape[0]
    whole = pl.BlockSpec(memory_space=pltpu.VMEM)
    message, place = pl.pallas_call(
        lambda *refs: prepare(slots, size * shards, *refs),
        out_shape=(
            jax.ShapeDtypeStruct((16, size), jnp.float32),
            jax.ShapeDtypeStruct((8, size), jnp.float32),
        ),
        in_specs=[pl.BlockSpec(memory_space=pltpu.HBM)] * 4,
        out_specs=(whole, whole),
        scratch_shapes=[
            pltpu.VMEM((12, size), jnp.float32),
            pltpu.VMEM((1, size), jnp.float32),
            pltpu.VMEM((1, size), jnp.float32),
            pltpu.VMEM((1, size), jnp.int32),
            pltpu.SemaphoreType.DMA((4,)),
        ],
        compiler_params=pltpu.CompilerParams(vmem_limit_bytes=16 * 2**20),
        name="prepare",
    )(
        *(
            pltpu.with_memory_space_constraint(x, pltpu.HBM)
            for x in (star_state, masses.reshape(1, size), phases.reshape(1, size), levels.reshape(1, size))
        )
    )
    sent = [message]
    for shift in range(1, shards):
        pairs = [(d, (d + shift) % shards) for d in range(shards)]
        sent.append(lax.ppermute(message, "src", pairs))

    limit = pltpu.CompilerParams(vmem_limit_bytes=16 * 2**20)
    owners = lax.axis_size("act")
    shares = (slots // 2, slots - slots // 2)
    parts = len(shares)

    def with_other(part):
        return [part, lax.ppermute(part, "act", [(i, i ^ 1) for i in range(owners)])]

    def call(body, operands, out_shape, scratch=(), pairs=0):
        cost = pl.CostEstimate(flops=41 * pairs, bytes_accessed=0, transcendentals=pairs)
        return pl.pallas_call(
            body,
            out_shape=out_shape,
            in_specs=[whole] * len(operands),
            out_specs=jax.tree.map(lambda _: whole, out_shape),
            scratch_shapes=list(scratch),
            compiler_params=limit,
            cost_estimate=cost if pairs else None,
        )(*operands)

    def rows(shape):
        return pltpu.VMEM(shape, jnp.float32)

    source_shape = jax.ShapeDtypeStruct((7, size // 16, 128), jnp.float32)
    target_shape = jax.ShapeDtypeStruct((6, slots, 128), jnp.float32)
    own_shape = jax.ShapeDtypeStruct((8, slots), jnp.float32)
    sources, targets, sums = [], [], []
    known = 0
    for fresh in [2] + [1] * (shards - 3):
        every = known + fresh
        outs = call(
            functools.partial(meet, slots, shares, known, fresh),
            [*sent[known:every], *sources, *targets, *sums],
            [source_shape] * fresh + [target_shape] * (fresh + every),
            [rows((slots, 8))],
        )
        sources += outs[:fresh]
        targets += outs[fresh : 2 * fresh]
        sums = list(outs[2 * fresh :])
        known = every
    early = slots * 7 // 8
    source, own, late, late_target = call(
        functools.partial(meet_own, slots, shares, early),
        [sent[known], targets[0], sums[0], *sources],
        (source_shape, own_shape, own_shape, target_shape),
        [
            rows((max(shares) * 6, 128)),
            rows((slots + max(shares), 8)),
            rows((4 * 48, 128)),
            rows((slots + 32, 8)),
        ],
    )
    others = known - 1
    own = with_other(own)
    forces = call(
        functools.partial(meet_rest, slots, shares, early),
        [source, late, late_target, *sources, *targets[1:], *sums[1:]],
        jax.ShapeDtypeStruct((8, known * slots), jnp.float32),
        [
            rows((4 * others * 48, 128)),
            rows((others * (slots + 32), 8)),
        ],
        others * max(shares) * size,
    )
    forces = with_other(forces)
    first = slots // 128
    own, again, target, still = call(
        functools.partial(meet_still, slots, shards, parts),
        [*sent, *own],
        (own_shape, own_shape, target_shape, target_shape),
        [rows((7, shards * (size // 128 - first) * 8, 128))],
        slots * shards * (size - slots),
    )
    return call(
        functools.partial(finish, slots, shards, parts),
        [*sent, *forces, own, again, target, still, star_state, place],
        jax.ShapeDtypeStruct((12, size), jnp.float32),
        [rows((7, shards * first * 8, 128)), rows((8 * 48, 128)), rows((slots + 64, 8))],
    )


def solution(mesh):
    in_specs = (
        P(None, ("groups", "src")),
        P(("groups", "src")),
        P(("groups", "src")),
        P(("groups", "src")),
        P(("groups", "src", "act")),
        P(("groups", "src", "act")),
    )
    out_specs = P(None, ("groups", "src"))
    few = 3 <= mesh.shape["src"] <= MAX_DIRECT and mesh.shape["act"] % 2 == 0
    return jax.shard_map(
        direct_per_device if few else gather_per_device,
        mesh=mesh,
        in_specs=in_specs,
        out_specs=out_specs,
        check_vma=False,
    )
```
